32 devices in a mesh: dp: 1 (over z), tx: 4 (over y), ty: 8 (over x, core).
Axes of the slice: x: 4, y: 4, z: 1, core: 2. Of those that a mesh axis runs over, the one named last changes fastest.
The devices are a block of a 4x4x8 slice.
Arguments:
- x_act: bfloat16 [8, 1536, 2048], P('dp', None, 'tx')
- cot_out: bfloat16 [8, 1536, 2048], P('dp', None, 'tx')
- ln1_gain: bfloat16 [2048], P('tx')
- ln1_bias: bfloat16 [2048], P('tx')
- ln2_gain: bfloat16 [2048], P('tx')
- ln2_bias: bfloat16 [2048], P('tx')
- w_qkv: bfloat16 [2048, 8, 768], P('tx', 'ty')
- b_qkv: bfloat16 [8, 768], P('ty')
- w_dense: bfloat16 [2048, 2048], P('ty', 'tx')
- b_dense: bfloat16 [2048], P('tx')
- w_up: bfloat16 [2048, 8192], P('tx', 'ty')
- b_up: bfloat16 [8192], P('ty')
- w_down: bfloat16 [8192, 2048], P('ty', 'tx')
- b_down: bfloat16 [2048], P('tx')
Outputs:
- output 1: bfloat16 [8, 1536, 2048], P('dp', None, 'tx')
- output 2: bfloat16 [8, 1536, 2048], P('dp', None, 'tx')
- output 3: float32 [2048], P(('dp', 'tx'))
- output 4: float32 [2048], P(('dp', 'tx'))
- output 5: float32 [2048], P(('dp', 'tx'))
- output 6: float32 [2048], P(('dp', 'tx'))
- output 7: float32 [2048, 8, 768], P(('dp', 'tx'), 'ty')
- output 8: float32 [8, 768], P(('dp', 'ty'))
- output 9: float32 [2048, 2048], P(('dp', 'ty'), 'tx')
- output 10: float32 [2048], P(('dp', 'tx'))
- output 11: float32 [2048, 8192], P(('dp', 'tx'), 'ty')
- output 12: float32 [8192], P(('dp', 'ty'))
- output 13: float32 [8192, 2048], P(('dp', 'ty'), 'tx')
- output 14: float32 [2048], P(('dp', 'tx'))
All inputs are finite; a program needn't handle non-finite values.
Results may differ from the reference program's by a relative error of at most 0.02.
Values are sent between devices in bfloat16 or wider.
A program may use at most 768 MiB of HBM per device.

```python
import jax
import jax.numpy as jnp
from jax import lax

BATCH = 8
SEQ_LEN = 1536
D_MODEL = 2048
N_HEADS = 8
HEAD_DIM = 256
ROT_DIM = HEAD_DIM // 4
FF_DIM = 4 * D_MODEL
LN_EPS = 1e-5
ROPE_BASE = 10000.0


def setup_inputs(seed: int = 0, part: int = 0) -> dict:
    base_key = jax.random.key(seed)
    act_keys = jax.random.split(jax.random.fold_in(base_key, part), 4)
    param_keys = jax.random.split(jax.random.key(seed + 1), 12)
    shape = (BATCH, SEQ_LEN, D_MODEL)
    col_pos = (jnp.arange(D_MODEL, dtype=jnp.float32) + 0.5) / D_MODEL
    noise = jax.random.normal(act_keys[0], shape, jnp.float32)
    slopes = 1.5 * jax.random.normal(act_keys[1], (BATCH, SEQ_LEN, 1), jnp.float32)
    offsets = 0.5 * jax.random.normal(act_keys[2], (BATCH, SEQ_LEN, 1), jnp.float32)
    x_act = noise * (0.5 + 1.5 * col_pos) + slopes * (2.0 * col_pos - 1.0) + offsets
    cot_out = jax.random.normal(act_keys[3], shape, jnp.float32)

    def normal_param(index, dims, spread, center):
        draw = jax.random.normal(param_keys[index], dims, jnp.float32)
        return (center + spread * draw).astype(jnp.bfloat16)

    return {
        'x_act': x_act.astype(jnp.bfloat16),
        'cot_out': cot_out.astype(jnp.bfloat16),
        'ln1_gain': normal_param(0, (D_MODEL,), 0.3, 1.0),
        'ln1_bias': normal_param(1, (D_MODEL,), 0.3, 0.0),
        'ln2_gain': normal_param(2, (D_MODEL,), 0.3, 1.0),
        'ln2_bias': normal_param(3, (D_MODEL,), 0.3, 0.0),
        'w_qkv': normal_param(4, (D_MODEL, N_HEADS, 3 * HEAD_DIM), D_MODEL ** -0.5, 0.0),
        'b_qkv': normal_param(5, (N_HEADS, 3 * HEAD_DIM), 0.3, 0.0),
        'w_dense': normal_param(6, (D_MODEL, D_MODEL), D_MODEL ** -0.5, 0.0),
        'b_dense': normal_param(7, (D_MODEL,), 0.3, 0.0),
        'w_up': normal_param(8, (D_MODEL, FF_DIM), D_MODEL ** -0.5, 0.0),
        'b_up': normal_param(9, (FF_DIM,), 0.3, 0.0),
        'w_down': normal_param(10, (FF_DIM, D_MODEL), FF_DIM ** -0.5, 0.0),
        'b_down': normal_param(11, (D_MODEL,), 0.3, 0.0),
    }


def rotary_tables(positions):
    inv_freq = ROPE_BASE ** (-jnp.arange(0, ROT_DIM, 2, dtype=jnp.float32) / ROT_DIM)
    angles = positions[:, None] * inv_freq[None, :]
    angles = jnp.concatenate([angles, angles], axis=-1)
    return jnp.cos(angles), jnp.sin(angles)


def apply_rotary(tensor, cos_tab, sin_tab):
    half_rot = ROT_DIM // 2
    rot_part = tensor[..., :ROT_DIM]
    turned = jnp.concatenate([-rot_part[..., half_rot:], rot_part[..., :half_rot]], axis=-1)
    mixed = rot_part * cos_tab[:, None, :] + turned * sin_tab[:, None, :]
    return jnp.concatenate([mixed, tensor[..., ROT_DIM:]], axis=-1)


def head_attention(operands):
    q_head, k_head, v_head = operands
    scores = jnp.einsum('bqe,bke->bqk', q_head.astype(jnp.float32), k_head.astype(jnp.float32)) * HEAD_DIM ** -0.5
    seq_index = jnp.arange(SEQ_LEN)
    causal = seq_index[:, None] >= seq_index[None, :]
    scores = jnp.where(causal[None], scores, -1e30)
    probs = jax.nn.softmax(scores, axis=-1).astype(jnp.bfloat16)
    context = jnp.einsum('bqk,bke->bqe', probs.astype(jnp.float32), v_head.astype(jnp.float32))
    return context.astype(jnp.bfloat16)


def layer_forward(x_act, ln1_gain, ln1_bias, ln2_gain, ln2_bias, w_qkv, b_qkv, w_dense, b_dense, w_up, b_up, w_down, b_down):
    tokens = BATCH * SEQ_LEN
    x_float = x_act.astype(jnp.float32)
    mean = jnp.mean(x_float, axis=-1, keepdims=True)
    variance = jnp.mean(x_float * x_float, axis=-1, keepdims=True) - mean * mean
    x_hat = (x_float - mean) * lax.rsqrt(variance + LN_EPS)
    h_attn = (x_hat * ln1_gain.astype(jnp.float32) + ln1_bias.astype(jnp.float32)).astype(jnp.bfloat16)
    h_mlp = (x_hat * ln2_gain.astype(jnp.float32) + ln2_bias.astype(jnp.float32)).astype(jnp.bfloat16)
    qkv_act = jnp.dot(h_attn.reshape(tokens, D_MODEL), w_qkv.reshape(D_MODEL, 3 * D_MODEL), preferred_element_type=jnp.float32)
    qkv_act = (qkv_act.reshape(BATCH, SEQ_LEN, N_HEADS, 3 * HEAD_DIM) + b_qkv.astype(jnp.float32)).astype(jnp.bfloat16)
    cos_tab, sin_tab = rotary_tables(jnp.arange(SEQ_LEN, dtype=jnp.float32))
    q_rot = apply_rotary(qkv_act[..., :HEAD_DIM].astype(jnp.float32), cos_tab, sin_tab).astype(jnp.bfloat16)
    k_rot = apply_rotary(qkv_act[..., HEAD_DIM:2 * HEAD_DIM].astype(jnp.float32), cos_tab, sin_tab).astype(jnp.bfloat16)
    values = qkv_act[..., 2 * HEAD_DIM:]
    per_head = (jnp.moveaxis(q_rot, 2, 0), jnp.moveaxis(k_rot, 2, 0), jnp.moveaxis(values, 2, 0))
    context = lax.map(jax.checkpoint(head_attention), per_head)
    context = jnp.moveaxis(context, 0, 2).reshape(tokens, D_MODEL)
    attn_out = jnp.dot(context, w_dense, preferred_element_type=jnp.float32) + b_dense.astype(jnp.float32)
    pre_act = jnp.dot(h_mlp.reshape(tokens, D_MODEL), w_up, preferred_element_type=jnp.float32) + b_up.astype(jnp.float32)
    pre_act = pre_act.astype(jnp.bfloat16)
    gelu_out = jax.nn.gelu(pre_act.astype(jnp.float32), approximate=False).astype(jnp.bfloat16)
    mlp_out = jnp.dot(gelu_out, w_down, preferred_element_type=jnp.float32) + b_down.astype(jnp.float32)
    y_float = x_float + (attn_out + mlp_out).reshape(BATCH, SEQ_LEN, D_MODEL)
    return y_float.astype(jnp.bfloat16)


def reference(x_act, cot_out, ln1_gain, ln1_bias, ln2_gain, ln2_bias, w_qkv, b_qkv, w_dense, b_dense, w_up, b_up, w_down, b_down):
    y_out, pullback = jax.vjp(layer_forward, x_act, ln1_gain, ln1_bias, ln2_gain, ln2_bias, w_qkv, b_qkv, w_dense, b_dense, w_up, b_up, w_down, b_down)
    grad_list = pullback(cot_out)
    return (y_out, grad_list[0], grad_list[1].astype(jnp.float32), grad_list[2].astype(jnp.float32), grad_list[3].astype(jnp.float32), grad_list[4].astype(jnp.float32), grad_list[5].astype(jnp.float32), grad_list[6].astype(jnp.float32), grad_list[7].astype(jnp.float32), grad_list[8].astype(jnp.float32), grad_list[9].astype(jnp.float32), grad_list[10].astype(jnp.float32), grad_list[11].astype(jnp.float32), grad_list[12].astype(jnp.float32))
```

```python
import functools
import jax
import jax.numpy as jnp
from jax import lax
from jax.experimental import pallas as pl
from jax.experimental.pallas import tpu as pltpu
from jax.sharding import PartitionSpec as P


LN_EPS = 1e-5
ROPE_BASE = 10000.0
ROTARY_DIVISOR = 4
LANES = 128
Q_ROWS = 256

NT = (((1,), (1,)), ((), ()))
TN = (((0,), (0,)), ((), ()))
NN = (((1,), (0,)), ((), ()))


def dot(a, b, dims):
    return lax.dot_general(a, b, dims, preferred_element_type=jnp.float32)


def rotary_tables(seq_len, rot_dim):
    half = rot_dim // 2
    lane = jnp.arange(LANES)
    freq_index = jnp.where(lane < half, lane, lane - half)
    inv_freq = ROPE_BASE ** (-(2 * freq_index).astype(jnp.float32) / rot_dim)
    angles = jnp.arange(seq_len, dtype=jnp.float32)[:, None] * inv_freq[None, :]
    inside = (lane < rot_dim)[None, :]
    cos_tab = jnp.where(inside, jnp.cos(angles), 1.0)
    sin = jnp.where(inside, jnp.sin(angles), 0.0)
    first = (lane < half)[None, :]
    return cos_tab, jnp.where(first, -sin, 0.0), jnp.where(first, 0.0, sin)


def rotate(part, cos_tab, sin_lo, sin_hi, half, sign):
    head = part[:, :LANES]
    forward = pltpu.roll(head, half, 1)
    backward = pltpu.roll(head, LANES - half, 1)
    mixed = head * cos_tab + sign * (backward * sin_lo + forward * sin_hi)
    return jnp.concatenate([mixed, part[:, LANES:]], axis=1)


def causal_probs(q_rows, keys, row_start, scale):
    scores = dot(q_rows, keys, NT) * scale
    rows = row_start + lax.broadcasted_iota(jnp.int32, scores.shape, 0)
    cols = lax.broadcasted_iota(jnp.int32, scores.shape, 1)
    scores = jnp.where(rows >= cols, scores, -1e30)
    exps = jnp.exp(scores - jnp.max(scores, axis=1, keepdims=True))
    return exps * (1.0 / jnp.sum(exps, axis=1, keepdims=True))


def attn_fwd_kernel(qkv_ref, cos_ref, lo_ref, hi_ref, ctx_ref, q_ref, k_ref, *, half, scale, span):
    seq_len, width = ctx_ref.shape[1:]

    @pl.loop(0, seq_len // Q_ROWS)
    def _(step):
        rows = pl.ds(pl.multiple_of(step * Q_ROWS, Q_ROWS), Q_ROWS)
        for out, col in ((q_ref, 0), (k_ref, width)):
            part = qkv_ref[0, rows, col:col + width].astype(jnp.float32)
            out[rows, :] = rotate(part, cos_ref[rows, :], lo_ref[rows, :], hi_ref[rows, :], half, 1.0).astype(jnp.bfloat16)

    for end in range(span, seq_len + 1, span):
        @pl.loop(0, span // Q_ROWS)
        def _(step, end=end):
            start = pl.multiple_of(end - span + step * Q_ROWS, Q_ROWS)
            rows = pl.ds(start, Q_ROWS)
            probs = causal_probs(q_ref[rows, :], k_ref[:end, :], start, scale).astype(jnp.bfloat16)
            ctx_ref[0, rows, :] = dot(probs, qkv_ref[0, :end, 2 * width:], NN).astype(jnp.bfloat16)


def attn_bwd_kernel(qkv_ref, dctx_ref, cos_ref, lo_ref, hi_ref, dqkv_ref, db_ref, q_ref, k_ref, dk_ref, dv_ref, *, half, scale, span):
    seq_len, width = dctx_ref.shape[1:]

    @pl.loop(0, seq_len // Q_ROWS)
    def _(step):
        rows = pl.ds(pl.multiple_of(step * Q_ROWS, Q_ROWS), Q_ROWS)
        for out, col in ((q_ref, 0), (k_ref, width)):
            part = qkv_ref[0, rows, col:col + width].astype(jnp.float32)
            out[rows, :] = rotate(part, cos_ref[rows, :], lo_ref[rows, :], hi_ref[rows, :], half, 1.0).astype(jnp.bfloat16)
        dk_ref[rows, :] = jnp.zeros((Q_ROWS, width), jnp.float32)
        dv_ref[rows, :] = jnp.zeros((Q_ROWS, width), jnp.float32)

    db_ref[...] = jnp.zeros(db_ref.shape, jnp.float32)

    def store(rows, col, grad_rot, turn):
        grad = grad_rot.astype(jnp.bfloat16)
        if turn:
            wide = grad.astype(jnp.float32)
            grad = rotate(wide, cos_ref[rows, :], lo_ref[rows, :], hi_ref[rows, :], half, -1.0).astype(jnp.bfloat16)
        dqkv_ref[0, rows, col:col + width] = grad
        db_ref[0, :, col:col + width] += jnp.sum(grad.astype(jnp.float32), axis=0, keepdims=True)

    for end in range(span, seq_len + 1, span):
        @pl.loop(0, span // Q_ROWS)
        def _(step, end=end):
            start = pl.multiple_of(end - span + step * Q_ROWS, Q_ROWS)
            rows = pl.ds(start, Q_ROWS)
            q_rows = q_ref[rows, :]
            dctx = dctx_ref[0, rows, :]
            probs = causal_probs(q_rows, k_ref[:end, :], start, scale)
            dprobs = dot(dctx, qkv_ref[0, :end, 2 * width:], NT).astype(jnp.bfloat16).astype(jnp.float32)
            dv_ref[:end, :] += dot(probs.astype(jnp.bfloat16), dctx, TN)
            inner = jnp.sum(probs * dprobs, axis=1, keepdims=True)
            dscores = (probs * (dprobs - inner) * scale).astype(jnp.bfloat16)
            dk_ref[:end, :] += dot(dscores, q_rows, TN)
            store(rows, 0, dot(dscores, k_ref[:end, :], NN), True)

    @pl.loop(0, seq_len // Q_ROWS)
    def _(step):
        rows = pl.ds(pl.multiple_of(step * Q_ROWS, Q_ROWS), Q_ROWS)
        store(rows, width, dk_ref[rows, :], True)
        store(rows, 2 * width, dv_ref[rows, :], False)


def attention_calls(n_seq, seq_len, width):
    half = width // ROTARY_DIVISOR // 2
    scale = width ** -0.5
    span = 512 if seq_len % 512 == 0 else seq_len
    tables = rotary_tables(seq_len, 2 * half)
    seq_spec = lambda cols: pl.BlockSpec((1, seq_len, cols), lambda s: (s, 0, 0))
    tab_spec = pl.BlockSpec((seq_len, LANES), lambda s: (0, 0))
    rot_scratch = pltpu.VMEM((seq_len, width), jnp.bfloat16)
    acc_scratch = pltpu.VMEM((seq_len, width), jnp.float32)
    pairs = n_seq * seq_len * seq_len // 2
    params = pltpu.CompilerParams(dimension_semantics=("arbitrary",), vmem_limit_bytes=56 * 1024 * 1024)
    forward = pl.pallas_call(
        functools.partial(attn_fwd_kernel, half=half, scale=scale, span=span),
        grid=(n_seq,),
        in_specs=[seq_spec(3 * width), tab_spec, tab_spec, tab_spec],
        out_specs=seq_spec(width),
        out_shape=jax.ShapeDtypeStruct((n_seq, seq_len, width), jnp.bfloat16),
        scratch_shapes=[rot_scratch, rot_scratch],
        compiler_params=params,
        name="attn_fwd",
        cost_estimate=pl.CostEstimate(flops=8 * pairs * width, bytes_accessed=8 * n_seq * seq_len * width, transcendentals=pairs),
    )
    backward = pl.pallas_call(
        functools.partial(attn_bwd_kernel, half=half, scale=scale, span=span),
        grid=(n_seq,),
        in_specs=[seq_spec(3 * width), seq_spec(width), tab_spec, tab_spec, tab_spec],
        out_specs=[seq_spec(3 * width), pl.BlockSpec((1, 1, 3 * width), lambda s: (s, 0, 0))],
        out_shape=[jax.ShapeDtypeStruct((n_seq, seq_len, 3 * width), jnp.bfloat16), jax.ShapeDtypeStruct((n_seq, 1, 3 * width), jnp.float32)],
        scratch_shapes=[rot_scratch, rot_scratch, acc_scratch, acc_scratch],
        compiler_params=params,
        name="attn_bwd",
        cost_estimate=pl.CostEstimate(flops=20 * pairs * width, bytes_accessed=14 * n_seq * seq_len * width, transcendentals=pairs),
    )
    return (lambda qkv: forward(qkv, *tables)), (lambda qkv, dctx: backward(qkv, dctx, *tables))


def copy_kernel(row_ref, in_ref, out_ref):
    out_ref[...] = in_ref[...]


def place_groups(full, row):
    groups, tokens, width = full.shape
    rows = tokens // 4
    return pl.pallas_call(
        copy_kernel,
        grid_spec=pltpu.PrefetchScalarGridSpec(
            num_scalar_prefetch=1,
            grid=(groups, tokens // rows),
            in_specs=[pl.BlockSpec((1, rows, width), lambda t, c, row_ref: (lax.rem(row_ref[0] + groups - t, groups), c, 0))],
            out_specs=pl.BlockSpec((1, rows, width), lambda t, c, row_ref: (t, c, 0)),
        ),
        out_shape=jax.ShapeDtypeStruct(full.shape, full.dtype),
        name="place_groups",
        cost_estimate=pl.CostEstimate(flops=full.size, bytes_accessed=4 * full.size, transcendentals=0),
    )(row.reshape(1), full)


def split_width(value, out_refs):
    width = out_refs[0].shape[1]
    for index, out_ref in enumerate(out_refs):
        out_ref[...] = value[:, index * width:(index + 1) * width].astype(out_ref.dtype)


def finish_y_kernel(x_ref, mixed_ref, bias_ref, *out_refs):
    split_width(x_ref[...].astype(jnp.float32) + mixed_ref[...].astype(jnp.float32) + bias_ref[...], out_refs)


def normalize(act):
    act = act.astype(jnp.float32)
    mean = act.mean(-1, keepdims=True)
    inv_std = lax.rsqrt((act * act).mean(-1, keepdims=True) - mean * mean + LN_EPS)
    return (act - mean) * inv_std, inv_std


def finish_dx_kernel(x_ref, a6_ref, cot_ref, *out_refs):
    x_hat, inv_std = normalize(x_ref[...])
    value_a6 = a6_ref[...].astype(jnp.float32)
    mean_a6 = value_a6.mean(-1, keepdims=True)
    mean_a6x = (value_a6 * x_hat).mean(-1, keepdims=True)
    split_width(cot_ref[...].astype(jnp.float32) + inv_std * (value_a6 - mean_a6 - x_hat * mean_a6x), out_refs)


def row_call(kernel, parts, *operands):
    n_rows, width = operands[0].shape
    rows = 128 if n_rows % 128 == 0 else n_rows
    specs = [pl.BlockSpec((rows, width), lambda s: (s, 0)) if op.shape[0] == n_rows else pl.BlockSpec(op.shape, lambda s: (0, 0)) for op in operands]
    return pl.pallas_call(
        kernel,
        grid=(n_rows // rows,),
        in_specs=specs,
        out_specs=[pl.BlockSpec((rows, width // parts), lambda s: (s, 0))] * parts,
        out_shape=[jax.ShapeDtypeStruct((n_rows, width // parts), jnp.bfloat16)] * parts,
        cost_estimate=pl.CostEstimate(flops=16 * n_rows * width, bytes_accessed=8 * n_rows * width, transcendentals=0),
    )(*operands)


def gelu_bf16(pre_act):
    return jax.nn.gelu(pre_act.astype(jnp.float32), approximate=False).astype(jnp.bfloat16)


def solution(mesh):
    tx_size, ty_size = mesh.shape['tx'], mesh.shape['ty']
    act_spec = P('dp', None, 'tx')
    width_spec = P('tx')
    in_specs = (act_spec, act_spec, width_spec, width_spec, width_spec, width_spec, P('tx', 'ty', None), P('ty', None), P('ty', 'tx'), width_spec, P('tx', 'ty'), P('ty'), P('ty', 'tx'), width_spec)
    width_out = P(('dp', 'tx'))
    out_specs = (act_spec, act_spec, width_out, width_out, width_out, width_out, P(('dp', 'tx'), 'ty', None), P(('dp', 'ty'), None), P(('dp', 'ty'), 'tx'), width_out, P(('dp', 'tx'), 'ty'), P(('dp', 'ty')), P(('dp', 'ty'), 'tx'), width_out)
    antipode = tx_size // 2

    def shift(value, hops):
        return lax.ppermute(value, 'tx', [(s, (s - hops) % tx_size) for s in range(tx_size)])

    def small_sum(value, axis, size):
        step = 1
        while step < size:
            value = value + lax.ppermute(value, axis, [(s, s ^ step) for s in range(size)])
            step *= 2
        return value

    def ring_gather(block):
        blocks = {0: block}
        for hops in range(1, antipode):
            blocks[hops] = shift(blocks[hops - 1], 1)
            blocks[tx_size - hops] = shift(blocks[(tx_size - hops + 1) % tx_size], -1)
        rows = block.shape[0] // 2
        blocks[antipode] = jnp.concatenate([shift(blocks[antipode - 1][:rows], 1), shift(blocks[antipode + 1][rows:], -1)], axis=0)
        return [blocks[r] for r in range(tx_size)]

    def ring_scatter(make_part, rows):
        half = rows // 2
        far_low = make_part(antipode, 0, half).astype(jnp.bfloat16)
        far_high = make_part(antipode, half, rows).astype(jnp.bfloat16)
        moving_up, moving_down = shift(far_low, -1), shift(far_high, 1)
        moving_up = jnp.pad(moving_up, ((0, rows - half), (0, 0)))
        moving_down = jnp.pad(moving_down, ((half, 0), (0, 0)))
        for hops in range(antipode - 1, 0, -1):
            up = make_part(hops, 0, rows) + moving_up.astype(jnp.float32)
            down = make_part(tx_size - hops, 0, rows) + moving_down.astype(jnp.float32)
            up, down = up.astype(jnp.bfloat16), down.astype(jnp.bfloat16)
            moving_up, moving_down = shift(up, -1), shift(down, 1)
        return lambda own, low, high: own + moving_up[low:high].astype(jnp.float32) + moving_down[low:high].astype(jnp.float32)

    def body(x_act, cot_out, ln1_gain, ln1_bias, ln2_gain, ln2_bias, w_qkv, b_qkv, w_dense, b_dense, w_up, b_up, w_down, b_down):
        batch, seq_len, d_local = x_act.shape
        n_seq = batch // tx_size
        own = n_seq * seq_len // ty_size
        row, col = lax.axis_index('tx'), lax.axis_index('ty')
        qkv_width = w_qkv.shape[1] * w_qkv.shape[2]
        head = qkv_width // 3
        attn_fwd, attn_bwd = attention_calls(n_seq, seq_len, head)

        def to_tokens(act):
            parts = act.reshape(tx_size, ty_size, own, d_local)
            pick = lambda index: lax.dynamic_slice(parts, (index, col, 0, 0), (1, 1, own, d_local)).reshape(own, d_local)
            return jnp.concatenate([pick(row)] + [shift(pick((row - r) % tx_size), r) for r in range(1, tx_size)], axis=1)

        def to_width(parts):
            blocks = [parts[0]] + [shift(parts[r], -r) for r in range(1, tx_size)]
            stacked = jnp.stack(blocks)
            full = lax.all_gather(stacked, 'ty', axis=1, tiled=True)
            return place_groups(full, row).reshape(batch, seq_len, d_local)

        x_own = to_tokens(x_act)
        small = ring_gather(jnp.stack([ln1_gain, ln1_bias, ln2_gain, ln2_bias, b_dense, b_down]))
        small = jnp.concatenate(small, axis=1).astype(jnp.float32)
        gain_attn, bias_attn, gain_mlp, bias_mlp = small[0], small[1], small[2], small[3]
        bias_out = small[4] + small[5]
        x_group = lax.all_gather(x_own, 'ty', axis=0, tiled=True)
        w_in = jnp.concatenate([w_qkv.reshape(d_local, qkv_width), w_up], axis=1)
        w_in = jnp.concatenate(ring_gather(w_in), axis=0)
        wq, wu = w_in[:, :qkv_width], w_in[:, qkv_width:]
        cot_own = to_tokens(cot_out)
        cot_group = lax.all_gather(cot_own, 'ty', axis=0, tiled=True)
        w_back = jnp.concatenate(ring_gather(jnp.concatenate([w_dense, w_down], axis=0)), axis=1)

        x_hat, _ = normalize(x_group)
        h_attn = (x_hat * gain_attn + bias_attn).astype(jnp.bfloat16)
        h_mlp = (x_hat * gain_mlp + bias_mlp).astype(jnp.bfloat16)
        qkv_act = (dot(h_attn, wq, NN) + b_qkv.reshape(-1).astype(jnp.float32)).astype(jnp.bfloat16)
        qkv_seq = qkv_act.reshape(n_seq, seq_len, qkv_width)
        context = attn_fwd(qkv_seq).reshape(-1, head)
        pre_act = (dot(h_mlp, wu, NN) + b_up.astype(jnp.float32)).astype(jnp.bfloat16)
        gelu_out, gelu_pullback = jax.vjp(gelu_bf16, pre_act)
        inner = jnp.concatenate([context, gelu_out], axis=1)
        y_part = dot(inner, w_back, NN).astype(jnp.bfloat16)
        mixed = lax.psum_scatter(y_part, 'ty', scatter_dimension=0, tiled=True)
        y_out = to_width(row_call(finish_y_kernel, tx_size, x_own, mixed, bias_out.reshape(1, -1)))

        d_gelu = dot(cot_group, w_back[head:], NT).astype(jnp.bfloat16)
        (d_pre,) = gelu_pullback(d_gelu)
        d_ctx = dot(cot_group, w_back[:head], NT).astype(jnp.bfloat16)
        d_qkv_seq, d_b_qkv = attn_bwd(qkv_seq, d_ctx.reshape(n_seq, seq_len, head))
        d_qkv = d_qkv_seq.reshape(-1, qkv_width)
        d_b_up = d_pre.astype(jnp.float32).sum(0)
        d_h_mlp = dot(d_pre, wu, NT).astype(jnp.bfloat16).astype(jnp.float32)
        d_h_attn = dot(d_qkv, wq, NT).astype(jnp.bfloat16).astype(jnp.float32)
        a6_part = (d_h_attn * gain_attn + d_h_mlp * gain_mlp).astype(jnp.bfloat16)
        value_a6 = lax.psum_scatter(a6_part, 'ty', scatter_dimension=0, tiled=True)
        dx_act = to_width(row_call(finish_dx_kernel, tx_size, x_own, value_a6, cot_own))

        d_ln = jnp.stack([(d_h_attn * x_hat).sum(0), d_h_attn.sum(0), (d_h_mlp * x_hat).sum(0), d_h_mlp.sum(0)])
        d_ln = small_sum(d_ln, 'ty', ty_size).reshape(4, tx_size, d_local)
        d_ln = d_ln[:, 0] + sum(shift(d_ln[:, r], -r) for r in range(1, tx_size))
        d_bias = small_sum(jnp.concatenate([d_b_qkv.sum((0, 1)), d_b_up])[None], 'tx', tx_size)[0]
        d_b_out = cot_out.astype(jnp.float32).sum((0, 1))

        cols = lambda act, r: act[:, r * d_local:(r + 1) * d_local]
        add_back = ring_scatter(lambda r, low, high: dot(inner[:, low:high], cols(cot_group, r), TN), inner.shape[1])
        add_up = ring_scatter(lambda r, low, high: dot(cols(h_mlp, r)[:, low:high], d_pre, TN), d_local)
        add_qkv = ring_scatter(lambda r, low, high: dot(cols(h_attn, r)[:, low:high], d_qkv, TN), d_local)
        d_w_dense = add_back(dot(context, cols(cot_group, 0), TN), 0, head)
        d_w_down = add_back(dot(gelu_out, cols(cot_group, 0), TN), head, inner.shape[1])
        d_w_up = add_up(dot(cols(h_mlp, 0), d_pre, TN), 0, d_local)
        d_w_qkv = add_qkv(dot(cols(h_attn, 0), d_qkv, TN), 0, d_local)
        return (y_out, dx_act, d_ln[0], d_ln[1], d_ln[2], d_ln[3], d_w_qkv.reshape(w_qkv.shape), d_bias[:qkv_width].reshape(b_qkv.shape), d_w_dense, d_b_out, d_w_up, d_bias[qkv_width:], d_w_down, d_b_out)

    return jax.shard_map(body, mesh=mesh, in_specs=in_specs, out_specs=out_specs, check_vma=False)
```

```python
import functools
import jax
import jax.numpy as jnp
from jax import lax
from jax.experimental import pallas as pl
from jax.experimental.pallas import tpu as pltpu
from jax.sharding import PartitionSpec as P


LN_EPS = 1e-5
ROPE_BASE = 10000.0
ROTARY_DIVISOR = 4
LANES = 128
Q_ROWS = 256
LN_ROWS = 64
TILE = 256
SQRT_HALF = 0.5 ** 0.5
INV_SQRT_2PI = 0.3989422804014327

NT = (((1,), (1,)), ((), ()))
TN = (((0,), (0,)), ((), ()))
NN = (((1,), (0,)), ((), ()))


def dot(a, b, dims):
    return lax.dot_general(a, b, dims, preferred_element_type=jnp.float32)


def rotary_tables(seq_len, rot_dim):
    half = rot_dim // 2
    lane = jnp.arange(LANES)
    freq_index = jnp.where(lane < half, lane, lane - half)
    inv_freq = ROPE_BASE ** (-(2 * freq_index).astype(jnp.float32) / rot_dim)
    angles = jnp.arange(seq_len, dtype=jnp.float32)[:, None] * inv_freq[None, :]
    inside = (lane < rot_dim)[None, :]
    cos_tab = jnp.where(inside, jnp.cos(angles), 1.0)
    sin = jnp.where(inside, jnp.sin(angles), 0.0)
    first = (lane < half)[None, :]
    return cos_tab, jnp.where(first, -sin, 0.0), jnp.where(first, 0.0, sin)


def rotate(part, cos_tab, sin_lo, sin_hi, half, sign):
    head = part[:, :LANES]
    forward = pltpu.roll(head, half, 1)
    backward = pltpu.roll(head, LANES - half, 1)
    mixed = head * cos_tab + sign * (backward * sin_lo + forward * sin_hi)
    return jnp.concatenate([mixed, part[:, LANES:]], axis=1)


def causal_probs(q_rows, keys, row_start, scale):
    scores = dot(q_rows, keys, NT) * scale
    rows = row_start + lax.broadcasted_iota(jnp.int32, scores.shape, 0)
    cols = lax.broadcasted_iota(jnp.int32, scores.shape, 1)
    scores = jnp.where(rows >= cols, scores, -1e30)
    exps = jnp.exp(scores - jnp.max(scores, axis=1, keepdims=True))
    return exps * (1.0 / jnp.sum(exps, axis=1, keepdims=True))


def attn_fwd_kernel(qkv_ref, cos_ref, lo_ref, hi_ref, ctx_ref, q_ref, k_ref, *, half, scale, span):
    seq_len, width = ctx_ref.shape[1:]

    @pl.loop(0, seq_len // Q_ROWS)
    def _(step):
        rows = pl.ds(pl.multiple_of(step * Q_ROWS, Q_ROWS), Q_ROWS)
        for out, col in ((q_ref, 0), (k_ref, width)):
            part = qkv_ref[0, rows, col:col + width].astype(jnp.float32)
            out[rows, :] = rotate(part, cos_ref[rows, :], lo_ref[rows, :], hi_ref[rows, :], half, 1.0).astype(jnp.bfloat16)

    for end in range(span, seq_len + 1, span):
        @pl.loop(0, span // Q_ROWS)
        def _(step, end=end):
            start = pl.multiple_of(end - span + step * Q_ROWS, Q_ROWS)
            rows = pl.ds(start, Q_ROWS)
            probs = causal_probs(q_ref[rows, :], k_ref[:end, :], start, scale).astype(jnp.bfloat16)
            ctx_ref[0, rows, :] = dot(probs, qkv_ref[0, :end, 2 * width:], NN).astype(jnp.bfloat16)


def attn_bwd_kernel(qkv_ref, dctx_ref, cos_ref, lo_ref, hi_ref, dqkv_ref, db_ref, q_ref, k_ref, dk_ref, dv_ref, *, half, scale, span):
    seq_len, width = dctx_ref.shape[1:]

    @pl.loop(0, seq_len // Q_ROWS)
    def _(step):
        rows = pl.ds(pl.multiple_of(step * Q_ROWS, Q_ROWS), Q_ROWS)
        for out, col in ((q_ref, 0), (k_ref, width)):
            part = qkv_ref[0, rows, col:col + width].astype(jnp.float32)
            out[rows, :] = rotate(part, cos_ref[rows, :], lo_ref[rows, :], hi_ref[rows, :], half, 1.0).astype(jnp.bfloat16)
        dk_ref[rows, :] = jnp.zeros((Q_ROWS, width), jnp.float32)
        dv_ref[rows, :] = jnp.zeros((Q_ROWS, width), jnp.float32)

    db_ref[...] = jnp.zeros(db_ref.shape, jnp.float32)

    def store(rows, col, grad_rot, turn):
        grad = grad_rot.astype(jnp.bfloat16)
        if turn:
            wide = grad.astype(jnp.float32)
            grad = rotate(wide, cos_ref[rows, :], lo_ref[rows, :], hi_ref[rows, :], half, -1.0).astype(jnp.bfloat16)
        dqkv_ref[0, rows, col:col + width] = grad
        db_ref[0, :, col:col + width] += jnp.sum(grad.astype(jnp.float32), axis=0, keepdims=True)

    for end in range(span, seq_len + 1, span):
        @pl.loop(0, span // Q_ROWS)
        def _(step, end=end):
            start = pl.multiple_of(end - span + step * Q_ROWS, Q_ROWS)
            rows = pl.ds(start, Q_ROWS)
            q_rows = q_ref[rows, :]
            dctx = dctx_ref[0, rows, :]
            probs = causal_probs(q_rows, k_ref[:end, :], start, scale)
            dprobs = dot(dctx, qkv_ref[0, :end, 2 * width:], NT).astype(jnp.bfloat16).astype(jnp.float32)
            dv_ref[:end, :] += dot(probs.astype(jnp.bfloat16), dctx, TN)
            inner = jnp.sum(probs * dprobs, axis=1, keepdims=True)
            dscores = (probs * (dprobs - inner) * scale).astype(jnp.bfloat16)
            dk_ref[:end, :] += dot(dscores, q_rows, TN)
            store(rows, 0, dot(dscores, k_ref[:end, :], NN), True)

    @pl.loop(0, seq_len // Q_ROWS)
    def _(step):
        rows = pl.ds(pl.multiple_of(step * Q_ROWS, Q_ROWS), Q_ROWS)
        store(rows, width, dk_ref[rows, :], True)
        store(rows, 2 * width, dv_ref[rows, :], False)


def attention_calls(seq_len, width, index):
    n_seq = 1
    half = width // ROTARY_DIVISOR // 2
    scale = width ** -0.5
    span = 512 if seq_len % 512 == 0 else seq_len
    tables = rotary_tables(seq_len, 2 * half)
    seq_spec = lambda cols, first=0: pl.BlockSpec((1, seq_len, cols), lambda s: (s + first, 0, 0))
    tab_spec = pl.BlockSpec((seq_len, LANES), lambda s: (0, 0))
    rot_scratch = pltpu.VMEM((seq_len, width), jnp.bfloat16)
    acc_scratch = pltpu.VMEM((seq_len, width), jnp.float32)
    pairs = n_seq * seq_len * seq_len // 2
    params = pltpu.CompilerParams(dimension_semantics=("arbitrary",), vmem_limit_bytes=56 * 1024 * 1024)
    forward = pl.pallas_call(
        functools.partial(attn_fwd_kernel, half=half, scale=scale, span=span),
        grid=(n_seq,),
        in_specs=[seq_spec(3 * width, index), tab_spec, tab_spec, tab_spec],
        out_specs=seq_spec(width),
        out_shape=jax.ShapeDtypeStruct((n_seq, seq_len, width), jnp.bfloat16),
        scratch_shapes=[rot_scratch, rot_scratch],
        compiler_params=params,
        name="attn_fwd",
        cost_estimate=pl.CostEstimate(flops=8 * pairs * width, bytes_accessed=8 * n_seq * seq_len * width, transcendentals=pairs),
    )
    backward = pl.pallas_call(
        functools.partial(attn_bwd_kernel, half=half, scale=scale, span=span),
        grid=(n_seq,),
        in_specs=[seq_spec(3 * width, index), seq_spec(width, index), tab_spec, tab_spec, tab_spec],
        out_specs=[seq_spec(3 * width), pl.BlockSpec((1, 1, 3 * width), lambda s: (s, 0, 0))],
        out_shape=[jax.ShapeDtypeStruct((n_seq, seq_len, 3 * width), jnp.bfloat16), jax.ShapeDtypeStruct((n_seq, 1, 3 * width), jnp.float32)],
        scratch_shapes=[rot_scratch, rot_scratch, acc_scratch, acc_scratch],
        compiler_params=params,
        name="attn_bwd",
        cost_estimate=pl.CostEstimate(flops=20 * pairs * width, bytes_accessed=14 * n_seq * seq_len * width, transcendentals=pairs),
    )
    return (lambda qkv: forward(qkv, *tables)), (lambda qkv, dctx: backward(qkv, dctx, *tables))


def place_kernel(row_ref, full_ref, *rest, chunk, n_seq):
    out_ref, held_ref, in_sems, out_sems = rest[-4:]
    groups = full_ref.shape[0]
    fetch = [pltpu.make_async_copy(full_ref.at[lax.rem(row_ref[0] + groups - t, groups)], held_ref.at[t], in_sems.at[t]) for t in range(groups)]
    store = [pltpu.make_async_copy(held_ref.at[t], out_ref.at[t * n_seq + chunk], out_sems.at[t]) for t in range(groups)]
    for copy in fetch:
        copy.start()
    for t in range(groups):
        fetch[t].wait()
        store[t].start()
    for copy in store:
        copy.wait()


def place_groups(fulls, row):
    groups, tokens, width = fulls[0].shape
    n_seq = len(fulls)
    out = None
    for chunk, full in enumerate(fulls):
        operands = (row.reshape(1), full) + (() if out is None else (out,))
        any_spec = pl.BlockSpec(memory_space=pl.ANY)
        out = pl.pallas_call(
            functools.partial(place_kernel, chunk=chunk, n_seq=n_seq),
            in_specs=[pl.BlockSpec(memory_space=pltpu.SMEM)] + [any_spec] * (len(operands) - 1),
            out_specs=any_spec,
            out_shape=jax.ShapeDtypeStruct((groups * n_seq, tokens, width), full.dtype),
            scratch_shapes=[pltpu.VMEM(full.shape, full.dtype), pltpu.SemaphoreType.DMA((groups,)), pltpu.SemaphoreType.DMA((groups,))],
            input_output_aliases={} if chunk == 0 else {2: 0},
            name="place_groups",
            cost_estimate=pl.CostEstimate(flops=4 * full.size, bytes_accessed=4 * full.size, transcendentals=0),
        )(*operands)
    return out


def split_width(value, out_refs):
    width = out_refs[0].shape[1]
    for index, out_ref in enumerate(out_refs):
        out_ref[...] = value[:, index * width:(index + 1) * width].astype(out_ref.dtype)


def finish_y_kernel(x_ref, mixed_ref, bias_ref, *out_refs):
    split_width(x_ref[...].astype(jnp.float32) + mixed_ref[...].astype(jnp.float32) + bias_ref[...], out_refs)


def normalize(act):
    act = act.astype(jnp.float32)
    mean = act.mean(-1, keepdims=True)
    inv_std = lax.rsqrt((act * act).mean(-1, keepdims=True) - mean * mean + LN_EPS)
    return (act - mean) * inv_std, inv_std


def finish_dx_kernel(x_ref, a6_ref, cot_ref, *out_refs):
    x_hat, inv_std = normalize(x_ref[...])
    value_a6 = a6_ref[...].astype(jnp.float32)
    mean_a6 = value_a6.mean(-1, keepdims=True)
    mean_a6x = (value_a6 * x_hat).mean(-1, keepdims=True)
    split_width(cot_ref[...].astype(jnp.float32) + inv_std * (value_a6 - mean_a6 - x_hat * mean_a6x), out_refs)


def row_call(kernel, parts, *operands):
    n_rows, width = operands[0].shape
    rows = 128 if n_rows % 128 == 0 else n_rows
    specs = [pl.BlockSpec((rows, width), lambda s: (s, 0)) if op.shape[0] == n_rows else pl.BlockSpec(op.shape, lambda s: (0, 0)) for op in operands]
    return pl.pallas_call(
        kernel,
        grid=(n_rows // rows,),
        in_specs=specs,
        out_specs=[pl.BlockSpec((rows, width // parts), lambda s: (s, 0))] * parts,
        out_shape=[jax.ShapeDtypeStruct((n_rows, width // parts), jnp.bfloat16)] * parts,
        cost_estimate=pl.CostEstimate(flops=16 * n_rows * width, bytes_accessed=8 * n_rows * width, transcendentals=0),
    )(*operands)


def sublane_sum(value):
    return value.reshape(value.shape[0] // 8, 8, value.shape[1]).sum(0)


def front_kernel(x_ref, small_ref, w_ref, b_qkv_ref, b_up_ref, h_attn_ref, h_mlp_ref, qkv_ref, pre_ref, gelu_ref):
    rows = x_ref.shape[0]

    @pl.loop(0, rows // LN_ROWS)
    def _(step):
        at = pl.ds(pl.multiple_of(step * LN_ROWS, LN_ROWS), LN_ROWS)
        x_hat, _ = normalize(x_ref[at, :])
        h_attn_ref[at, :] = (x_hat * small_ref[0:1, :] + small_ref[1:2, :]).astype(jnp.bfloat16)
        h_mlp_ref[at, :] = (x_hat * small_ref[2:3, :] + small_ref[3:4, :]).astype(jnp.bfloat16)

    qkv_width = qkv_ref.shape[1]
    for low in range(0, qkv_width, TILE):
        acc = dot(h_attn_ref[...], w_ref[:, low:low + TILE], NN) + b_qkv_ref[:, low:low + TILE]
        qkv_ref[:, low:low + TILE] = acc.astype(jnp.bfloat16)
    for low in range(0, pre_ref.shape[1], TILE):
        acc = dot(h_mlp_ref[...], w_ref[:, qkv_width + low:qkv_width + low + TILE], NN) + b_up_ref[:, low:low + TILE]
        pre = acc.astype(jnp.bfloat16)
        pre_ref[:, low:low + TILE] = pre
        wide = pre.astype(jnp.float32)
        gelu_ref[:, low:low + TILE] = (0.5 * wide * (1.0 + lax.erf(wide * SQRT_HALF))).astype(jnp.bfloat16)


def y_kernel(ctx_ref, gelu_ref, *refs):
    w_refs, y_ref = refs[:-1], refs[-1]
    head = ctx_ref.shape[1]
    for index, w_ref in enumerate(w_refs):
        width = w_ref.shape[1]
        acc = dot(ctx_ref[...], w_ref[:head, :], NN) + dot(gelu_ref[...], w_ref[head:, :], NN)
        y_ref[:, index * width:(index + 1) * width] = acc.astype(jnp.bfloat16)


def d_pre_kernel(cot_ref, pre_ref, *refs):
    w_refs, (d_ctx_ref, d_pre_ref, d_bias_ref) = refs[:-3], refs[-3:]
    width = w_refs[0].shape[1]

    def back(low, high):
        return sum(dot(cot_ref[:, r * width:(r + 1) * width], w_ref[low:high, :], NT) for r, w_ref in enumerate(w_refs)).astype(jnp.bfloat16)

    head = d_ctx_ref.shape[1]

    @pl.when(pl.program_id(0) == 0)
    def _():
        d_bias_ref[...] = jnp.zeros(d_bias_ref.shape, jnp.float32)

    d_ctx_ref[...] = back(0, head)
    for low in range(0, d_pre_ref.shape[1], TILE):
        at = slice(low, low + TILE)
        d_gelu = back(head + low, head + low + TILE).astype(jnp.float32)
        pre = pre_ref[:, at].astype(jnp.float32)
        slope = 0.5 * (1.0 + lax.erf(pre * SQRT_HALF)) + pre * (jnp.exp(-0.5 * pre * pre) * INV_SQRT_2PI)
        d_pre = (d_gelu * slope).astype(jnp.bfloat16)
        d_pre_ref[:, at] = d_pre
        d_bias_ref[:, at] += sublane_sum(d_pre.astype(jnp.float32))


def d_h_kernel(d_qkv_ref, d_pre_ref, x_ref, small_ref, w_ref, a6_ref, sums_ref):
    qkv_width = d_qkv_ref.shape[1]

    @pl.when(pl.program_id(0) == 0)
    def _():
        sums_ref[...] = jnp.zeros(sums_ref.shape, jnp.float32)

    x_float = x_ref[...].astype(jnp.float32)
    mean = x_float.mean(-1, keepdims=True)
    inv_std = lax.rsqrt((x_float * x_float).mean(-1, keepdims=True) - mean * mean + LN_EPS)
    for low in range(0, a6_ref.shape[1], TILE):
        at = slice(low, low + TILE)
        d_attn = dot(d_qkv_ref[...], w_ref[at, :qkv_width], NT).astype(jnp.bfloat16).astype(jnp.float32)
        d_mlp = dot(d_pre_ref[...], w_ref[at, qkv_width:], NT).astype(jnp.bfloat16).astype(jnp.float32)
        a6_ref[:, at] = (d_attn * small_ref[0:1, at] + d_mlp * small_ref[2:3, at]).astype(jnp.bfloat16)
        x_hat = (x_ref[:, at].astype(jnp.float32) - mean) * inv_std
        sums_ref[0, :, at] += sublane_sum(d_attn * x_hat)
        sums_ref[1, :, at] += sublane_sum(d_attn)
        sums_ref[2, :, at] += sublane_sum(d_mlp * x_hat)
        sums_ref[3, :, at] += sublane_sum(d_mlp)


def tile_call(kernel, tiled, whole, outs, row_range, flops):
    start, count = row_range
    rows = next(r for r in (512, 256, 128, 64, count) if count % r == 0)
    first = start // rows
    in_specs = [pl.BlockSpec((rows, op.shape[1]), lambda s, f=(first if op.shape[0] != count else 0): (s + f, 0)) for op in tiled]
    in_specs += [pl.BlockSpec(op.shape, lambda s, n=op.ndim: (0,) * n) for op in whole]
    out_specs, out_shapes = [], []
    for form, dtype in outs:
        if isinstance(form, int):
            out_specs.append(pl.BlockSpec((rows, form), lambda s: (s, 0)))
            out_shapes.append(jax.ShapeDtypeStruct((count, form), dtype))
        else:
            out_specs.append(pl.BlockSpec(form, lambda s, n=len(form): (0,) * n))
            out_shapes.append(jax.ShapeDtypeStruct(form, dtype))
    moved = sum(op.size * 2 * count // op.shape[0] for op in tiled) + sum(op.size * 2 for op in whole) + sum(2 * shape.size for shape in out_shapes)
    return pl.pallas_call(
        kernel,
        grid=(count // rows,),
        in_specs=in_specs,
        out_specs=out_specs,
        out_shape=out_shapes,
        compiler_params=pltpu.CompilerParams(dimension_semantics=("arbitrary",), vmem_limit_bytes=60 * 1024 * 1024),
        cost_estimate=pl.CostEstimate(flops=flops, bytes_accessed=moved, transcendentals=0),
    )(*tiled, *whole)


def solution(mesh):
    tx_size, ty_size = mesh.shape['tx'], mesh.shape['ty']
    act_spec = P('dp', None, 'tx')
    width_spec = P('tx')
    in_specs = (act_spec, act_spec, width_spec, width_spec, width_spec, width_spec, P('tx', 'ty', None), P('ty', None), P('ty', 'tx'), width_spec, P('tx', 'ty'), P('ty'), P('ty', 'tx'), width_spec)
    width_out = P(('dp', 'tx'))
    out_specs = (act_spec, act_spec, width_out, width_out, width_out, width_out, P(('dp', 'tx'), 'ty', None), P(('dp', 'ty'), None), P(('dp', 'ty'), 'tx'), width_out, P(('dp', 'tx'), 'ty'), P(('dp', 'ty')), P(('dp', 'ty'), 'tx'), width_out)
    antipode = tx_size // 2

    def shift(value, hops):
        return lax.ppermute(value, 'tx', [(s, (s - hops) % tx_size) for s in range(tx_size)])

    def small_sum(value, axis, size):
        step = 1
        while step < size:
            value = value + lax.ppermute(value, axis, [(s, s ^ step) for s in range(size)])
            step *= 2
        return value

    def ring_gather(block):
        blocks = {0: block}
        for hops in range(1, antipode):
            blocks[hops] = shift(blocks[hops - 1], 1)
            blocks[tx_size - hops] = shift(blocks[(tx_size - hops + 1) % tx_size], -1)
        rows = block.shape[0] // 2
        blocks[antipode] = jnp.concatenate([shift(blocks[antipode - 1][:rows], 1), shift(blocks[antipode + 1][rows:], -1)], axis=0)
        return [blocks[r] for r in range(tx_size)]

    def ring_scatter(make_part, rows):
        half = rows // 2
        far_low = make_part(antipode, 0, half).astype(jnp.bfloat16)
        far_high = make_part(antipode, half, rows).astype(jnp.bfloat16)
        moving_up, moving_down = shift(far_low, -1), shift(far_high, 1)
        moving_up = jnp.pad(moving_up, ((0, rows - half), (0, 0)))
        moving_down = jnp.pad(moving_down, ((half, 0), (0, 0)))
        for hops in range(antipode - 1, 0, -1):
            up = make_part(hops, 0, rows) + moving_up.astype(jnp.float32)
            down = make_part(tx_size - hops, 0, rows) + moving_down.astype(jnp.float32)
            up, down = up.astype(jnp.bfloat16), down.astype(jnp.bfloat16)
            moving_up, moving_down = shift(up, -1), shift(down, 1)
        return lambda own, low, high: own + moving_up[low:high].astype(jnp.float32) + moving_down[low:high].astype(jnp.float32)

    def body(x_act, cot_out, ln1_gain, ln1_bias, ln2_gain, ln2_bias, w_qkv, b_qkv, w_dense, b_dense, w_up, b_up, w_down, b_down):
        batch, seq_len, d_local = x_act.shape
        n_seq = batch // tx_size
        own = seq_len // ty_size
        row, col = lax.axis_index('tx'), lax.axis_index('ty')
        qkv_width = w_qkv.shape[1] * w_qkv.shape[2]
        head = qkv_width // 3
        chunks = range(n_seq)
        attention = [attention_calls(seq_len, head, s) for s in chunks]

        def to_tokens(act):
            parts = act.reshape(tx_size, n_seq, ty_size, own, d_local)
            pick = lambda index: lax.dynamic_slice(parts, (index, 0, col, 0, 0), (1, n_seq, 1, own, d_local)).reshape(n_seq, own, d_local)
            blocks = [pick(row)] + [shift(pick((row - r) % tx_size), r) for r in range(1, tx_size)]
            return jnp.concatenate(blocks, axis=2)

        def to_width(parts):
            blocks = [parts[0]] + [shift(parts[r], -r) for r in range(1, tx_size)]
            return lax.all_gather(jnp.stack(blocks), 'ty', axis=1, tiled=True)

        line = lax.broadcasted_iota(jnp.int32, (8, d_local), 0)
        small = jnp.zeros((8, d_local), jnp.bfloat16)
        for index, vector in enumerate((ln1_gain, ln1_bias, ln2_gain, ln2_bias, b_dense, b_down)):
            small = jnp.where(line == index, vector[None, :], small)
        small = [small] + [shift(small, r) for r in range(1, tx_size)]
        small = jnp.concatenate(small, axis=1).astype(jnp.float32)
        bias_out = small[4] + small[5]
        x_own = to_tokens(x_act)
        cot_own = to_tokens(cot_out)
        x_group = lax.all_gather(x_own, 'ty', axis=1, tiled=True)
        cot_group = lax.all_gather(cot_own, 'ty', axis=1, tiled=True)
        x_group, cot_group = x_group.reshape(n_seq * seq_len, -1), cot_group.reshape(n_seq * seq_len, -1)
        w_in = jnp.concatenate([w_qkv.reshape(d_local, qkv_width), w_up], axis=1)
        w_in = ring_gather(w_in)
        w_in = jnp.concatenate(w_in, axis=0)
        w_back = ring_gather(jnp.concatenate([w_dense, w_down], axis=0))
        back_size = tx_size * w_back[0].size

        n_tok, d_model = x_group.shape
        ff_width = w_up.shape[1]
        h_attn, h_mlp, qkv_act, pre_act, gelu_out = tile_call(
            front_kernel, [x_group], [small, w_in, b_qkv.reshape(1, -1).astype(jnp.float32), b_up.reshape(1, -1).astype(jnp.float32)],
            [(d_model, jnp.bfloat16), (d_model, jnp.bfloat16), (qkv_width, jnp.bfloat16), (ff_width, jnp.bfloat16), (ff_width, jnp.bfloat16)],
            (0, n_tok), 2 * n_tok * w_in.size)
        qkv_seq = qkv_act.reshape(n_seq, seq_len, qkv_width)
        context, y_full = [], []
        for s in chunks:
            context.append(attention[s][0](qkv_seq).reshape(seq_len, head))
            (y_part,) = tile_call(y_kernel, [context[s], gelu_out], w_back, [(d_model, jnp.bfloat16)], (s * seq_len, seq_len), 2 * seq_len * back_size)
            mixed = lax.psum_scatter(y_part, 'ty', scatter_dimension=0, tiled=True)
            y_full.append(to_width(row_call(finish_y_kernel, tx_size, x_own[s], mixed, bias_out.reshape(1, -1))))
        y_out = place_groups(y_full, row)
        context = jnp.concatenate(context, axis=0)

        d_ctx, d_pre, d_b_up = tile_call(
            d_pre_kernel, [cot_group, pre_act], w_back,
            [(head, jnp.bfloat16), (ff_width, jnp.bfloat16), ((8, ff_width), jnp.float32)], (0, n_tok), 2 * n_tok * back_size)
        d_ctx, d_b_up = d_ctx.reshape(n_seq, seq_len, head), d_b_up.sum(0)
        d_qkv, d_b_qkv, d_ln, dx_full = [], [], [], []
        for s in chunks:
            d_qkv_seq, d_b_seq = attention[s][1](qkv_seq, d_ctx)
            d_qkv.append(d_qkv_seq.reshape(seq_len, qkv_width))
            d_b_qkv.append(d_b_seq.reshape(-1))
            a6_part, sums = tile_call(
                d_h_kernel, [d_qkv[s], d_pre, x_group], [small, w_in],
                [(d_model, jnp.bfloat16), ((4, 8, d_model), jnp.float32)], (s * seq_len, seq_len), 2 * seq_len * w_in.size)
            d_ln.append(sums)
            value_a6 = lax.psum_scatter(a6_part, 'ty', scatter_dimension=0, tiled=True)
            dx_full.append(to_width(row_call(finish_dx_kernel, tx_size, x_own[s], value_a6, cot_own[s])))
        dx_act = place_groups(dx_full, row)
        d_qkv = jnp.concatenate(d_qkv, axis=0)

        d_ln = small_sum(sum(d_ln).sum(1), 'ty', ty_size).reshape(4, tx_size, d_local)
        d_ln = d_ln[:, 0] + sum(shift(d_ln[:, r], -r) for r in range(1, tx_size))
        d_bias = small_sum(jnp.concatenate([sum(d_b_qkv), d_b_up])[None], 'tx', tx_size)[0]
        d_b_out = cot_out.astype(jnp.float32).sum((0, 1))

        cols = lambda act, r: act[:, r * d_local:(r + 1) * d_local]
        inner = jnp.concatenate([context, gelu_out], axis=1)
        add_back = ring_scatter(lambda r, low, high: dot(inner[:, low:high], cols(cot_group, r), TN), inner.shape[1])
        add_up = ring_scatter(lambda r, low, high: dot(cols(h_mlp, r)[:, low:high], d_pre, TN), d_local)
        add_qkv = ring_scatter(lambda r, low, high: dot(cols(h_attn, r)[:, low:high], d_qkv, TN), d_local)
        d_w_dense = add_back(dot(context, cols(cot_group, 0), TN), 0, head)
        d_w_down = add_back(dot(gelu_out, cols(cot_group, 0), TN), head, inner.shape[1])
        d_w_up = add_up(dot(cols(h_mlp, 0), d_pre, TN), 0, d_local)
        d_w_qkv = add_qkv(dot(cols(h_attn, 0), d_qkv, TN), 0, d_local)
        return (y_out, dx_act, d_ln[0], d_ln[1], d_ln[2], d_ln[3], d_w_qkv.reshape(w_qkv.shape), d_bias[:qkv_width].reshape(b_qkv.shape), d_w_dense, d_b_out, d_w_up, d_bias[qkv_width:], d_w_down, d_b_out)

    return jax.shard_map(body, mesh=mesh, in_specs=in_specs, out_specs=out_specs, check_vma=False)
```

```python
import functools
import jax
import jax.numpy as jnp
from jax import lax
from jax.experimental import pallas as pl
from jax.experimental.pallas import tpu as pltpu
from jax.sharding import PartitionSpec as P


LN_EPS = 1e-5
ROPE_BASE = 10000.0
ROTARY_DIVISOR = 4
LANES = 128
Q_ROWS = 256
LN_ROWS = 64
MIB = 1024 * 1024
TILE = 256
SQRT_HALF = 0.5 ** 0.5
INV_SQRT_2PI = 0.3989422804014327

NT = (((1,), (1,)), ((), ()))
TN = (((0,), (0,)), ((), ()))
NN = (((1,), (0,)), ((), ()))


def dot(a, b, dims):
    return lax.dot_general(a, b, dims, preferred_element_type=jnp.float32)


def rotary_tables(seq_len, rot_dim):
    half = rot_dim // 2
    lane = jnp.arange(LANES)
    freq_index = jnp.where(lane < half, lane, lane - half)
    inv_freq = ROPE_BASE ** (-(2 * freq_index).astype(jnp.float32) / rot_dim)
    angles = jnp.arange(seq_len, dtype=jnp.float32)[:, None] * inv_freq[None, :]
    inside = (lane < rot_dim)[None, :]
    cos_tab = jnp.where(inside, jnp.cos(angles), 1.0)
    sin = jnp.where(inside, jnp.sin(angles), 0.0)
    first = (lane < half)[None, :]
    return cos_tab, jnp.where(first, -sin, 0.0), jnp.where(first, 0.0, sin)


def rotate(part, cos_tab, sin_lo, sin_hi, half, sign):
    head = part[:, :LANES]
    forward = pltpu.roll(head, half, 1)
    backward = pltpu.roll(head, LANES - half, 1)
    mixed = head * cos_tab + sign * (backward * sin_lo + forward * sin_hi)
    return jnp.concatenate([mixed, part[:, LANES:]], axis=1)


def causal_probs(q_rows, keys, row_start, scale):
    scores = dot(q_rows, keys, NT) * scale
    rows = row_start + lax.broadcasted_iota(jnp.int32, scores.shape, 0)
    cols = lax.broadcasted_iota(jnp.int32, scores.shape, 1)
    scores = jnp.where(rows >= cols, scores, -1e30)
    exps = jnp.exp(scores - jnp.max(scores, axis=1, keepdims=True))
    return exps * (1.0 / jnp.sum(exps, axis=1, keepdims=True))


def attn_fwd_kernel(qkv_ref, cos_ref, lo_ref, hi_ref, ctx_ref, q_ref, k_ref, *, half, scale, span):
    seq_len, width = ctx_ref.shape[1:]

    @pl.loop(0, seq_len // Q_ROWS)
    def _(step):
        rows = pl.ds(pl.multiple_of(step * Q_ROWS, Q_ROWS), Q_ROWS)
        for out, col in ((q_ref, 0), (k_ref, width)):
            part = qkv_ref[0, rows, col:col + width].astype(jnp.float32)
            out[rows, :] = rotate(part, cos_ref[rows, :], lo_ref[rows, :], hi_ref[rows, :], half, 1.0).astype(jnp.bfloat16)

    for end in range(span, seq_len + 1, span):
        @pl.loop(0, span // Q_ROWS)
        def _(step, end=end):
            start = pl.multiple_of(end - span + step * Q_ROWS, Q_ROWS)
            rows = pl.ds(start, Q_ROWS)
            probs = causal_probs(q_ref[rows, :], k_ref[:end, :], start, scale).astype(jnp.bfloat16)
            ctx_ref[0, rows, :] = dot(probs, qkv_ref[0, :end, 2 * width:], NN).astype(jnp.bfloat16)


def attn_bwd_kernel(qkv_ref, dctx_ref, cos_ref, lo_ref, hi_ref, dqkv_ref, db_ref, q_ref, k_ref, dk_ref, dv_ref, *, half, scale, span):
    seq_len, width = dctx_ref.shape[1:]

    @pl.loop(0, seq_len // Q_ROWS)
    def _(step):
        rows = pl.ds(pl.multiple_of(step * Q_ROWS, Q_ROWS), Q_ROWS)
        for out, col in ((q_ref, 0), (k_ref, width)):
            part = qkv_ref[0, rows, col:col + width].astype(jnp.float32)
            out[rows, :] = rotate(part, cos_ref[rows, :], lo_ref[rows, :], hi_ref[rows, :], half, 1.0).astype(jnp.bfloat16)
        dk_ref[rows, :] = jnp.zeros((Q_ROWS, width), jnp.float32)
        dv_ref[rows, :] = jnp.zeros((Q_ROWS, width), jnp.float32)

    db_ref[...] = jnp.zeros(db_ref.shape, jnp.float32)

    def store(rows, col, grad_rot, turn):
        grad = grad_rot.astype(jnp.bfloat16)
        if turn:
            wide = grad.astype(jnp.float32)
            grad = rotate(wide, cos_ref[rows, :], lo_ref[rows, :], hi_ref[rows, :], half, -1.0).astype(jnp.bfloat16)
        dqkv_ref[0, rows, col:col + width] = grad
        db_ref[0, :, col:col + width] += jnp.sum(grad.astype(jnp.float32), axis=0, keepdims=True)

    for end in range(span, seq_len + 1, span):
        @pl.loop(0, span // Q_ROWS)
        def _(step, end=end):
            start = pl.multiple_of(end - span + step * Q_ROWS, Q_ROWS)
            rows = pl.ds(start, Q_ROWS)
            q_rows = q_ref[rows, :]
            dctx = dctx_ref[0, rows, :]
            probs = causal_probs(q_rows, k_ref[:end, :], start, scale)
            dprobs = dot(dctx, qkv_ref[0, :end, 2 * width:], NT).astype(jnp.bfloat16).astype(jnp.float32)
            dv_ref[:end, :] += dot(probs.astype(jnp.bfloat16), dctx, TN)
            inner = jnp.sum(probs * dprobs, axis=1, keepdims=True)
            dscores = (probs * (dprobs - inner) * scale).astype(jnp.bfloat16)
            dk_ref[:end, :] += dot(dscores, q_rows, TN)
            store(rows, 0, dot(dscores, k_ref[:end, :], NN), True)

    @pl.loop(0, seq_len // Q_ROWS)
    def _(step):
        rows = pl.ds(pl.multiple_of(step * Q_ROWS, Q_ROWS), Q_ROWS)
        store(rows, width, dk_ref[rows, :], True)
        store(rows, 2 * width, dv_ref[rows, :], False)


def attention_calls(seq_len, width, index):
    n_seq = 1
    half = width // ROTARY_DIVISOR // 2
    scale = width ** -0.5
    span = 512 if seq_len % 512 == 0 else seq_len
    tables = rotary_tables(seq_len, 2 * half)
    seq_spec = lambda cols, first=0: pl.BlockSpec((1, seq_len, cols), lambda s: (s + first, 0, 0))
    tab_spec = pl.BlockSpec((seq_len, LANES), lambda s: (0, 0))
    rot_scratch = pltpu.VMEM((seq_len, width), jnp.bfloat16)
    acc_scratch = pltpu.VMEM((seq_len, width), jnp.float32)
    pairs = n_seq * seq_len * seq_len // 2
    params = pltpu.CompilerParams(dimension_semantics=("arbitrary",), vmem_limit_bytes=32 * MIB)
    forward = pl.pallas_call(
        functools.partial(attn_fwd_kernel, half=half, scale=scale, span=span),
        grid=(n_seq,),
        in_specs=[seq_spec(3 * width, index), tab_spec, tab_spec, tab_spec],
        out_specs=seq_spec(width),
        out_shape=jax.ShapeDtypeStruct((n_seq, seq_len, width), jnp.bfloat16),
        scratch_shapes=[rot_scratch, rot_scratch],
        compiler_params=params,
        name="attn_fwd",
        cost_estimate=pl.CostEstimate(flops=8 * pairs * width, bytes_accessed=8 * n_seq * seq_len * width, transcendentals=pairs),
    )
    backward = pl.pallas_call(
        functools.partial(attn_bwd_kernel, half=half, scale=scale, span=span),
        grid=(n_seq,),
        in_specs=[seq_spec(3 * width, index), seq_spec(width, index), tab_spec, tab_spec, tab_spec],
        out_specs=[seq_spec(3 * width), pl.BlockSpec((1, 1, 3 * width), lambda s: (s, 0, 0))],
        out_shape=[jax.ShapeDtypeStruct((n_seq, seq_len, 3 * width), jnp.bfloat16), jax.ShapeDtypeStruct((n_seq, 1, 3 * width), jnp.float32)],
        scratch_shapes=[rot_scratch, rot_scratch, acc_scratch, acc_scratch],
        compiler_params=params,
        name="attn_bwd",
        cost_estimate=pl.CostEstimate(flops=20 * pairs * width, bytes_accessed=14 * n_seq * seq_len * width, transcendentals=pairs),
    )
    return (lambda qkv: forward(qkv, *tables)), (lambda qkv, dctx: backward(qkv, dctx, *tables))


def place_kernel(row_ref, full_ref, *rest, chunk, n_seq):
    out_ref, held_ref, in_sems, out_sems = rest[-4:]
    groups = full_ref.shape[0]
    fetch = [pltpu.make_async_copy(full_ref.at[lax.rem(row_ref[0] + groups - t, groups)], held_ref.at[t], in_sems.at[t]) for t in range(groups)]
    store = [pltpu.make_async_copy(held_ref.at[t], out_ref.at[t * n_seq + chunk], out_sems.at[t]) for t in range(groups)]
    for copy in fetch:
        copy.start()
    for t in range(groups):
        fetch[t].wait()
        store[t].start()
    for copy in store:
        copy.wait()


def place_pieces_kernel(place_ref, *refs, chunk, n_seq):
    out_ref, held_ref, in_sems, out_sems = refs[-4:]
    groups, own, _ = refs[0].shape
    columns = held_ref.shape[0] // 2
    row, column, core = place_ref[0], place_ref[1], place_ref[2]
    fetch, store = [], []
    for index in range(2 * columns):
        source = 2 * lax.rem(column + index % columns, columns) + (core if index < columns else 1 - core)
        at = pl.ds(pl.multiple_of(source * own, own), own)
        fetch.append(pltpu.make_async_copy(refs[index], held_ref.at[index], in_sems.at[index]))
        for t in range(groups):
            piece = held_ref.at[index, lax.rem(row + groups - t, groups)]
            store.append(pltpu.make_async_copy(piece, out_ref.at[t * n_seq + chunk, at], out_sems.at[index]))
    for copy in fetch:
        copy.start()
    for index in range(2 * columns):
        fetch[index].wait()
        for copy in store[index * groups:(index + 1) * groups]:
            copy.start()
    for copy in store:
        copy.wait()


def place_call(kernel, place, operands, out, chunk, n_seq, tokens):
    groups, _, width = operands[0].shape
    operands = [place, *operands] + ([] if out is None else [out])
    any_spec = pl.BlockSpec(memory_space=pl.ANY)
    pieces = len(operands) - 1 - (out is not None)
    held = operands[1].shape if pieces == 1 else (pieces,) + operands[1].shape
    sems = pltpu.SemaphoreType.DMA((groups if pieces == 1 else pieces,))
    return pl.pallas_call(
        functools.partial(kernel, chunk=chunk, n_seq=n_seq),
        in_specs=[pl.BlockSpec(memory_space=pltpu.SMEM)] + [any_spec] * (len(operands) - 1),
        out_specs=any_spec,
        out_shape=jax.ShapeDtypeStruct((groups * n_seq, tokens, width), jnp.bfloat16),
        scratch_shapes=[pltpu.VMEM(held, jnp.bfloat16), sems, sems],
        input_output_aliases={} if out is None else {len(operands) - 1: 0},
        cost_estimate=pl.CostEstimate(flops=groups * tokens * width, bytes_accessed=4 * groups * tokens * width, transcendentals=0),
    )(*operands)


def split_width(value, out_refs):
    width = out_refs[0].shape[1]
    for index, out_ref in enumerate(out_refs):
        out_ref[...] = value[:, index * width:(index + 1) * width].astype(out_ref.dtype)


def finish_y_kernel(x_ref, mixed_ref, bias_ref, *out_refs):
    split_width(x_ref[...].astype(jnp.float32) + mixed_ref[...].astype(jnp.float32) + bias_ref[...], out_refs)


def normalize(act):
    act = act.astype(jnp.float32)
    mean = act.mean(-1, keepdims=True)
    inv_std = lax.rsqrt((act * act).mean(-1, keepdims=True) - mean * mean + LN_EPS)
    return (act - mean) * inv_std, inv_std


def finish_dx_kernel(x_ref, a6_ref, cot_ref, *out_refs):
    x_hat, inv_std = normalize(x_ref[...])
    value_a6 = a6_ref[...].astype(jnp.float32)
    mean_a6 = value_a6.mean(-1, keepdims=True)
    mean_a6x = (value_a6 * x_hat).mean(-1, keepdims=True)
    split_width(cot_ref[...].astype(jnp.float32) + inv_std * (value_a6 - mean_a6 - x_hat * mean_a6x), out_refs)


def row_call(kernel, parts, index, rows, *operands):
    width = operands[0].shape[1]
    specs = [pl.BlockSpec((min(rows, op.shape[0]), width), lambda s, i=(index if op.shape[0] > rows else 0): (i, 0)) for op in operands]
    return pl.pallas_call(
        kernel,
        grid=(1,),
        in_specs=specs,
        out_specs=[pl.BlockSpec((rows, width // parts), lambda s: (0, 0))] * parts,
        out_shape=[jax.ShapeDtypeStruct((rows, width // parts), jnp.bfloat16)] * parts,
        compiler_params=pltpu.CompilerParams(vmem_limit_bytes=16 * MIB),
        cost_estimate=pl.CostEstimate(flops=16 * rows * width, bytes_accessed=8 * rows * width, transcendentals=0),
    )(*operands)


def sublane_sum(value):
    return value.reshape(value.shape[0] // 8, 8, value.shape[1]).sum(0)


def front_kernel(x_ref, next_ref, small_ref, w_ref, b_qkv_ref, b_up_ref, h_attn_ref, h_mlp_ref, qkv_ref, pre_ref, gelu_ref, norm_ref):
    rows = x_ref.shape[0]
    step = pl.program_id(0)
    now = lax.rem(step, 2)

    def norm(from_ref, slot, at):
        x_hat, _ = normalize(from_ref[at, :])
        norm_ref[slot, 0, at, :] = (x_hat * small_ref[0:1, :] + small_ref[1:2, :]).astype(jnp.bfloat16)
        norm_ref[slot, 1, at, :] = (x_hat * small_ref[2:3, :] + small_ref[3:4, :]).astype(jnp.bfloat16)

    @pl.when(step == 0)
    def _():
        @pl.loop(0, rows // LN_ROWS)
        def _(part):
            norm(x_ref, 0, pl.ds(pl.multiple_of(part * LN_ROWS, LN_ROWS), LN_ROWS))

    qkv_width = qkv_ref.shape[1]
    tiles = [(0, low) for low in range(0, qkv_width, TILE)] + [(1, low) for low in range(0, pre_ref.shape[1], TILE)]
    ahead = -(-rows // (len(tiles) * 16)) * 16
    for index, (which, low) in enumerate(tiles):
        at = slice(low, low + TILE)
        if which == 0:
            qkv_ref[:, at] = (dot(norm_ref[now, 0], w_ref[:, at], NN) + b_qkv_ref[:, at]).astype(jnp.bfloat16)
        else:
            acc = dot(norm_ref[now, 1], w_ref[:, qkv_width + low:qkv_width + low + TILE], NN) + b_up_ref[:, at]
            pre = acc.astype(jnp.bfloat16)
            pre_ref[:, at] = pre
            wide = pre.astype(jnp.float32)
            gelu_ref[:, at] = (0.5 * wide * (1.0 + lax.erf(wide * SQRT_HALF))).astype(jnp.bfloat16)
        start, stop = index * ahead, min(rows, (index + 1) * ahead)
        if start < stop:
            rows_at = slice(start, stop)
            norm(next_ref, 1 - now, rows_at)
            h_attn_ref[rows_at, :] = norm_ref[now, 0, rows_at, :]
            h_mlp_ref[rows_at, :] = norm_ref[now, 1, rows_at, :]


def y_kernel(ctx_ref, gelu_ref, *refs):
    w_refs, y_ref = refs[:-1], refs[-1]
    head = ctx_ref.shape[1]
    for index, w_ref in enumerate(w_refs):
        width = w_ref.shape[1]
        acc = dot(ctx_ref[...], w_ref[:head, :], NN) + dot(gelu_ref[...], w_ref[head:, :], NN)
        y_ref[:, index * width:(index + 1) * width] = acc.astype(jnp.bfloat16)


def d_pre_kernel(cot_ref, pre_ref, *refs):
    w_refs, (d_ctx_ref, d_pre_ref, d_bias_ref) = refs[:-3], refs[-3:]
    width = w_refs[0].shape[1]

    def back(low, high):
        return sum(dot(cot_ref[:, r * width:(r + 1) * width], w_ref[low:high, :], NT) for r, w_ref in enumerate(w_refs)).astype(jnp.bfloat16)

    head = d_ctx_ref.shape[1]

    @pl.when(pl.program_id(0) == 0)
    def _():
        d_bias_ref[...] = jnp.zeros(d_bias_ref.shape, jnp.float32)

    d_ctx_ref[...] = back(0, head)
    for low in range(0, d_pre_ref.shape[1], TILE):
        at = slice(low, low + TILE)
        d_gelu = back(head + low, head + low + TILE).astype(jnp.float32)
        pre = pre_ref[:, at].astype(jnp.float32)
        slope = 0.5 * (1.0 + lax.erf(pre * SQRT_HALF)) + pre * (jnp.exp(-0.5 * pre * pre) * INV_SQRT_2PI)
        d_pre = (d_gelu * slope).astype(jnp.bfloat16)
        d_pre_ref[:, at] = d_pre
        d_bias_ref[:, at] += sublane_sum(d_pre.astype(jnp.float32))


def d_h_kernel(d_qkv_ref, d_pre_ref, x_ref, small_ref, w_ref, a6_ref, sums_ref):
    qkv_width = d_qkv_ref.shape[1]

    @pl.when(pl.program_id(0) == 0)
    def _():
        sums_ref[...] = jnp.zeros(sums_ref.shape, jnp.float32)

    x_float = x_ref[...].astype(jnp.float32)
    mean = x_float.mean(-1, keepdims=True)
    inv_std = lax.rsqrt((x_float * x_float).mean(-1, keepdims=True) - mean * mean + LN_EPS)
    for low in range(0, a6_ref.shape[1], TILE):
        at = slice(low, low + TILE)
        d_attn = dot(d_qkv_ref[...], w_ref[at, :qkv_width], NT).astype(jnp.bfloat16).astype(jnp.float32)
        d_mlp = dot(d_pre_ref[...], w_ref[at, qkv_width:], NT).astype(jnp.bfloat16).astype(jnp.float32)
        a6_ref[:, at] = (d_attn * small_ref[0:1, at] + d_mlp * small_ref[2:3, at]).astype(jnp.bfloat16)
        x_hat = (x_ref[:, at].astype(jnp.float32) - mean) * inv_std
        sums_ref[0, :, at] += sublane_sum(d_attn * x_hat)
        sums_ref[1, :, at] += sublane_sum(d_attn)
        sums_ref[2, :, at] += sublane_sum(d_mlp * x_hat)
        sums_ref[3, :, at] += sublane_sum(d_mlp)


def tile_call(kernel, tiled, whole, outs, row_range, flops, limit, ahead=False):
    start, count = row_range
    rows = next(r for r in (512, 256, 128, 64, count) if count % r == 0)
    first = start // rows
    in_specs = [pl.BlockSpec((rows, op.shape[1]), lambda s, f=(first if op.shape[0] != count else 0): (s + f, 0)) for op in tiled]
    if ahead:
        in_specs.append(pl.BlockSpec((rows, tiled[0].shape[1]), lambda s: (jnp.minimum(s + 1, count // rows - 1), 0)))
        tiled = [*tiled, tiled[0]]
    in_specs += [pl.BlockSpec(op.shape, lambda s, n=op.ndim: (0,) * n, pipeline_mode=pl.Buffered(1)) for op in whole]
    out_specs, out_shapes = [], []
    for form, dtype in outs:
        if isinstance(form, int):
            out_specs.append(pl.BlockSpec((rows, form), lambda s: (s, 0)))
            out_shapes.append(jax.ShapeDtypeStruct((count, form), dtype))
        else:
            out_specs.append(pl.BlockSpec(form, lambda s, n=len(form): (0,) * n))
            out_shapes.append(jax.ShapeDtypeStruct(form, dtype))
    moved = sum(op.size * 2 * count // op.shape[0] for op in tiled) + sum(op.size * 2 for op in whole) + sum(2 * shape.size for shape in out_shapes)
    return pl.pallas_call(
        kernel,
        grid=(count // rows,),
        in_specs=in_specs,
        out_specs=out_specs,
        out_shape=out_shapes,
        compiler_params=pltpu.CompilerParams(dimension_semantics=("arbitrary",), vmem_limit_bytes=limit * MIB),
        scratch_shapes=[pltpu.VMEM((2, 2, rows, tiled[0].shape[1]), jnp.bfloat16)] if ahead else [],
        cost_estimate=pl.CostEstimate(flops=flops, bytes_accessed=moved, transcendentals=0),
    )(*tiled, *whole)


def solution(mesh):
    tx_size, ty_size = mesh.shape['tx'], mesh.shape['ty']
    act_spec = P('dp', None, 'tx')
    width_spec = P('tx')
    in_specs = (act_spec, act_spec, width_spec, width_spec, width_spec, width_spec, P('tx', 'ty', None), P('ty', None), P('ty', 'tx'), width_spec, P('tx', 'ty'), P('ty'), P('ty', 'tx'), width_spec)
    width_out = P(('dp', 'tx'))
    out_specs = (act_spec, act_spec, width_out, width_out, width_out, width_out, P(('dp', 'tx'), 'ty', None), P(('dp', 'ty'), None), P(('dp', 'ty'), 'tx'), width_out, P(('dp', 'tx'), 'ty'), P(('dp', 'ty')), P(('dp', 'ty'), 'tx'), width_out)
    antipode = tx_size // 2

    def shift(value, hops):
        return lax.ppermute(value, 'tx', [(s, (s - hops) % tx_size) for s in range(tx_size)])

    def small_sum(value, axis, size):
        step = 1
        while step < size:
            value = value + lax.ppermute(value, axis, [(s, s ^ step) for s in range(size)])
            step *= 2
        return value

    def along(value, hops):
        return lax.ppermute(value, 'ty', [(s, (s - 2 * hops) % ty_size) for s in range(ty_size)])

    def partner(value):
        return lax.ppermute(value, 'ty', [(s, s ^ 1) for s in range(ty_size)])

    def ring_gather(block, move, size):
        far = size // 2
        blocks = {0: block}
        for hops in range(1, far):
            blocks[hops] = move(blocks[hops - 1], 1)
            blocks[size - hops] = move(blocks[(size - hops + 1) % size], -1)
        half = block.shape[0] // 2
        blocks[far] = jnp.concatenate([move(blocks[far - 1][:half], 1), move(blocks[far + 1][half:], -1)], axis=0)
        return [blocks[r] for r in range(size)]

    def ring_scatter(make_part, rows):
        half = rows // 2
        far_low = make_part(antipode, 0, half).astype(jnp.bfloat16)
        far_high = make_part(antipode, half, rows).astype(jnp.bfloat16)
        moving_up, moving_down = shift(far_low, -1), shift(far_high, 1)
        moving_up = jnp.pad(moving_up, ((0, rows - half), (0, 0)))
        moving_down = jnp.pad(moving_down, ((half, 0), (0, 0)))
        for hops in range(antipode - 1, 0, -1):
            up = make_part(hops, 0, rows) + moving_up.astype(jnp.float32)
            down = make_part(tx_size - hops, 0, rows) + moving_down.astype(jnp.float32)
            up, down = up.astype(jnp.bfloat16), down.astype(jnp.bfloat16)
            moving_up, moving_down = shift(up, -1), shift(down, 1)
        return lambda own, low, high: own + moving_up[low:high].astype(jnp.float32) + moving_down[low:high].astype(jnp.float32)

    def body(x_act, cot_out, ln1_gain, ln1_bias, ln2_gain, ln2_bias, w_qkv, b_qkv, w_dense, b_dense, w_up, b_up, w_down, b_down):
        batch, seq_len, d_local = x_act.shape
        n_seq = batch // tx_size
        own = seq_len // ty_size
        row, col = lax.axis_index('tx'), lax.axis_index('ty')
        qkv_width = w_qkv.shape[1] * w_qkv.shape[2]
        head = qkv_width // 3
        chunks = range(n_seq)
        attention = [attention_calls(seq_len, head, s) for s in chunks]

        def to_tokens(act):
            parts = act.reshape(tx_size, n_seq, ty_size, own, d_local)
            pick = lambda index: lax.dynamic_slice(parts, (index, 0, col, 0, 0), (1, n_seq, 1, own, d_local)).reshape(n_seq, own, d_local)
            blocks = [pick(row)] + [shift(pick((row - r) % tx_size), r) for r in range(1, tx_size)]
            return jnp.concatenate(blocks, axis=2)

        place = jnp.stack([row, col // 2, col % 2])

        def to_width(parts):
            return jnp.stack([parts[0]] + [shift(parts[r], -r) for r in range(1, tx_size)])

        line = lax.broadcasted_iota(jnp.int32, (8, d_local), 0)
        small = jnp.zeros((8, d_local), jnp.bfloat16)
        for index, vector in enumerate((ln1_gain, ln1_bias, ln2_gain, ln2_bias, b_dense, b_down)):
            small = jnp.where(line == index, vector[None, :], small)
        small = [small] + [shift(small, r) for r in range(1, tx_size)]
        small = jnp.concatenate(small, axis=1).astype(jnp.float32)
        bias_out = small[4] + small[5]
        x_own = to_tokens(x_act)
        cot_own = to_tokens(cot_out)
        x_group = lax.all_gather(x_own, 'ty', axis=1, tiled=True)
        cot_group = lax.all_gather(cot_own, 'ty', axis=1, tiled=True)
        x_group, cot_group = x_group.reshape(n_seq * seq_len, -1), cot_group.reshape(n_seq * seq_len, -1)
        w_in = jnp.concatenate([w_qkv.reshape(d_local, qkv_width), w_up], axis=1)
        w_in = ring_gather(w_in, shift, tx_size)
        w_in = jnp.concatenate(w_in, axis=0)
        w_back = ring_gather(jnp.concatenate([w_dense, w_down], axis=0), shift, tx_size)
        back_size = tx_size * w_back[0].size

        n_tok, d_model = x_group.shape
        x_rows, cot_rows = x_own.reshape(-1, d_model), cot_own.reshape(-1, d_model)
        ff_width = w_up.shape[1]
        h_attn, h_mlp, qkv_act, pre_act, gelu_out = tile_call(
            front_kernel, [x_group], [small, w_in, b_qkv.reshape(1, -1).astype(jnp.float32), b_up.reshape(1, -1).astype(jnp.float32)],
            [(d_model, jnp.bfloat16), (d_model, jnp.bfloat16), (qkv_width, jnp.bfloat16), (ff_width, jnp.bfloat16), (ff_width, jnp.bfloat16)],
            (0, n_tok), 2 * n_tok * w_in.size, 48, True)
        qkv_seq = qkv_act.reshape(n_seq, seq_len, qkv_width)
        context, y_out = [], None
        for s in chunks:
            context.append(attention[s][0](qkv_seq).reshape(seq_len, head))
            (y_part,) = tile_call(y_kernel, [context[s], gelu_out], w_back, [(d_model, jnp.bfloat16)], (s * seq_len, seq_len), 2 * seq_len * back_size, 24)
            mixed = lax.psum_scatter(y_part, 'ty', scatter_dimension=0, tiled=True)
            blocks = to_width(row_call(finish_y_kernel, tx_size, s, own, x_rows, mixed, bias_out.reshape(1, -1)))
            full = lax.all_gather(blocks, 'ty', axis=1, tiled=True)
            y_out = place_call(place_kernel, place, [full], y_out, s, n_seq, seq_len)
        context = jnp.concatenate(context, axis=0)

        d_ctx, d_pre, d_b_up = tile_call(
            d_pre_kernel, [cot_group, pre_act], w_back,
            [(head, jnp.bfloat16), (ff_width, jnp.bfloat16), ((8, ff_width), jnp.float32)], (0, n_tok), 2 * n_tok * back_size, 32)
        d_ctx, d_b_up = d_ctx.reshape(n_seq, seq_len, head), d_b_up.sum(0)
        d_qkv, d_b_qkv, d_ln, dx_act = [], [], [], None
        for s in chunks:
            d_qkv_seq, d_b_seq = attention[s][1](qkv_seq, d_ctx)
            d_qkv.append(d_qkv_seq.reshape(seq_len, qkv_width))
            d_b_qkv.append(d_b_seq.reshape(-1))
            a6_part, sums = tile_call(
                d_h_kernel, [d_qkv[s], d_pre, x_group], [small, w_in],
                [(d_model, jnp.bfloat16), ((4, 8, d_model), jnp.float32)], (s * seq_len, seq_len), 2 * seq_len * w_in.size, 32)
            d_ln.append(sums)
            value_a6 = lax.psum_scatter(a6_part, 'ty', scatter_dimension=0, tiled=True)
            parts = row_call(finish_dx_kernel, tx_size, s, own, x_rows, value_a6, cot_rows)
            blocks = ring_gather(to_width(parts), along, ty_size // 2)
            blocks = blocks + [partner(block) for block in blocks]
            dx_act = place_call(place_pieces_kernel, place, blocks, dx_act, s, n_seq, seq_len)
        d_qkv = jnp.concatenate(d_qkv, axis=0)

        d_ln = small_sum(sum(d_ln).sum(1), 'ty', ty_size).reshape(4, tx_size, d_local)
        d_ln = d_ln[:, 0] + sum(shift(d_ln[:, r], -r) for r in range(1, tx_size))
        d_bias = small_sum(jnp.concatenate([sum(d_b_qkv), d_b_up])[None], 'tx', tx_size)[0]
        d_b_out = cot_out.astype(jnp.float32).sum((0, 1))

        cols = lambda act, r: act[:, r * d_local:(r + 1) * d_local]
        inner = jnp.concatenate([context, gelu_out], axis=1)
        add_back = ring_scatter(lambda r, low, high: dot(inner[:, low:high], cols(cot_group, r), TN), inner.shape[1])
        add_up = ring_scatter(lambda r, low, high: dot(cols(h_mlp, r)[:, low:high], d_pre, TN), d_local)
        add_qkv = ring_scatter(lambda r, low, high: dot(cols(h_attn, r)[:, low:high], d_qkv, TN), d_local)
        d_w_dense = add_back(dot(context, cols(cot_group, 0), TN), 0, head)
        d_w_down = add_back(dot(gelu_out, cols(cot_group, 0), TN), head, inner.shape[1])
        d_w_up = add_up(dot(cols(h_mlp, 0), d_pre, TN), 0, d_local)
        d_w_qkv = add_qkv(dot(cols(h_attn, 0), d_qkv, TN), 0, d_local)
        return (y_out, dx_act, d_ln[0], d_ln[1], d_ln[2], d_ln[3], d_w_qkv.reshape(w_qkv.shape), d_bias[:qkv_width].reshape(b_qkv.shape), d_w_dense, d_b_out, d_w_up, d_bias[qkv_width:], d_w_down, d_b_out)

    return jax.shard_map(body, mesh=mesh, in_specs=in_specs, out_specs=out_specs, check_vma=False)
```

```python
import functools
import jax
import jax.numpy as jnp
from jax import lax
from jax.experimental import pallas as pl
from jax.experimental.pallas import tpu as pltpu
from jax.sharding import PartitionSpec as P


LN_EPS = 1e-5
ROPE_BASE = 10000.0
ROTARY_DIVISOR = 4
LANES = 128
Q_ROWS = 256
LN_ROWS = 64
MIB = 1024 * 1024
TILE = 256
SQRT_HALF = 0.5 ** 0.5
INV_SQRT_2PI = 0.3989422804014327

NT = (((1,), (1,)), ((), ()))
TN = (((0,), (0,)), ((), ()))
NN = (((1,), (0,)), ((), ()))


def dot(a, b, dims):
    return lax.dot_general(a, b, dims, preferred_element_type=jnp.float32)


def rotary_tables(seq_len, rot_dim):
    half = rot_dim // 2
    lane = jnp.arange(LANES)
    freq_index = jnp.where(lane < half, lane, lane - half)
    inv_freq = ROPE_BASE ** (-(2 * freq_index).astype(jnp.float32) / rot_dim)
    angles = jnp.arange(seq_len, dtype=jnp.float32)[:, None] * inv_freq[None, :]
    inside = (lane < rot_dim)[None, :]
    cos_tab = jnp.where(inside, jnp.cos(angles), 1.0)
    sin = jnp.where(inside, jnp.sin(angles), 0.0)
    first = (lane < half)[None, :]
    return cos_tab, jnp.where(first, -sin, 0.0), jnp.where(first, 0.0, sin)


def rotate(part, cos_tab, sin_lo, sin_hi, half, sign):
    head = part[:, :LANES]
    forward = pltpu.roll(head, half, 1)
    backward = pltpu.roll(head, LANES - half, 1)
    mixed = head * cos_tab + sign * (backward * sin_lo + forward * sin_hi)
    return jnp.concatenate([mixed, part[:, LANES:]], axis=1)


def causal_probs(q_rows, keys, row_start, scale):
    scores = dot(q_rows, keys, NT) * scale
    rows = row_start + lax.broadcasted_iota(jnp.int32, scores.shape, 0)
    cols = lax.broadcasted_iota(jnp.int32, scores.shape, 1)
    scores = jnp.where(rows >= cols, scores, -1e30)
    exps = jnp.exp(scores - jnp.max(scores, axis=1, keepdims=True))
    return exps * (1.0 / jnp.sum(exps, axis=1, keepdims=True))


def attn_fwd_kernel(qkv_ref, ctx_ref, *, scale, span):
    seq_len, width = ctx_ref.shape[1:]
    for end in range(span, seq_len + 1, span):
        @pl.loop(0, span // Q_ROWS)
        def _(step, end=end):
            start = pl.multiple_of(end - span + step * Q_ROWS, Q_ROWS)
            rows = pl.ds(start, Q_ROWS)
            probs = causal_probs(qkv_ref[0, rows, :width], qkv_ref[0, :end, width:2 * width], start, scale).astype(jnp.bfloat16)
            ctx_ref[0, rows, :] = dot(probs, qkv_ref[0, :end, 2 * width:], NN).astype(jnp.bfloat16)


def attn_bwd_kernel(qkv_ref, dctx_ref, cos_ref, lo_ref, hi_ref, dqkv_ref, db_ref, dk_ref, dv_ref, *, half, scale, span):
    seq_len, width = dctx_ref.shape[1:]
    dk_ref[...] = jnp.zeros(dk_ref.shape, jnp.float32)
    dv_ref[...] = jnp.zeros(dv_ref.shape, jnp.float32)
    db_ref[...] = jnp.zeros(db_ref.shape, jnp.float32)

    def store(rows, col, grad_rot, turn):
        grad = grad_rot.astype(jnp.bfloat16)
        if turn:
            wide = grad.astype(jnp.float32)
            grad = rotate(wide, cos_ref[rows, :], lo_ref[rows, :], hi_ref[rows, :], half, -1.0).astype(jnp.bfloat16)
        dqkv_ref[0, rows, col:col + width] = grad
        db_ref[0, :, col:col + width] += sublane_sum(grad.astype(jnp.float32))

    for end in range(span, seq_len + 1, span):
        @pl.loop(0, span // Q_ROWS)
        def _(step, end=end):
            start = pl.multiple_of(end - span + step * Q_ROWS, Q_ROWS)
            rows = pl.ds(start, Q_ROWS)
            q_rows, keys = qkv_ref[0, rows, :width], qkv_ref[0, :end, width:2 * width]
            dctx = dctx_ref[0, rows, :]
            probs = causal_probs(q_rows, keys, start, scale)
            dprobs = dot(dctx, qkv_ref[0, :end, 2 * width:], NT).astype(jnp.bfloat16).astype(jnp.float32)
            dv_ref[:end, :] += dot(probs.astype(jnp.bfloat16), dctx, TN)
            inner = jnp.sum(probs * dprobs, axis=1, keepdims=True)
            dscores = (probs * (dprobs - inner) * scale).astype(jnp.bfloat16)
            dk_ref[:end, :] += dot(dscores, q_rows, TN)
            store(rows, 0, dot(dscores, keys, NN), True)

    @pl.loop(0, seq_len // Q_ROWS)
    def _(step):
        rows = pl.ds(pl.multiple_of(step * Q_ROWS, Q_ROWS), Q_ROWS)
        store(rows, width, dk_ref[rows, :], True)
        store(rows, 2 * width, dv_ref[rows, :], False)


def attention_calls(n_seq, seq_len, width, tables):
    half = width // ROTARY_DIVISOR // 2
    scale = width ** -0.5
    span = 512 if seq_len % 512 == 0 else seq_len
    seq_spec = lambda cols, first=0: pl.BlockSpec((1, seq_len, cols), lambda s: (s + first, 0, 0))
    tab_spec = pl.BlockSpec((seq_len, LANES), lambda s: (0, 0))
    acc_scratch = pltpu.VMEM((seq_len, width), jnp.float32)
    pairs = seq_len * seq_len // 2
    params = pltpu.CompilerParams(dimension_semantics=("arbitrary",), vmem_limit_bytes=60 * MIB)

    def forward(qkv):
        return pl.pallas_call(
            functools.partial(attn_fwd_kernel, scale=scale, span=span),
            grid=(n_seq,),
            in_specs=[seq_spec(3 * width)],
            out_specs=seq_spec(width),
            out_shape=jax.ShapeDtypeStruct((n_seq, seq_len, width), jnp.bfloat16),
            compiler_params=params,
            name="af",
            cost_estimate=pl.CostEstimate(flops=8 * n_seq * pairs * width, bytes_accessed=8 * n_seq * seq_len * width, transcendentals=n_seq * pairs),
        )(qkv)

    def backward(qkv, dctx, index):
        return pl.pallas_call(
            functools.partial(attn_bwd_kernel, half=half, scale=scale, span=span),
            grid=(1,),
            in_specs=[seq_spec(3 * width, index), seq_spec(width, index), tab_spec, tab_spec, tab_spec],
            out_specs=[seq_spec(3 * width), pl.BlockSpec((1, 8, 3 * width), lambda s: (s, 0, 0))],
            out_shape=[jax.ShapeDtypeStruct((1, seq_len, 3 * width), jnp.bfloat16), jax.ShapeDtypeStruct((1, 8, 3 * width), jnp.float32)],
            scratch_shapes=[acc_scratch, acc_scratch],
            compiler_params=params,
            name="ab",
            cost_estimate=pl.CostEstimate(flops=20 * pairs * width, bytes_accessed=14 * seq_len * width, transcendentals=pairs),
        )(qkv, dctx, *tables)

    return forward, backward


def place_kernel(place_ref, full_ref, out_ref, held_ref, in_sems, out_sems, *, chunk, n_seq):
    groups = full_ref.shape[0]
    fetch = [pltpu.make_async_copy(full_ref.at[lax.rem(place_ref[0] + groups - t, groups)], held_ref.at[t], in_sems.at[t]) for t in range(groups)]
    store = [pltpu.make_async_copy(held_ref.at[t], out_ref.at[t], out_sems.at[t]) for t in range(groups)]
    for copy in fetch:
        copy.start()
    for t in range(groups):
        fetch[t].wait()
        store[t].start()
    for copy in store:
        copy.wait()


def place_pieces_kernel(place_ref, *refs, chunk, n_seq):
    out_ref, held_ref, in_sems, out_sems = refs[-4:]
    groups, own, _ = refs[0].shape
    columns = held_ref.shape[0] // 2
    row, column, core = place_ref[0], place_ref[1], place_ref[2]
    fetch, store = [], []
    for index in range(2 * columns):
        source = 2 * lax.rem(column + index % columns, columns) + (core if index < columns else 1 - core)
        at = pl.ds(pl.multiple_of(source * own, own), own)
        fetch.append(pltpu.make_async_copy(refs[index], held_ref.at[index], in_sems.at[index]))
        for t in range(groups):
            piece = held_ref.at[index, lax.rem(row + groups - t, groups)]
            store.append(pltpu.make_async_copy(piece, out_ref.at[t * n_seq + chunk, at], out_sems.at[index]))
    for copy in fetch:
        copy.start()
    for index in range(2 * columns):
        fetch[index].wait()
        for copy in store[index * groups:(index + 1) * groups]:
            copy.start()
    for copy in store:
        copy.wait()


def place_call(kernel, place, operands, out, chunk, n_seq, tokens):
    groups, _, width = operands[0].shape
    operands = [place, *operands] + ([] if out is None else [out])
    any_spec = pl.BlockSpec(memory_space=pl.ANY)
    pieces = len(operands) - 1 - (out is not None)
    held = operands[1].shape if pieces == 1 else (pieces,) + operands[1].shape
    sems = pltpu.SemaphoreType.DMA((groups if pieces == 1 else pieces,))
    return pl.pallas_call(
        functools.partial(kernel, chunk=chunk, n_seq=n_seq),
        in_specs=[pl.BlockSpec(memory_space=pltpu.SMEM)] + [any_spec] * (len(operands) - 1),
        out_specs=any_spec,
        out_shape=jax.ShapeDtypeStruct((groups * n_seq, tokens, width), jnp.bfloat16),
        scratch_shapes=[pltpu.VMEM(held, jnp.bfloat16), sems, sems],
        input_output_aliases={} if out is None else {len(operands) - 1: 0},
        cost_estimate=pl.CostEstimate(flops=groups * tokens * width, bytes_accessed=4 * groups * tokens * width, transcendentals=0),
    )(*operands)


def split_width(value, out_refs):
    width = out_refs[0].shape[1]
    for index, out_ref in enumerate(out_refs):
        out_ref[...] = value[:, index * width:(index + 1) * width].astype(out_ref.dtype)


def finish_y_kernel(x_ref, mixed_ref, bias_ref, *out_refs):
    split_width(x_ref[...].astype(jnp.float32) + mixed_ref[...].astype(jnp.float32) + bias_ref[...], out_refs)


def normalize(act):
    act = act.astype(jnp.float32)
    mean = act.mean(-1, keepdims=True)
    inv_std = lax.rsqrt((act * act).mean(-1, keepdims=True) - mean * mean + LN_EPS)
    return (act - mean) * inv_std, inv_std


def finish_dx_kernel(x_ref, a6_ref, cot_ref, *out_refs):
    x_hat, inv_std = normalize(x_ref[...])
    value_a6 = a6_ref[...].astype(jnp.float32)
    mean_a6 = value_a6.mean(-1, keepdims=True)
    mean_a6x = (value_a6 * x_hat).mean(-1, keepdims=True)
    split_width(cot_ref[...].astype(jnp.float32) + inv_std * (value_a6 - mean_a6 - x_hat * mean_a6x), out_refs)


def row_call(kernel, parts, index, rows, *operands):
    width = operands[0].shape[1]
    specs = [pl.BlockSpec((min(rows, op.shape[0]), width), lambda s, i=(index if op.shape[0] > rows else 0): (i, 0)) for op in operands]
    return pl.pallas_call(
        kernel,
        grid=(1,),
        in_specs=specs,
        out_specs=[pl.BlockSpec((rows, width // parts), lambda s: (0, 0))] * parts,
        out_shape=[jax.ShapeDtypeStruct((rows, width // parts), jnp.bfloat16)] * parts,
        compiler_params=pltpu.CompilerParams(vmem_limit_bytes=16 * MIB),
        cost_estimate=pl.CostEstimate(flops=16 * rows * width, bytes_accessed=8 * rows * width, transcendentals=0),
    )(*operands)


def sublane_sum(value):
    return value.reshape(value.shape[0] // 8, 8, value.shape[1]).sum(0)


def norm_kernel(x_ref, small_ref, h_attn_ref, h_mlp_ref):
    @pl.loop(0, x_ref.shape[0] // LN_ROWS)
    def _(step):
        at = pl.ds(pl.multiple_of(step * LN_ROWS, LN_ROWS), LN_ROWS)
        x_hat, _ = normalize(x_ref[at, :])
        h_attn_ref[at, :] = (x_hat * small_ref[0:1, :] + small_ref[1:2, :]).astype(jnp.bfloat16)
        h_mlp_ref[at, :] = (x_hat * small_ref[2:3, :] + small_ref[3:4, :]).astype(jnp.bfloat16)


def front_kernel(h_attn_ref, h_mlp_ref, cos_ref, lo_ref, hi_ref, w_ref, b_qkv_ref, b_up_ref, qkv_ref, pre_ref, gelu_ref):
    qkv_width = qkv_ref.shape[1]
    head = qkv_width // 3
    for low in range(0, qkv_width, head):
        at = slice(low, low + head)
        part = (dot(h_attn_ref[...], w_ref[:, at], NN) + b_qkv_ref[:, at]).astype(jnp.bfloat16)
        if low < 2 * head:
            part = rotate(part.astype(jnp.float32), cos_ref[...], lo_ref[...], hi_ref[...], head // ROTARY_DIVISOR // 2, 1.0).astype(jnp.bfloat16)
        qkv_ref[:, at] = part
    for low in range(0, pre_ref.shape[1], TILE):
        at = slice(low, low + TILE)
        acc = dot(h_mlp_ref[...], w_ref[:, qkv_width + low:qkv_width + low + TILE], NN) + b_up_ref[:, at]
        pre = acc.astype(jnp.bfloat16)
        pre_ref[:, at] = pre
        wide = pre.astype(jnp.float32)
        gelu_ref[:, at] = (0.5 * wide * (1.0 + lax.erf(wide * SQRT_HALF))).astype(jnp.bfloat16)


def y_kernel(ctx_ref, gelu_ref, *refs):
    w_refs, y_ref = refs[:-1], refs[-1]
    head = ctx_ref.shape[1]
    places, _, own, _ = y_ref.shape
    for index, w_ref in enumerate(w_refs):
        width = w_ref.shape[1]
        acc = dot(ctx_ref[...], w_ref[:head, :], NN) + dot(gelu_ref[...], w_ref[head:, :], NN)
        y_ref[:, 0, :, index * width:(index + 1) * width] = acc.astype(jnp.bfloat16).reshape(places, own, width)


def d_pre_kernel(cot_ref, pre_ref, *refs):
    w_refs, (d_ctx_ref, d_pre_ref, d_bias_ref) = refs[:-3], refs[-3:]
    width = w_refs[0].shape[1]

    def back(low, high):
        return sum(dot(cot_ref[:, r * width:(r + 1) * width], w_ref[low:high, :], NT) for r, w_ref in enumerate(w_refs)).astype(jnp.bfloat16)

    head = d_ctx_ref.shape[1]

    @pl.when(pl.program_id(0) == 0)
    def _():
        d_bias_ref[...] = jnp.zeros(d_bias_ref.shape, jnp.float32)

    d_ctx_ref[...] = back(0, head)
    for low in range(0, d_pre_ref.shape[1], TILE):
        at = slice(low, low + TILE)
        d_gelu = back(head + low, head + low + TILE).astype(jnp.float32)
        pre = pre_ref[:, at].astype(jnp.float32)
        slope = 0.5 * (1.0 + lax.erf(pre * SQRT_HALF)) + pre * (jnp.exp(-0.5 * pre * pre) * INV_SQRT_2PI)
        d_pre = (d_gelu * slope).astype(jnp.bfloat16)
        d_pre_ref[:, at] = d_pre
        d_bias_ref[:, at] += sublane_sum(d_pre.astype(jnp.float32))


def d_h_kernel(d_qkv_ref, d_pre_ref, x_ref, small_ref, w_ref, a6_ref, sums_ref):
    qkv_width = d_qkv_ref.shape[1]

    @pl.when(pl.program_id(0) == 0)
    def _():
        sums_ref[...] = jnp.zeros(sums_ref.shape, jnp.float32)

    x_float = x_ref[...].astype(jnp.float32)
    mean = x_float.mean(-1, keepdims=True)
    inv_std = lax.rsqrt((x_float * x_float).mean(-1, keepdims=True) - mean * mean + LN_EPS)
    for low in range(0, a6_ref.shape[1], TILE):
        at = slice(low, low + TILE)
        d_attn = dot(d_qkv_ref[...], w_ref[at, :qkv_width], NT).astype(jnp.bfloat16).astype(jnp.float32)
        d_mlp = dot(d_pre_ref[...], w_ref[at, qkv_width:], NT).astype(jnp.bfloat16).astype(jnp.float32)
        a6_ref[:, at] = (d_attn * small_ref[0:1, at] + d_mlp * small_ref[2:3, at]).astype(jnp.bfloat16)
        x_hat = (x_ref[:, at].astype(jnp.float32) - mean) * inv_std
        sums_ref[0, :, at] += sublane_sum(d_attn * x_hat)
        sums_ref[1, :, at] += sublane_sum(d_attn)
        sums_ref[2, :, at] += sublane_sum(d_mlp * x_hat)
        sums_ref[3, :, at] += sublane_sum(d_mlp)


def tile_call(kernel, tiled, whole, outs, row_range, flops, rows=512):
    start, count = row_range
    rows = next(r for r in (rows, 256, 128, 64, count) if count % r == 0 and all(op.shape[0] % r == 0 for op in tiled))
    first = start // rows

    def tile_spec(op):
        blocks = op.shape[0] // rows
        if blocks * rows < count:
            return pl.BlockSpec((rows, op.shape[1]), lambda s: (lax.rem(s, blocks), 0))
        return pl.BlockSpec((rows, op.shape[1]), lambda s, f=(first if op.shape[0] != count else 0): (s + f, 0))

    in_specs = [tile_spec(op) for op in tiled]
    in_specs += [pl.BlockSpec(op.shape, lambda s, n=op.ndim: (0,) * n, pipeline_mode=pl.Buffered(1)) for op in whole]
    out_specs, out_shapes = [], []
    for form, dtype in outs:
        if isinstance(form, int):
            out_specs.append(pl.BlockSpec((rows, form), lambda s: (s, 0)))
            out_shapes.append(jax.ShapeDtypeStruct((count, form), dtype))
        elif isinstance(form[0], tuple):
            out_specs.append(pl.BlockSpec(form[1], form[2]))
            out_shapes.append(jax.ShapeDtypeStruct(form[0], dtype))
        else:
            out_specs.append(pl.BlockSpec(form, lambda s, n=len(form): (0,) * n))
            out_shapes.append(jax.ShapeDtypeStruct(form, dtype))
    moved = sum(2 * op.shape[1] * count for op in tiled) + sum(2 * op.size for op in whole) + sum(2 * shape.size for shape in out_shapes)
    return pl.pallas_call(
        kernel,
        grid=(count // rows,),
        in_specs=in_specs,
        out_specs=out_specs,
        out_shape=out_shapes,
        compiler_params=pltpu.CompilerParams(dimension_semantics=("arbitrary",), vmem_limit_bytes=60 * MIB),
        cost_estimate=pl.CostEstimate(flops=flops, bytes_accessed=moved, transcendentals=0),
    )(*tiled, *whole)


def solution(mesh):
    tx_size, ty_size = mesh.shape['tx'], mesh.shape['ty']
    act_spec = P('dp', None, 'tx')
    width_spec = P('tx')
    in_specs = (act_spec, act_spec, width_spec, width_spec, width_spec, width_spec, P('tx', 'ty', None), P('ty', None), P('ty', 'tx'), width_spec, P('tx', 'ty'), P('ty'), P('ty', 'tx'), width_spec)
    width_out = P(('dp', 'tx'))
    out_specs = (act_spec, act_spec, width_out, width_out, width_out, width_out, P(('dp', 'tx'), 'ty', None), P(('dp', 'ty'), None), P(('dp', 'ty'), 'tx'), width_out, P(('dp', 'tx'), 'ty'), P(('dp', 'ty')), P(('dp', 'ty'), 'tx'), width_out)
    antipode = tx_size // 2

    def shift(value, hops):
        return lax.ppermute(value, 'tx', [(s, (s - hops) % tx_size) for s in range(tx_size)])

    def small_sum(value, axis, size):
        step = 1
        while step < size:
            value = value + lax.ppermute(value, axis, [(s, s ^ step) for s in range(size)])
            step *= 2
        return value

    def along(value, hops):
        return lax.ppermute(value, 'ty', [(s, (s - 2 * hops) % ty_size) for s in range(ty_size)])

    def partner(value):
        return lax.ppermute(value, 'ty', [(s, s ^ 1) for s in range(ty_size)])

    def ring_gather(block, move, size):
        far = size // 2
        blocks = {0: block}
        for hops in range(1, far):
            blocks[hops] = move(blocks[hops - 1], 1)
            blocks[size - hops] = move(blocks[(size - hops + 1) % size], -1)
        half = block.shape[0] // 2
        blocks[far] = jnp.concatenate([move(blocks[far - 1][:half], 1), move(blocks[far + 1][half:], -1)], axis=0)
        return [blocks[r] for r in range(size)]

    def ring_scatter(make_part, rows):
        half = rows // 2
        far = make_part(antipode).astype(jnp.bfloat16)
        moving_up, moving_down = shift(far[:half], -1), shift(far[half:], 1)
        moving_up = jnp.pad(moving_up, ((0, rows - half), (0, 0)))
        moving_down = jnp.pad(moving_down, ((half, 0), (0, 0)))
        for hops in range(antipode - 1, 0, -1):
            up = make_part(hops) + moving_up.astype(jnp.float32)
            down = make_part(tx_size - hops) + moving_down.astype(jnp.float32)
            up, down = up.astype(jnp.bfloat16), down.astype(jnp.bfloat16)
            moving_up, moving_down = shift(up, -1), shift(down, 1)
        return lambda own, low, high: own + moving_up[low:high].astype(jnp.float32) + moving_down[low:high].astype(jnp.float32)

    def body(x_act, cot_out, ln1_gain, ln1_bias, ln2_gain, ln2_bias, w_qkv, b_qkv, w_dense, b_dense, w_up, b_up, w_down, b_down):
        batch, seq_len, d_local = x_act.shape
        n_seq = batch // tx_size
        own = seq_len // ty_size
        row, col = lax.axis_index('tx'), lax.axis_index('ty')
        qkv_width = w_qkv.shape[1] * w_qkv.shape[2]
        head = qkv_width // 3
        chunks = range(n_seq)
        tables = rotary_tables(seq_len, head // ROTARY_DIVISOR)
        attn_fwd, attn_bwd = attention_calls(n_seq, seq_len, head, tables)

        def to_tokens(act):
            parts = act.reshape(tx_size, n_seq, ty_size, own, d_local)
            pick = lambda index: lax.dynamic_slice(parts, (index, 0, col, 0, 0), (1, n_seq, 1, own, d_local)).reshape(n_seq, own, d_local)
            blocks = [pick(row)] + [shift(pick((row - r) % tx_size), r) for r in range(1, tx_size)]
            return jnp.concatenate(blocks, axis=2)

        place = jnp.stack([row, col // 2, col % 2])

        def to_width(parts):
            return jnp.stack([parts[0]] + [shift(parts[r], -r) for r in range(1, tx_size)])

        line = lax.broadcasted_iota(jnp.int32, (8, d_local), 0)
        small = jnp.zeros((8, d_local), jnp.bfloat16)
        for index, vector in enumerate((ln1_gain, ln1_bias, ln2_gain, ln2_bias, b_dense, b_down)):
            small = jnp.where(line == index, vector[None, :], small)
        small = [small] + [shift(small, r) for r in range(1, tx_size)]
        small = jnp.concatenate(small, axis=1).astype(jnp.float32)
        bias_out = small[4] + small[5]
        x_own = to_tokens(x_act)
        cot_own = to_tokens(cot_out)
        x_group = lax.all_gather(x_own, 'ty', axis=1, tiled=True)
        cot_group = lax.all_gather(cot_own, 'ty', axis=1, tiled=True)
        x_group, cot_group = x_group.reshape(n_seq * seq_len, -1), cot_group.reshape(n_seq * seq_len, -1)
        w_in = jnp.concatenate([w_qkv.reshape(d_local, qkv_width), w_up], axis=1)
        w_in = ring_gather(w_in, shift, tx_size)
        w_in = jnp.concatenate(w_in, axis=0)
        w_back = ring_gather(jnp.concatenate([w_dense, w_down], axis=0), shift, tx_size)
        back_size = tx_size * w_back[0].size

        n_tok, d_model = x_group.shape
        x_rows, cot_rows = x_own.reshape(-1, d_model), cot_own.reshape(-1, d_model)
        ff_width = w_up.shape[1]
        h_attn, h_mlp = tile_call(norm_kernel, [x_group], [small], [(d_model, jnp.bfloat16), (d_model, jnp.bfloat16)], (0, n_tok), 16 * x_group.size)
        qkv_act, pre_act, gelu_out = tile_call(
            front_kernel, [h_attn, h_mlp, *tables], [w_in, b_qkv.reshape(1, -1).astype(jnp.float32), b_up.reshape(1, -1).astype(jnp.float32)],
            [(qkv_width, jnp.bfloat16), (ff_width, jnp.bfloat16), (ff_width, jnp.bfloat16)], (0, n_tok), 2 * n_tok * w_in.size)
        qkv_seq = qkv_act.reshape(n_seq, seq_len, qkv_width)
        context = attn_fwd(qkv_seq).reshape(n_tok, head)
        blocks_per_seq = ty_size // 2
        y_form = ((ty_size, n_seq, own, d_model), (2, 1, own, d_model), lambda s: (lax.rem(s, blocks_per_seq), s // blocks_per_seq, 0, 0))
        (y_part,) = tile_call(y_kernel, [context, gelu_out], w_back, [(y_form, jnp.bfloat16)], (0, n_tok), 2 * n_tok * back_size, 2 * own)
        mixed = lax.psum_scatter(y_part.reshape(n_tok, d_model), 'ty', scatter_dimension=0, tiled=True)
        blocks = to_width(row_call(finish_y_kernel, tx_size, 0, n_seq * own, x_rows, mixed, bias_out.reshape(1, -1)))
        full = lax.all_gather(blocks.reshape(tx_size * n_seq, own, d_local), 'ty', axis=1, tiled=True)
        y_out = place_call(place_kernel, place, [full.reshape(tx_size, n_seq * seq_len, d_local)], None, 0, 1, n_seq * seq_len)

        d_ctx, d_pre, d_b_up = tile_call(
            d_pre_kernel, [cot_group, pre_act], w_back,
            [(head, jnp.bfloat16), (ff_width, jnp.bfloat16), ((8, ff_width), jnp.float32)], (0, n_tok), 2 * n_tok * back_size)
        d_ctx, d_b_up = d_ctx.reshape(n_seq, seq_len, head), d_b_up.sum(0)
        d_qkv, d_b_qkv, d_ln, dx_act = [], [], [], None
        for s in chunks:
            d_qkv_seq, d_b_seq = attn_bwd(qkv_seq, d_ctx, s)
            d_qkv.append(d_qkv_seq.reshape(seq_len, qkv_width))
            d_b_qkv.append(d_b_seq.sum((0, 1)))
            a6_part, sums = tile_call(
                d_h_kernel, [d_qkv[s], d_pre, x_group], [small, w_in],
                [(d_model, jnp.bfloat16), ((4, 8, d_model), jnp.float32)], (s * seq_len, seq_len), 2 * seq_len * w_in.size)
            d_ln.append(sums)
            value_a6 = lax.psum_scatter(a6_part, 'ty', scatter_dimension=0, tiled=True)
            parts = row_call(finish_dx_kernel, tx_size, s, own, x_rows, value_a6, cot_rows)
            blocks = ring_gather(to_width(parts), along, ty_size // 2)
            blocks = blocks + [partner(block) for block in blocks]
            dx_act = place_call(place_pieces_kernel, place, blocks, dx_act, s, n_seq, seq_len)
        d_qkv = jnp.concatenate(d_qkv, axis=0)

        d_ln = small_sum(sum(d_ln).sum(1), 'ty', ty_size).reshape(4, tx_size, d_local)
        d_ln = d_ln[:, 0] + sum(shift(d_ln[:, r], -r) for r in range(1, tx_size))
        d_bias = small_sum(jnp.concatenate([sum(d_b_qkv), d_b_up])[None], 'tx', tx_size)[0]
        d_b_out = cot_out.astype(jnp.float32).sum((0, 1))

        cols = lambda act, r: act[:, r * d_local:(r + 1) * d_local]
        inner = jnp.concatenate([context, gelu_out], axis=1)
        add_back = ring_scatter(lambda r: dot(inner, cols(cot_group, r), TN), inner.shape[1])
        add_up = ring_scatter(lambda r: dot(cols(h_mlp, r), d_pre, TN), d_local)
        add_qkv = ring_scatter(lambda r: dot(cols(h_attn, r), d_qkv, TN), d_local)
        d_w_dense = add_back(dot(context, cols(cot_group, 0), TN), 0, head)
        d_w_down = add_back(dot(gelu_out, cols(cot_group, 0), TN), head, inner.shape[1])
        d_w_up = add_up(dot(cols(h_mlp, 0), d_pre, TN), 0, d_local)
        d_w_qkv = add_qkv(dot(cols(h_attn, 0), d_qkv, TN), 0, d_local)
        y_out = y_out.reshape(batch, seq_len, d_local)
        return (y_out, dx_act, d_ln[0], d_ln[1], d_ln[2], d_ln[3], d_w_qkv.reshape(w_qkv.shape), d_bias[:qkv_width].reshape(b_qkv.shape), d_w_dense, d_b_out, d_w_up, d_bias[qkv_width:], d_w_down, d_b_out)

    return jax.shard_map(body, mesh=mesh, in_specs=in_specs, out_specs=out_specs, check_vma=False)
```

```python
import functools
import jax
import jax.numpy as jnp
from jax import lax
from jax.experimental import pallas as pl
from jax.experimental.pallas import tpu as pltpu
from jax.sharding import PartitionSpec as P


LN_EPS = 1e-5
ROPE_BASE = 10000.0
ROTARY_DIVISOR = 4
LANES = 128
Q_ROWS = 256
LN_ROWS = 64
MIB = 1024 * 1024
TILE = 256
SQRT_HALF = 0.5 ** 0.5
INV_SQRT_2PI = 0.3989422804014327

NT = (((1,), (1,)), ((), ()))
TN = (((0,), (0,)), ((), ()))
NN = (((1,), (0,)), ((), ()))


def dot(a, b, dims):
    return lax.dot_general(a, b, dims, preferred_element_type=jnp.float32)


def rotary_tables(seq_len, rot_dim):
    half = rot_dim // 2
    lane = jnp.arange(LANES)
    freq_index = jnp.where(lane < half, lane, lane - half)
    inv_freq = ROPE_BASE ** (-(2 * freq_index).astype(jnp.float32) / rot_dim)
    angles = jnp.arange(seq_len, dtype=jnp.float32)[:, None] * inv_freq[None, :]
    inside = (lane < rot_dim)[None, :]
    cos_tab = jnp.where(inside, jnp.cos(angles), 1.0)
    sin = jnp.where(inside, jnp.sin(angles), 0.0)
    first = (lane < half)[None, :]
    return cos_tab, jnp.where(first, -sin, 0.0), jnp.where(first, 0.0, sin)


def rotate(part, cos_tab, sin_lo, sin_hi, half, sign):
    head = part[:, :LANES]
    forward = pltpu.roll(head, half, 1)
    backward = pltpu.roll(head, LANES - half, 1)
    mixed = head * cos_tab + sign * (backward * sin_lo + forward * sin_hi)
    return jnp.concatenate([mixed, part[:, LANES:]], axis=1)


def causal_probs(q_rows, keys, row_start, scale):
    scores = dot(q_rows, keys, NT) * scale
    rows = row_start + lax.broadcasted_iota(jnp.int32, scores.shape, 0)
    cols = lax.broadcasted_iota(jnp.int32, scores.shape, 1)
    scores = jnp.where(rows >= cols, scores, -1e30)
    exps = jnp.exp(scores - jnp.max(scores, axis=1, keepdims=True))
    return exps * (1.0 / jnp.sum(exps, axis=1, keepdims=True))


def attn_fwd_kernel(qkv_ref, ctx_ref, *, scale, span):
    seq_len, width = ctx_ref.shape[1:]
    for end in range(span, seq_len + 1, span):
        @pl.loop(0, span // Q_ROWS)
        def _(step, end=end):
            start = pl.multiple_of(end - span + step * Q_ROWS, Q_ROWS)
            rows = pl.ds(start, Q_ROWS)
            probs = causal_probs(qkv_ref[0, rows, :width], qkv_ref[0, :end, width:2 * width], start, scale).astype(jnp.bfloat16)
            ctx_ref[0, rows, :] = dot(probs, qkv_ref[0, :end, 2 * width:], NN).astype(jnp.bfloat16)


def attn_bwd_kernel(qkv_ref, dctx_ref, cos_ref, lo_ref, hi_ref, dqkv_ref, db_ref, dk_ref, dv_ref, *, half, scale, span):
    seq_len, width = dctx_ref.shape[1:]
    dk_ref[...] = jnp.zeros(dk_ref.shape, jnp.float32)
    dv_ref[...] = jnp.zeros(dv_ref.shape, jnp.float32)
    db_ref[...] = jnp.zeros(db_ref.shape, jnp.float32)

    def store(rows, col, grad_rot, turn):
        grad = grad_rot.astype(jnp.bfloat16)
        if turn:
            wide = grad.astype(jnp.float32)
            grad = rotate(wide, cos_ref[rows, :], lo_ref[rows, :], hi_ref[rows, :], half, -1.0).astype(jnp.bfloat16)
        dqkv_ref[0, rows, col:col + width] = grad
        db_ref[0, :, col:col + width] += sublane_sum(grad.astype(jnp.float32))

    for end in range(span, seq_len + 1, span):
        @pl.loop(0, span // Q_ROWS)
        def _(step, end=end):
            start = pl.multiple_of(end - span + step * Q_ROWS, Q_ROWS)
            rows = pl.ds(start, Q_ROWS)
            q_rows, keys = qkv_ref[0, rows, :width], qkv_ref[0, :end, width:2 * width]
            dctx = dctx_ref[0, rows, :]
            probs = causal_probs(q_rows, keys, start, scale)
            dprobs = dot(dctx, qkv_ref[0, :end, 2 * width:], NT).astype(jnp.bfloat16).astype(jnp.float32)
            dv_ref[:end, :] += dot(probs.astype(jnp.bfloat16), dctx, TN)
            inner = jnp.sum(probs * dprobs, axis=1, keepdims=True)
            dscores = (probs * (dprobs - inner) * scale).astype(jnp.bfloat16)
            dk_ref[:end, :] += dot(dscores, q_rows, TN)
            store(rows, 0, dot(dscores, keys, NN), True)

    @pl.loop(0, seq_len // Q_ROWS)
    def _(step):
        rows = pl.ds(pl.multiple_of(step * Q_ROWS, Q_ROWS), Q_ROWS)
        store(rows, width, dk_ref[rows, :], True)
        store(rows, 2 * width, dv_ref[rows, :], False)


def attention_calls(n_seq, seq_len, width, tables):
    half = width // ROTARY_DIVISOR // 2
    scale = width ** -0.5
    span = 512 if seq_len % 512 == 0 else seq_len
    seq_spec = lambda cols, first=0: pl.BlockSpec((1, seq_len, cols), lambda s: (s + first, 0, 0))
    tab_spec = pl.BlockSpec((seq_len, LANES), lambda s: (0, 0))
    acc_scratch = pltpu.VMEM((seq_len, width), jnp.float32)
    pairs = seq_len * seq_len // 2
    params = pltpu.CompilerParams(dimension_semantics=("arbitrary",), vmem_limit_bytes=60 * MIB)

    def forward(qkv):
        return pl.pallas_call(
            functools.partial(attn_fwd_kernel, scale=scale, span=span),
            grid=(n_seq,),
            in_specs=[seq_spec(3 * width)],
            out_specs=seq_spec(width),
            out_shape=jax.ShapeDtypeStruct((n_seq, seq_len, width), jnp.bfloat16),
            compiler_params=params,
            name="af",
            cost_estimate=pl.CostEstimate(flops=8 * n_seq * pairs * width, bytes_accessed=8 * n_seq * seq_len * width, transcendentals=n_seq * pairs),
        )(qkv)

    def backward(qkv, dctx, index):
        return pl.pallas_call(
            functools.partial(attn_bwd_kernel, half=half, scale=scale, span=span),
            grid=(1,),
            in_specs=[seq_spec(3 * width, index), seq_spec(width, index), tab_spec, tab_spec, tab_spec],
            out_specs=[seq_spec(3 * width), pl.BlockSpec((1, 8, 3 * width), lambda s: (s, 0, 0))],
            out_shape=[jax.ShapeDtypeStruct((1, seq_len, 3 * width), jnp.bfloat16), jax.ShapeDtypeStruct((1, 8, 3 * width), jnp.float32)],
            scratch_shapes=[acc_scratch, acc_scratch],
            compiler_params=params,
            name="ab",
            cost_estimate=pl.CostEstimate(flops=20 * pairs * width, bytes_accessed=14 * seq_len * width, transcendentals=pairs),
        )(qkv, dctx, *tables)

    return forward, backward


def place_kernel(place_ref, full_ref, *rest, chunk, n_seq):
    out_ref, held_ref, in_sems, out_sems = rest[-4:]
    groups = full_ref.shape[0]
    fetch = [pltpu.make_async_copy(full_ref.at[lax.rem(place_ref[0] + groups - t, groups)], held_ref.at[t], in_sems.at[t]) for t in range(groups)]
    store = [pltpu.make_async_copy(held_ref.at[t], out_ref.at[t * n_seq + chunk], out_sems.at[t]) for t in range(groups)]
    for copy in fetch:
        copy.start()
    for t in range(groups):
        fetch[t].wait()
        store[t].start()
    for copy in store:
        copy.wait()


def place_pieces_kernel(place_ref, *refs, chunk, n_seq):
    out_ref, held_ref, in_sems, out_sems = refs[-4:]
    groups, own, _ = refs[0].shape
    columns = held_ref.shape[0] // 2
    row, column, core = place_ref[0], place_ref[1], place_ref[2]
    fetch, store = [], []
    for index in range(2 * columns):
        source = 2 * lax.rem(column + index % columns, columns) + (core if index < columns else 1 - core)
        at = pl.ds(pl.multiple_of(source * own, own), own)
        fetch.append(pltpu.make_async_copy(refs[index], held_ref.at[index], in_sems.at[index]))
        for t in range(groups):
            piece = held_ref.at[index, lax.rem(row + groups - t, groups)]
            store.append(pltpu.make_async_copy(piece, out_ref.at[t * n_seq + chunk, at], out_sems.at[index]))
    for copy in fetch:
        copy.start()
    for index in range(2 * columns):
        fetch[index].wait()
        for copy in store[index * groups:(index + 1) * groups]:
            copy.start()
    for copy in store:
        copy.wait()


def place_call(kernel, place, operands, out, chunk, n_seq, tokens):
    groups, _, width = operands[0].shape
    operands = [place, *operands] + ([] if out is None else [out])
    any_spec = pl.BlockSpec(memory_space=pl.ANY)
    pieces = len(operands) - 1 - (out is not None)
    held = operands[1].shape if pieces == 1 else (pieces,) + operands[1].shape
    sems = pltpu.SemaphoreType.DMA((groups if pieces == 1 else pieces,))
    return pl.pallas_call(
        functools.partial(kernel, chunk=chunk, n_seq=n_seq),
        in_specs=[pl.BlockSpec(memory_space=pltpu.SMEM)] + [any_spec] * (len(operands) - 1),
        out_specs=any_spec,
        out_shape=jax.ShapeDtypeStruct((groups * n_seq, tokens, width), jnp.bfloat16),
        scratch_shapes=[pltpu.VMEM(held, jnp.bfloat16), sems, sems],
        input_output_aliases={} if out is None else {len(operands) - 1: 0},
        cost_estimate=pl.CostEstimate(flops=groups * tokens * width, bytes_accessed=4 * groups * tokens * width, transcendentals=0),
    )(*operands)


def split_width(value, out_refs):
    width = out_refs[0].shape[1]
    for index, out_ref in enumerate(out_refs):
        out_ref[...] = value[:, index * width:(index + 1) * width].astype(out_ref.dtype)


def finish_y_kernel(x_ref, mixed_ref, bias_ref, *out_refs):
    split_width(x_ref[...].astype(jnp.float32) + mixed_ref[...].astype(jnp.float32) + bias_ref[...], out_refs)


def normalize(act):
    act = act.astype(jnp.float32)
    mean = act.mean(-1, keepdims=True)
    inv_std = lax.rsqrt((act * act).mean(-1, keepdims=True) - mean * mean + LN_EPS)
    return (act - mean) * inv_std, inv_std


def finish_dx_kernel(x_ref, a6_ref, cot_ref, *out_refs):
    x_hat, inv_std = normalize(x_ref[...])
    value_a6 = a6_ref[...].astype(jnp.float32)
    mean_a6 = value_a6.mean(-1, keepdims=True)
    mean_a6x = (value_a6 * x_hat).mean(-1, keepdims=True)
    split_width(cot_ref[...].astype(jnp.float32) + inv_std * (value_a6 - mean_a6 - x_hat * mean_a6x), out_refs)


def row_call(kernel, parts, index, rows, *operands):
    width = operands[0].shape[1]
    specs = [pl.BlockSpec((min(rows, op.shape[0]), width), lambda s, i=(index if op.shape[0] > rows else 0): (i, 0)) for op in operands]
    return pl.pallas_call(
        kernel,
        grid=(1,),
        in_specs=specs,
        out_specs=[pl.BlockSpec((rows, width // parts), lambda s: (0, 0))] * parts,
        out_shape=[jax.ShapeDtypeStruct((rows, width // parts), jnp.bfloat16)] * parts,
        compiler_params=pltpu.CompilerParams(vmem_limit_bytes=16 * MIB),
        cost_estimate=pl.CostEstimate(flops=16 * rows * width, bytes_accessed=8 * rows * width, transcendentals=0),
    )(*operands)


def sublane_sum(value):
    return value.reshape(value.shape[0] // 8, 8, value.shape[1]).sum(0)


def norm_kernel(x_ref, small_ref, h_attn_ref, h_mlp_ref):
    @pl.loop(0, x_ref.shape[0] // LN_ROWS)
    def _(step):
        at = pl.ds(pl.multiple_of(step * LN_ROWS, LN_ROWS), LN_ROWS)
        x_hat, _ = normalize(x_ref[at, :])
        h_attn_ref[at, :] = (x_hat * small_ref[0:1, :] + small_ref[1:2, :]).astype(jnp.bfloat16)
        h_mlp_ref[at, :] = (x_hat * small_ref[2:3, :] + small_ref[3:4, :]).astype(jnp.bfloat16)


def offsets(refs, axis):
    starts = [0]
    for ref in refs:
        starts.append(starts[-1] + ref.shape[axis])
    return list(zip(refs, starts, starts[1:]))


def front_kernel(h_attn_ref, h_mlp_ref, cos_ref, lo_ref, hi_ref, b_qkv_ref, b_up_ref, *refs):
    w_refs, (qkv_ref, pre_ref, gelu_ref) = refs[:-3], refs[-3:]
    qkv_width = qkv_ref.shape[1]
    head = qkv_width // 3

    def project(h_ref, cols):
        return sum(dot(h_ref[:, start:stop], w_ref[:, cols], NN) for w_ref, start, stop in offsets(w_refs, 0))

    for low in range(0, qkv_width, head):
        at = slice(low, low + head)
        part = (project(h_attn_ref, at) + b_qkv_ref[:, at]).astype(jnp.bfloat16)
        if low < 2 * head:
            part = rotate(part.astype(jnp.float32), cos_ref[...], lo_ref[...], hi_ref[...], head // ROTARY_DIVISOR // 2, 1.0).astype(jnp.bfloat16)
        qkv_ref[:, at] = part
    for low in range(0, pre_ref.shape[1], TILE):
        at = slice(low, low + TILE)
        pre = (project(h_mlp_ref, slice(qkv_width + low, qkv_width + low + TILE)) + b_up_ref[:, at]).astype(jnp.bfloat16)
        pre_ref[:, at] = pre
        wide = pre.astype(jnp.float32)
        gelu_ref[:, at] = (0.5 * wide * (1.0 + lax.erf(wide * SQRT_HALF))).astype(jnp.bfloat16)


def y_kernel(ctx_ref, gelu_ref, *refs):
    w_refs, y_ref = refs[:-1], refs[-1]
    head = ctx_ref.shape[1]
    places, _, own, _ = y_ref.shape
    for w_ref, start, stop in offsets(w_refs, 1):
        acc = dot(ctx_ref[...], w_ref[:head, :], NN) + dot(gelu_ref[...], w_ref[head:, :], NN)
        y_ref[:, 0, :, start:stop] = acc.astype(jnp.bfloat16).reshape(places, own, stop - start)


def d_pre_kernel(cot_ref, pre_ref, *refs):
    w_refs, (d_ctx_ref, d_pre_ref, d_bias_ref) = refs[:-3], refs[-3:]

    def back(low, high):
        return sum(dot(cot_ref[:, start:stop], w_ref[low:high, :], NT) for w_ref, start, stop in offsets(w_refs, 1)).astype(jnp.bfloat16)

    head = d_ctx_ref.shape[1]

    @pl.when(pl.program_id(0) == 0)
    def _():
        d_bias_ref[...] = jnp.zeros(d_bias_ref.shape, jnp.float32)

    d_ctx_ref[...] = back(0, head)
    for low in range(0, d_pre_ref.shape[1], TILE):
        at = slice(low, low + TILE)
        d_gelu = back(head + low, head + low + TILE).astype(jnp.float32)
        pre = pre_ref[:, at].astype(jnp.float32)
        slope = 0.5 * (1.0 + lax.erf(pre * SQRT_HALF)) + pre * (jnp.exp(-0.5 * pre * pre) * INV_SQRT_2PI)
        d_pre = (d_gelu * slope).astype(jnp.bfloat16)
        d_pre_ref[:, at] = d_pre
        d_bias_ref[:, at] += sublane_sum(d_pre.astype(jnp.float32))


def d_h_kernel(d_qkv_ref, d_pre_ref, x_ref, small_ref, *refs):
    w_refs, (a6_ref, sums_ref) = refs[:-2], refs[-2:]
    qkv_width = d_qkv_ref.shape[1]

    @pl.when(pl.program_id(0) == 0)
    def _():
        sums_ref[...] = jnp.zeros(sums_ref.shape, jnp.float32)

    x_float = x_ref[...].astype(jnp.float32)
    mean = x_float.mean(-1, keepdims=True)
    inv_std = lax.rsqrt((x_float * x_float).mean(-1, keepdims=True) - mean * mean + LN_EPS)
    for w_ref, start, stop in offsets(w_refs, 0):
        for low in range(0, stop - start, TILE):
            part = slice(low, min(low + TILE, stop - start))
            at = slice(start + part.start, start + part.stop)
            d_attn = dot(d_qkv_ref[...], w_ref[part, :qkv_width], NT).astype(jnp.bfloat16).astype(jnp.float32)
            d_mlp = dot(d_pre_ref[...], w_ref[part, qkv_width:], NT).astype(jnp.bfloat16).astype(jnp.float32)
            a6_ref[:, at] = (d_attn * small_ref[0:1, at] + d_mlp * small_ref[2:3, at]).astype(jnp.bfloat16)
            x_hat = (x_ref[:, at].astype(jnp.float32) - mean) * inv_std
            sums_ref[0, :, at] += sublane_sum(d_attn * x_hat)
            sums_ref[1, :, at] += sublane_sum(d_attn)
            sums_ref[2, :, at] += sublane_sum(d_mlp * x_hat)
            sums_ref[3, :, at] += sublane_sum(d_mlp)


def tile_call(kernel, tiled, whole, outs, row_range, flops, rows=512):
    start, count = row_range
    rows = next(r for r in (rows, 256, 128, 64, count) if count % r == 0 and all(op.shape[0] % r == 0 for op in tiled))
    first = start // rows

    def tile_spec(op):
        blocks = op.shape[0] // rows
        if blocks * rows < count:
            return pl.BlockSpec((rows, op.shape[1]), lambda s: (lax.rem(s, blocks), 0))
        return pl.BlockSpec((rows, op.shape[1]), lambda s, f=(first if op.shape[0] != count else 0): (s + f, 0))

    in_specs = [tile_spec(op) for op in tiled]
    in_specs += [pl.BlockSpec(op.shape, lambda s, n=op.ndim: (0,) * n, pipeline_mode=pl.Buffered(1)) for op in whole]
    out_specs, out_shapes = [], []
    for form, dtype in outs:
        if isinstance(form, int):
            out_specs.append(pl.BlockSpec((rows, form), lambda s: (s, 0)))
            out_shapes.append(jax.ShapeDtypeStruct((count, form), dtype))
        elif isinstance(form[0], tuple):
            out_specs.append(pl.BlockSpec(form[1], form[2]))
            out_shapes.append(jax.ShapeDtypeStruct(form[0], dtype))
        else:
            out_specs.append(pl.BlockSpec(form, lambda s, n=len(form): (0,) * n))
            out_shapes.append(jax.ShapeDtypeStruct(form, dtype))
    moved = sum(2 * op.shape[1] * count for op in tiled) + sum(2 * op.size for op in whole) + sum(2 * shape.size for shape in out_shapes)
    return pl.pallas_call(
        kernel,
        grid=(count // rows,),
        in_specs=in_specs,
        out_specs=out_specs,
        out_shape=out_shapes,
        compiler_params=pltpu.CompilerParams(dimension_semantics=("arbitrary",), vmem_limit_bytes=60 * MIB),
        cost_estimate=pl.CostEstimate(flops=flops, bytes_accessed=moved, transcendentals=0),
    )(*tiled, *whole)


def solution(mesh):
    tx_size, ty_size = mesh.shape['tx'], mesh.shape['ty']
    act_spec = P('dp', None, 'tx')
    width_spec = P('tx')
    in_specs = (act_spec, act_spec, width_spec, width_spec, width_spec, width_spec, P('tx', 'ty', None), P('ty', None), P('ty', 'tx'), width_spec, P('tx', 'ty'), P('ty'), P('ty', 'tx'), width_spec)
    width_out = P(('dp', 'tx'))
    out_specs = (act_spec, act_spec, width_out, width_out, width_out, width_out, P(('dp', 'tx'), 'ty', None), P(('dp', 'ty'), None), P(('dp', 'ty'), 'tx'), width_out, P(('dp', 'tx'), 'ty'), P(('dp', 'ty')), P(('dp', 'ty'), 'tx'), width_out)
    antipode = tx_size // 2

    def shift(value, hops):
        return lax.ppermute(value, 'tx', [(s, (s - hops) % tx_size) for s in range(tx_size)])

    def small_sum(value, axis, size):
        step = 1
        while step < size:
            value = value + lax.ppermute(value, axis, [(s, s ^ step) for s in range(size)])
            step *= 2
        return value

    def along(value, hops):
        return lax.ppermute(value, 'ty', [(s, (s - 2 * hops) % ty_size) for s in range(ty_size)])

    def partner(value):
        return lax.ppermute(value, 'ty', [(s, s ^ 1) for s in range(ty_size)])

    def ring_gather(block, axis):
        blocks = {0: [block]}
        for hops in range(1, antipode):
            blocks[hops] = [shift(blocks[hops - 1][0], 1)]
            blocks[tx_size - hops] = [shift(blocks[(tx_size - hops + 1) % tx_size][0], -1)]
        half = block.shape[axis] // 2
        low = lax.slice_in_dim(blocks[antipode - 1][0], 0, half, axis=axis)
        high = lax.slice_in_dim(blocks[antipode + 1][0], half, 2 * half, axis=axis)
        blocks[antipode] = [shift(low, 1), shift(high, -1)]
        return [piece for r in range(tx_size) for piece in blocks[r]]

    def ring_scatter(make_part, rows):
        half = rows // 2
        far = make_part(antipode).astype(jnp.bfloat16)
        moving_up, moving_down = shift(far[:half], -1), shift(far[half:], 1)
        moving_up = jnp.pad(moving_up, ((0, rows - half), (0, 0)))
        moving_down = jnp.pad(moving_down, ((half, 0), (0, 0)))
        for hops in range(antipode - 1, 0, -1):
            up = make_part(hops) + moving_up.astype(jnp.float32)
            down = make_part(tx_size - hops) + moving_down.astype(jnp.float32)
            up, down = up.astype(jnp.bfloat16), down.astype(jnp.bfloat16)
            moving_up, moving_down = shift(up, -1), shift(down, 1)
        return lambda own, low, high: own + moving_up[low:high].astype(jnp.float32) + moving_down[low:high].astype(jnp.float32)

    def body(x_act, cot_out, ln1_gain, ln1_bias, ln2_gain, ln2_bias, w_qkv, b_qkv, w_dense, b_dense, w_up, b_up, w_down, b_down):
        batch, seq_len, d_local = x_act.shape
        n_seq = batch // tx_size
        own = seq_len // ty_size
        row, col = lax.axis_index('tx'), lax.axis_index('ty')
        qkv_width = w_qkv.shape[1] * w_qkv.shape[2]
        head = qkv_width // 3
        chunks = range(n_seq)
        tables = rotary_tables(seq_len, head // ROTARY_DIVISOR)
        attn_fwd, attn_bwd = attention_calls(n_seq, seq_len, head, tables)

        def to_tokens(act):
            parts = act.reshape(tx_size, n_seq, ty_size, own, d_local)
            pick = lambda index: lax.dynamic_slice(parts, (index, 0, col, 0, 0), (1, n_seq, 1, own, d_local)).reshape(n_seq, own, d_local)
            blocks = [pick(row)] + [shift(pick((row - r) % tx_size), r) for r in range(1, tx_size)]
            return jnp.concatenate(blocks, axis=2)

        place = jnp.stack([row, col // 2, col % 2])

        def to_width(parts):
            return jnp.stack([parts[0]] + [shift(parts[r], -r) for r in range(1, tx_size)])

        line = lax.broadcasted_iota(jnp.int32, (8, d_local), 0)
        small = jnp.zeros((8, d_local), jnp.bfloat16)
        for index, vector in enumerate((ln1_gain, ln1_bias, ln2_gain, ln2_bias, b_dense, b_down)):
            small = jnp.where(line == index, vector[None, :], small)
        small = [small] + [shift(small, r) for r in range(1, tx_size)]
        small = jnp.concatenate(small, axis=1).astype(jnp.float32)
        bias_out = small[4] + small[5]
        x_own = to_tokens(x_act)
        cot_own = to_tokens(cot_out)
        x_group = lax.all_gather(x_own, 'ty', axis=1, tiled=True)
        cot_group = lax.all_gather(cot_own, 'ty', axis=1, tiled=True)
        x_group, cot_group = x_group.reshape(n_seq * seq_len, -1), cot_group.reshape(n_seq * seq_len, -1)
        w_in = jnp.concatenate([w_qkv.reshape(d_local, qkv_width), w_up], axis=1)
        w_in = ring_gather(w_in, 0)
        w_back = jnp.concatenate([w_dense, w_down], axis=0)
        w_back = ring_gather(w_back, 1)
        in_size, back_size = sum(w.size for w in w_in), sum(w.size for w in w_back)

        n_tok, d_model = x_group.shape
        x_rows, cot_rows = x_own.reshape(-1, d_model), cot_own.reshape(-1, d_model)
        ff_width = w_up.shape[1]
        h_attn, h_mlp = tile_call(norm_kernel, [x_group], [small], [(d_model, jnp.bfloat16), (d_model, jnp.bfloat16)], (0, n_tok), 16 * x_group.size)
        qkv_act, pre_act, gelu_out = tile_call(
            front_kernel, [h_attn, h_mlp, *tables], [b_qkv.reshape(1, -1).astype(jnp.float32), b_up.reshape(1, -1).astype(jnp.float32), *w_in],
            [(qkv_width, jnp.bfloat16), (ff_width, jnp.bfloat16), (ff_width, jnp.bfloat16)], (0, n_tok), 2 * n_tok * in_size)
        qkv_seq = qkv_act.reshape(n_seq, seq_len, qkv_width)
        context = attn_fwd(qkv_seq).reshape(n_tok, head)
        blocks_per_seq = ty_size // 2
        y_form = ((ty_size, n_seq, own, d_model), (2, 1, own, d_model), lambda s: (lax.rem(s, blocks_per_seq), s // blocks_per_seq, 0, 0))
        (y_part,) = tile_call(y_kernel, [context, gelu_out], w_back, [(y_form, jnp.bfloat16)], (0, n_tok), 2 * n_tok * back_size, 2 * own)
        mixed = lax.psum_scatter(y_part.reshape(n_tok, d_model), 'ty', scatter_dimension=0, tiled=True)
        blocks = to_width(row_call(finish_y_kernel, tx_size, 0, n_seq * own, x_rows, mixed, bias_out.reshape(1, -1)))
        full = lax.all_gather(blocks.reshape(tx_size * n_seq, own, d_local), 'ty', axis=1, tiled=True)
        y_out = place_call(place_kernel, place, [full.reshape(tx_size, n_seq * seq_len, d_local)], None, 0, 1, n_seq * seq_len)

        d_ctx, d_pre, d_b_up = tile_call(
            d_pre_kernel, [cot_group, pre_act], w_back,
            [(head, jnp.bfloat16), (ff_width, jnp.bfloat16), ((8, ff_width), jnp.float32)], (0, n_tok), 2 * n_tok * back_size)
        d_ctx, d_b_up = d_ctx.reshape(n_seq, seq_len, head), d_b_up.sum(0)
        d_qkv, d_b_qkv, d_ln, dx_act = [], [], [], None
        for s in chunks:
            d_qkv_seq, d_b_seq = attn_bwd(qkv_seq, d_ctx, s)
            d_qkv.append(d_qkv_seq.reshape(seq_len, qkv_width))
            d_b_qkv.append(d_b_seq.sum((0, 1)))
            a6_part, sums = tile_call(
                d_h_kernel, [d_qkv[s], d_pre, x_group], [small, *w_in],
                [(d_model, jnp.bfloat16), ((4, 8, d_model), jnp.float32)], (s * seq_len, seq_len), 2 * seq_len * in_size)
            d_ln.append(sums)
            value_a6 = lax.psum_scatter(a6_part, 'ty', scatter_dimension=0, tiled=True)
            parts = row_call(finish_dx_kernel, tx_size, s, own, x_rows, value_a6, cot_rows)
            block = to_width(parts)
            if s < n_seq - 1:
                blocks = [block] + [along(block, hops) for hops in range(1, ty_size // 2)]
                blocks = blocks + [partner(piece) for piece in blocks]
                dx_act = place_call(place_pieces_kernel, place, blocks, dx_act, s, n_seq, seq_len)
            else:
                full = lax.all_gather(block, 'ty', axis=1, tiled=True)
                dx_act = place_call(place_kernel, place, [full], dx_act, s, n_seq, seq_len)
        d_qkv = jnp.concatenate(d_qkv, axis=0)

        d_ln = sum(d_ln).sum(1).reshape(4, tx_size, d_local)
        d_bias = jnp.concatenate([sum(d_b_qkv), d_b_up]).reshape(4, -1)
        sent = [jnp.concatenate([d_ln[:, r], d_bias], axis=1) for r in range(tx_size)]
        got = [sent[0]] + [shift(sent[r], -r) for r in range(1, tx_size)]
        got = sum(got[r] + got[r + antipode] for r in range(antipode))
        d_bias = got[:, d_local:].reshape(-1)
        d_ln = small_sum(got[:, :d_local], 'ty', ty_size)
        d_b_out = cot_out.astype(jnp.float32).sum((0, 1))

        cols = lambda act, r: act[:, r * d_local:(r + 1) * d_local]
        inner = jnp.concatenate([context, gelu_out], axis=1)
        add_back = ring_scatter(lambda r: dot(inner, cols(cot_group, r), TN), inner.shape[1])
        add_up = ring_scatter(lambda r: dot(cols(h_mlp, r), d_pre, TN), d_local)
        add_qkv = ring_scatter(lambda r: dot(cols(h_attn, r), d_qkv, TN), d_local)
        d_w_dense = add_back(dot(context, cols(cot_group, 0), TN), 0, head)
        d_w_down = add_back(dot(gelu_out, cols(cot_group, 0), TN), head, inner.shape[1])
        d_w_up = add_up(dot(cols(h_mlp, 0), d_pre, TN), 0, d_local)
        d_w_qkv = add_qkv(dot(cols(h_attn, 0), d_qkv, TN), 0, d_local)
        y_out = y_out.reshape(batch, seq_len, d_local)
        return (y_out, dx_act, d_ln[0], d_ln[1], d_ln[2], d_ln[3], d_w_qkv.reshape(w_qkv.shape), d_bias[:qkv_width].reshape(b_qkv.shape), d_w_dense, d_b_out, d_w_up, d_bias[qkv_width:], d_w_down, d_b_out)

    return jax.shard_map(body, mesh=mesh, in_specs=in_specs, out_specs=out_specs, check_vma=False)
```

```python
import functools
import jax
import jax.numpy as jnp
from jax import lax
from jax.experimental import pallas as pl
from jax.experimental.pallas import tpu as pltpu
from jax.sharding import PartitionSpec as P


LN_EPS = 1e-5
ROPE_BASE = 10000.0
ROTARY_DIVISOR = 4
LANES = 128
Q_ROWS = 256
LN_ROWS = 64
MIB = 1024 * 1024
TILE = 256
SQRT_HALF = 0.5 ** 0.5
INV_SQRT_2PI = 0.3989422804014327

NT = (((1,), (1,)), ((), ()))
TN = (((0,), (0,)), ((), ()))
NN = (((1,), (0,)), ((), ()))


def dot(a, b, dims):
    return lax.dot_general(a, b, dims, preferred_element_type=jnp.float32)


def rotary_tables(seq_len, rot_dim):
    half = rot_dim // 2
    lane = jnp.arange(LANES)
    freq_index = jnp.where(lane < half, lane, lane - half)
    inv_freq = ROPE_BASE ** (-(2 * freq_index).astype(jnp.float32) / rot_dim)
    angles = jnp.arange(seq_len, dtype=jnp.float32)[:, None] * inv_freq[None, :]
    inside = (lane < rot_dim)[None, :]
    cos_tab = jnp.where(inside, jnp.cos(angles), 1.0)
    sin = jnp.where(inside, jnp.sin(angles), 0.0)
    first = (lane < half)[None, :]
    return cos_tab, jnp.where(first, -sin, 0.0), jnp.where(first, 0.0, sin)


def rotate(part, cos_tab, sin_lo, sin_hi, half, sign):
    head = part[:, :LANES]
    forward = pltpu.roll(head, half, 1)
    backward = pltpu.roll(head, LANES - half, 1)
    mixed = head * cos_tab + sign * (backward * sin_lo + forward * sin_hi)
    return jnp.concatenate([mixed, part[:, LANES:]], axis=1)


def causal_probs(q_rows, keys, row_start, scale):
    scores = dot(q_rows, keys, NT) * scale
    rows = row_start + lax.broadcasted_iota(jnp.int32, scores.shape, 0)
    cols = lax.broadcasted_iota(jnp.int32, scores.shape, 1)
    scores = jnp.where(rows >= cols, scores, -1e30)
    exps = jnp.exp(scores - jnp.max(scores, axis=1, keepdims=True))
    return exps * (1.0 / jnp.sum(exps, axis=1, keepdims=True))


def attn_fwd_kernel(qkv_ref, ctx_ref, *, scale, span):
    seq_len, width = ctx_ref.shape[1:]
    for end in range(span, seq_len + 1, span):
        @pl.loop(0, span // Q_ROWS)
        def _(step, end=end):
            start = pl.multiple_of(end - span + step * Q_ROWS, Q_ROWS)
            rows = pl.ds(start, Q_ROWS)
            probs = causal_probs(qkv_ref[0, rows, :width], qkv_ref[0, :end, width:2 * width], start, scale).astype(jnp.bfloat16)
            ctx_ref[0, rows, :] = dot(probs, qkv_ref[0, :end, 2 * width:], NN).astype(jnp.bfloat16)


def attn_bwd_kernel(qkv_ref, dctx_ref, cos_ref, lo_ref, hi_ref, dqkv_ref, db_ref, dk_ref, dv_ref, *, half, scale, span):
    seq_len, width = dctx_ref.shape[1:]
    dk_ref[...] = jnp.zeros(dk_ref.shape, jnp.float32)
    dv_ref[...] = jnp.zeros(dv_ref.shape, jnp.float32)
    db_ref[...] = jnp.zeros(db_ref.shape, jnp.float32)

    def store(rows, col, grad_rot, turn):
        grad = grad_rot.astype(jnp.bfloat16)
        if turn:
            wide = grad.astype(jnp.float32)
            grad = rotate(wide, cos_ref[rows, :], lo_ref[rows, :], hi_ref[rows, :], half, -1.0).astype(jnp.bfloat16)
        dqkv_ref[0, rows, col:col + width] = grad
        db_ref[0, :, col:col + width] += sublane_sum(grad.astype(jnp.float32))

    for end in range(span, seq_len + 1, span):
        @pl.loop(0, span // Q_ROWS)
        def _(step, end=end):
            start = pl.multiple_of(end - span + step * Q_ROWS, Q_ROWS)
            rows = pl.ds(start, Q_ROWS)
            q_rows, keys = qkv_ref[0, rows, :width], qkv_ref[0, :end, width:2 * width]
            dctx = dctx_ref[0, rows, :]
            probs = causal_probs(q_rows, keys, start, scale)
            dprobs = dot(dctx, qkv_ref[0, :end, 2 * width:], NT).astype(jnp.bfloat16).astype(jnp.float32)
            dv_ref[:end, :] += dot(probs.astype(jnp.bfloat16), dctx, TN)
            inner = jnp.sum(probs * dprobs, axis=1, keepdims=True)
            dscores = (probs * (dprobs - inner) * scale).astype(jnp.bfloat16)
            dk_ref[:end, :] += dot(dscores, q_rows, TN)
            store(rows, 0, dot(dscores, keys, NN), True)

    @pl.loop(0, seq_len // Q_ROWS)
    def _(step):
        rows = pl.ds(pl.multiple_of(step * Q_ROWS, Q_ROWS), Q_ROWS)
        store(rows, width, dk_ref[rows, :], True)
        store(rows, 2 * width, dv_ref[rows, :], False)


def attention_calls(n_seq, seq_len, width, tables):
    half = width // ROTARY_DIVISOR // 2
    scale = width ** -0.5
    span = 512 if seq_len % 512 == 0 else seq_len
    seq_spec = lambda cols, first=0: pl.BlockSpec((1, seq_len, cols), lambda s: (s + first, 0, 0))
    tab_spec = pl.BlockSpec((seq_len, LANES), lambda s: (0, 0))
    acc_scratch = pltpu.VMEM((seq_len, width), jnp.float32)
    pairs = seq_len * seq_len // 2
    params = pltpu.CompilerParams(dimension_semantics=("arbitrary",), vmem_limit_bytes=60 * MIB)

    def forward(qkv):
        return pl.pallas_call(
            functools.partial(attn_fwd_kernel, scale=scale, span=span),
            grid=(n_seq,),
            in_specs=[seq_spec(3 * width)],
            out_specs=seq_spec(width),
            out_shape=jax.ShapeDtypeStruct((n_seq, seq_len, width), jnp.bfloat16),
            compiler_params=params,
            name="af",
            cost_estimate=pl.CostEstimate(flops=8 * n_seq * pairs * width, bytes_accessed=8 * n_seq * seq_len * width, transcendentals=n_seq * pairs),
        )(qkv)

    def backward(qkv, dctx, index):
        return pl.pallas_call(
            functools.partial(attn_bwd_kernel, half=half, scale=scale, span=span),
            grid=(1,),
            in_specs=[seq_spec(3 * width, index), seq_spec(width, index), tab_spec, tab_spec, tab_spec],
            out_specs=[seq_spec(3 * width), pl.BlockSpec((1, 8, 3 * width), lambda s: (s, 0, 0))],
            out_shape=[jax.ShapeDtypeStruct((1, seq_len, 3 * width), jnp.bfloat16), jax.ShapeDtypeStruct((1, 8, 3 * width), jnp.float32)],
            scratch_shapes=[acc_scratch, acc_scratch],
            compiler_params=params,
            name="ab",
            cost_estimate=pl.CostEstimate(flops=20 * pairs * width, bytes_accessed=14 * seq_len * width, transcendentals=pairs),
        )(qkv, dctx, *tables)

    return forward, backward


def place_kernel(place_ref, full_ref, *rest, chunk, n_seq):
    out_ref, held_ref, in_sems, out_sems = rest[-4:]
    groups = full_ref.shape[0]
    fetch = [pltpu.make_async_copy(full_ref.at[lax.rem(place_ref[0] + groups - t, groups)], held_ref.at[t], in_sems.at[t]) for t in range(groups)]
    store = [pltpu.make_async_copy(held_ref.at[t], out_ref.at[t * n_seq + chunk], out_sems.at[t]) for t in range(groups)]
    for copy in fetch:
        copy.start()
    for t in range(groups):
        fetch[t].wait()
        store[t].start()
    for copy in store:
        copy.wait()


def place_pieces_kernel(place_ref, *refs, spans, n_seq):
    out_ref, held_ref, in_sems, out_sems = refs[-4:]
    row, column, core = place_ref[0], place_ref[1], place_ref[2]
    groups, columns = out_ref.shape[0] // n_seq, out_ref.shape[1] // refs[0].shape[1] // 2
    own = refs[0].shape[1]
    fetch, store, low = [], [], 0
    for index, (distance, other, first) in enumerate(spans):
        count = refs[index].shape[0]
        source = 2 * lax.rem(column + distance, columns) + (1 - core if other else core)
        at = pl.ds(pl.multiple_of(source * own, own), own)
        fetch.append(pltpu.make_async_copy(refs[index], held_ref.at[pl.ds(low, count)], in_sems.at[index]))
        stores = []
        for place in range(count // n_seq):
            to = lax.rem(row + groups - first - place, groups) * n_seq
            stores.append(pltpu.make_async_copy(held_ref.at[pl.ds(low + place * n_seq, n_seq)], out_ref.at[pl.ds(to, n_seq), at], out_sems.at[index]))
        store.append(stores)
        low += count
    for copy in fetch:
        copy.start()
    for index, stores in enumerate(store):
        fetch[index].wait()
        for copy in stores:
            copy.start()
    for stores in store:
        for copy in stores:
            copy.wait()


def place_call(kernel, place, operands, out, shape, held, n_sems):
    operands = [place, *operands] + ([] if out is None else [out])
    any_spec = pl.BlockSpec(memory_space=pl.ANY)
    size = held[0] * held[1] * held[2]
    sems = pltpu.SemaphoreType.DMA((n_sems,))
    return pl.pallas_call(
        kernel,
        in_specs=[pl.BlockSpec(memory_space=pltpu.SMEM)] + [any_spec] * (len(operands) - 1),
        out_specs=any_spec,
        out_shape=jax.ShapeDtypeStruct(shape, jnp.bfloat16),
        scratch_shapes=[pltpu.VMEM(held, jnp.bfloat16), sems, sems],
        input_output_aliases={} if out is None else {len(operands) - 1: 0},
        cost_estimate=pl.CostEstimate(flops=size, bytes_accessed=4 * size, transcendentals=0),
    )(*operands)


def split_width(value, out_refs):
    width = out_refs[0].shape[1]
    for index, out_ref in enumerate(out_refs):
        out_ref[...] = value[:, index * width:(index + 1) * width].astype(out_ref.dtype)


def finish_y_kernel(x_ref, mixed_ref, bias_ref, *out_refs):
    split_width(x_ref[...].astype(jnp.float32) + mixed_ref[...].astype(jnp.float32) + bias_ref[...], out_refs)


def normalize(act):
    act = act.astype(jnp.float32)
    mean = act.mean(-1, keepdims=True)
    inv_std = lax.rsqrt((act * act).mean(-1, keepdims=True) - mean * mean + LN_EPS)
    return (act - mean) * inv_std, inv_std


def finish_dx_kernel(x_ref, a6_ref, cot_ref, *out_refs):
    x_hat, inv_std = normalize(x_ref[...])
    value_a6 = a6_ref[...].astype(jnp.float32)
    mean_a6 = value_a6.mean(-1, keepdims=True)
    mean_a6x = (value_a6 * x_hat).mean(-1, keepdims=True)
    split_width(cot_ref[...].astype(jnp.float32) + inv_std * (value_a6 - mean_a6 - x_hat * mean_a6x), out_refs)


def row_call(kernel, parts, index, rows, *operands):
    width = operands[0].shape[1]
    specs = [pl.BlockSpec((min(rows, op.shape[0]), width), lambda s, i=(index if op.shape[0] > rows else 0): (i, 0)) for op in operands]
    return pl.pallas_call(
        kernel,
        grid=(1,),
        in_specs=specs,
        out_specs=[pl.BlockSpec((rows, width // parts), lambda s: (0, 0))] * parts,
        out_shape=[jax.ShapeDtypeStruct((rows, width // parts), jnp.bfloat16)] * parts,
        compiler_params=pltpu.CompilerParams(vmem_limit_bytes=16 * MIB),
        cost_estimate=pl.CostEstimate(flops=16 * rows * width, bytes_accessed=8 * rows * width, transcendentals=0),
    )(*operands)


def sublane_sum(value):
    return value.reshape(value.shape[0] // 8, 8, value.shape[1]).sum(0)


def norm_kernel(x_ref, small_ref, h_attn_ref, h_mlp_ref):
    @pl.loop(0, x_ref.shape[0] // LN_ROWS)
    def _(step):
        at = pl.ds(pl.multiple_of(step * LN_ROWS, LN_ROWS), LN_ROWS)
        x_hat, _ = normalize(x_ref[at, :])
        h_attn_ref[at, :] = (x_hat * small_ref[0:1, :] + small_ref[1:2, :]).astype(jnp.bfloat16)
        h_mlp_ref[at, :] = (x_hat * small_ref[2:3, :] + small_ref[3:4, :]).astype(jnp.bfloat16)


def offsets(refs, axis):
    starts = [0]
    for ref in refs:
        starts.append(starts[-1] + ref.shape[axis])
    return list(zip(refs, starts, starts[1:]))


def front_kernel(h_attn_ref, h_mlp_ref, cos_ref, lo_ref, hi_ref, b_qkv_ref, b_up_ref, *refs):
    w_refs, (qkv_ref, pre_ref, gelu_ref) = refs[:-3], refs[-3:]
    qkv_width = qkv_ref.shape[1]
    head = qkv_width // 3

    def project(h_ref, cols):
        return sum(dot(h_ref[:, start:stop], w_ref[:, cols], NN) for w_ref, start, stop in offsets(w_refs, 0))

    for low in range(0, qkv_width, head):
        at = slice(low, low + head)
        part = (project(h_attn_ref, at) + b_qkv_ref[:, at]).astype(jnp.bfloat16)
        if low < 2 * head:
            part = rotate(part.astype(jnp.float32), cos_ref[...], lo_ref[...], hi_ref[...], head // ROTARY_DIVISOR // 2, 1.0).astype(jnp.bfloat16)
        qkv_ref[:, at] = part
    for low in range(0, pre_ref.shape[1], TILE):
        at = slice(low, low + TILE)
        pre = (project(h_mlp_ref, slice(qkv_width + low, qkv_width + low + TILE)) + b_up_ref[:, at]).astype(jnp.bfloat16)
        pre_ref[:, at] = pre
        wide = pre.astype(jnp.float32)
        gelu_ref[:, at] = (0.5 * wide * (1.0 + lax.erf(wide * SQRT_HALF))).astype(jnp.bfloat16)


def y_kernel(ctx_ref, gelu_ref, *refs):
    w_refs, y_ref = refs[:-1], refs[-1]
    head = ctx_ref.shape[1]
    places, _, own, _ = y_ref.shape
    for w_ref, start, stop in offsets(w_refs, 1):
        acc = dot(ctx_ref[...], w_ref[:head, :], NN) + dot(gelu_ref[...], w_ref[head:, :], NN)
        y_ref[:, 0, :, start:stop] = acc.astype(jnp.bfloat16).reshape(places, own, stop - start)


def d_pre_kernel(cot_ref, pre_ref, *refs):
    w_refs, (d_ctx_ref, d_pre_ref, d_bias_ref) = refs[:-3], refs[-3:]

    def back(low, high):
        return sum(dot(cot_ref[:, start:stop], w_ref[low:high, :], NT) for w_ref, start, stop in offsets(w_refs, 1)).astype(jnp.bfloat16)

    head = d_ctx_ref.shape[1]

    @pl.when(pl.program_id(0) == 0)
    def _():
        d_bias_ref[...] = jnp.zeros(d_bias_ref.shape, jnp.float32)

    d_ctx_ref[...] = back(0, head)
    for low in range(0, d_pre_ref.shape[1], TILE):
        at = slice(low, low + TILE)
        d_gelu = back(head + low, head + low + TILE).astype(jnp.float32)
        pre = pre_ref[:, at].astype(jnp.float32)
        slope = 0.5 * (1.0 + lax.erf(pre * SQRT_HALF)) + pre * (jnp.exp(-0.5 * pre * pre) * INV_SQRT_2PI)
        d_pre = (d_gelu * slope).astype(jnp.bfloat16)
        d_pre_ref[:, at] = d_pre
        d_bias_ref[:, at] += sublane_sum(d_pre.astype(jnp.float32))


def d_h_kernel(d_qkv_ref, d_pre_ref, x_ref, small_ref, *refs):
    w_refs, (a6_ref, sums_ref) = refs[:-2], refs[-2:]
    qkv_width = d_qkv_ref.shape[1]

    @pl.when(pl.program_id(0) == 0)
    def _():
        sums_ref[...] = jnp.zeros(sums_ref.shape, jnp.float32)

    x_float = x_ref[...].astype(jnp.float32)
    mean = x_float.mean(-1, keepdims=True)
    inv_std = lax.rsqrt((x_float * x_float).mean(-1, keepdims=True) - mean * mean + LN_EPS)
    for w_ref, start, stop in offsets(w_refs, 0):
        for low in range(0, stop - start, TILE):
            part = slice(low, min(low + TILE, stop - start))
            at = slice(start + part.start, start + part.stop)
            d_attn = dot(d_qkv_ref[...], w_ref[part, :qkv_width], NT).astype(jnp.bfloat16).astype(jnp.float32)
            d_mlp = dot(d_pre_ref[...], w_ref[part, qkv_width:], NT).astype(jnp.bfloat16).astype(jnp.float32)
            a6_ref[:, at] = (d_attn * small_ref[0:1, at] + d_mlp * small_ref[2:3, at]).astype(jnp.bfloat16)
            x_hat = (x_ref[:, at].astype(jnp.float32) - mean) * inv_std
            sums_ref[0, :, at] += sublane_sum(d_attn * x_hat)
            sums_ref[1, :, at] += sublane_sum(d_attn)
            sums_ref[2, :, at] += sublane_sum(d_mlp * x_hat)
            sums_ref[3, :, at] += sublane_sum(d_mlp)


def tile_call(kernel, tiled, whole, outs, row_range, flops, rows=512, total=None, into=()):
    start, count = row_range
    rows = next(r for r in (rows, 256, 128, 64, count) if count % r == 0 and all(op.shape[0] % r == 0 for op in tiled))
    first = start // rows

    def tile_spec(op):
        blocks = op.shape[0] // rows
        if blocks * rows < count or (total and op.shape[0] < total):
            return pl.BlockSpec((rows, op.shape[1]), lambda s: (lax.rem(s, blocks), 0))
        return pl.BlockSpec((rows, op.shape[1]), lambda s, f=(first if op.shape[0] != count else 0): (s + f, 0))

    in_specs = [tile_spec(op) for op in tiled]
    in_specs += [pl.BlockSpec(op.shape, lambda s, n=op.ndim: (0,) * n, pipeline_mode=pl.Buffered(1)) for op in whole]
    in_specs += [pl.BlockSpec(memory_space=pl.ANY)] * len(into)
    before = len(tiled) + len(whole)
    body = kernel if not into else lambda *refs: kernel(*refs[:before], *refs[before + len(into):])
    out_specs, out_shapes = [], []
    for form, dtype in outs:
        if isinstance(form, int):
            out_specs.append(pl.BlockSpec((rows, form), lambda s: (s + (first if total else 0), 0)))
            out_shapes.append(jax.ShapeDtypeStruct((total or count, form), dtype))
        elif isinstance(form[0], tuple):
            out_specs.append(pl.BlockSpec(form[1], form[2]))
            out_shapes.append(jax.ShapeDtypeStruct(form[0], dtype))
        else:
            out_specs.append(pl.BlockSpec(form, lambda s, n=len(form): (0,) * n))
            out_shapes.append(jax.ShapeDtypeStruct(form, dtype))
    moved = sum(2 * op.shape[1] * count for op in tiled) + sum(2 * op.size for op in whole) + sum(2 * shape.size for shape in out_shapes)
    return pl.pallas_call(
        body,
        grid=(count // rows,),
        in_specs=in_specs,
        out_specs=out_specs,
        out_shape=out_shapes,
        input_output_aliases={before + k: k for k in range(min(len(into), len(outs)))},
        compiler_params=pltpu.CompilerParams(dimension_semantics=("arbitrary",), vmem_limit_bytes=60 * MIB),
        cost_estimate=pl.CostEstimate(flops=flops, bytes_accessed=moved, transcendentals=0),
    )(*tiled, *whole, *into)


def solution(mesh):
    tx_size, ty_size = mesh.shape['tx'], mesh.shape['ty']
    act_spec = P('dp', None, 'tx')
    width_spec = P('tx')
    in_specs = (act_spec, act_spec, width_spec, width_spec, width_spec, width_spec, P('tx', 'ty', None), P('ty', None), P('ty', 'tx'), width_spec, P('tx', 'ty'), P('ty'), P('ty', 'tx'), width_spec)
    width_out = P(('dp', 'tx'))
    out_specs = (act_spec, act_spec, width_out, width_out, width_out, width_out, P(('dp', 'tx'), 'ty', None), P(('dp', 'ty'), None), P(('dp', 'ty'), 'tx'), width_out, P(('dp', 'tx'), 'ty'), P(('dp', 'ty')), P(('dp', 'ty'), 'tx'), width_out)
    antipode = tx_size // 2

    def shift(value, hops):
        return lax.ppermute(value, 'tx', [(s, (s - hops) % tx_size) for s in range(tx_size)])

    def small_sum(value, axis, size):
        step = 1
        while step < size:
            value = value + lax.ppermute(value, axis, [(s, s ^ step) for s in range(size)])
            step *= 2
        return value

    def along(value, hops):
        return lax.ppermute(value, 'ty', [(s, (s - 2 * hops) % ty_size) for s in range(ty_size)])

    def partner(value):
        return lax.ppermute(value, 'ty', [(s, s ^ 1) for s in range(ty_size)])

    def ring_gather(block, axis, move, size):
        far = size // 2
        blocks = {0: [block]}
        for hops in range(1, far):
            blocks[hops] = [move(blocks[hops - 1][0], 1)]
            blocks[size - hops] = [move(blocks[(size - hops + 1) % size][0], -1)]
        half = block.shape[axis] // 2
        low = lax.slice_in_dim(blocks[far - 1][0], 0, half, axis=axis)
        high = lax.slice_in_dim(blocks[far + 1][0], half, 2 * half, axis=axis)
        blocks[far] = [move(low, 1), move(high, -1)]
        return [blocks[r] for r in range(size)]

    def ring_scatter(make_part, rows):
        half = rows // 2
        far = make_part(antipode).astype(jnp.bfloat16)
        moving_up, moving_down = shift(far[:half], -1), shift(far[half:], 1)
        moving_up = jnp.pad(moving_up, ((0, rows - half), (0, 0)))
        moving_down = jnp.pad(moving_down, ((half, 0), (0, 0)))
        for hops in range(antipode - 1, 0, -1):
            up = make_part(hops) + moving_up.astype(jnp.float32)
            down = make_part(tx_size - hops) + moving_down.astype(jnp.float32)
            up, down = up.astype(jnp.bfloat16), down.astype(jnp.bfloat16)
            moving_up, moving_down = shift(up, -1), shift(down, 1)
        return lambda own, low, high: own + moving_up[low:high].astype(jnp.float32) + moving_down[low:high].astype(jnp.float32)

    def body(x_act, cot_out, ln1_gain, ln1_bias, ln2_gain, ln2_bias, w_qkv, b_qkv, w_dense, b_dense, w_up, b_up, w_down, b_down):
        batch, seq_len, d_local = x_act.shape
        n_seq = batch // tx_size
        own = seq_len // ty_size
        row, col = lax.axis_index('tx'), lax.axis_index('ty')
        qkv_width = w_qkv.shape[1] * w_qkv.shape[2]
        head = qkv_width // 3
        chunks = range(n_seq)
        tables = rotary_tables(seq_len, head // ROTARY_DIVISOR)
        attn_fwd, attn_bwd = attention_calls(n_seq, seq_len, head, tables)

        def to_tokens(act):
            parts = act.reshape(tx_size, n_seq, ty_size, own, d_local)
            pick = lambda index: lax.dynamic_slice(parts, (index, 0, col, 0, 0), (1, n_seq, 1, own, d_local)).reshape(n_seq, own, d_local)
            blocks = [pick(row)] + [shift(pick((row - r) % tx_size), r) for r in range(1, tx_size)]
            return jnp.concatenate(blocks, axis=2)

        place = jnp.stack([row, col // 2, col % 2])

        def to_width(parts):
            return jnp.stack([parts[0]] + [shift(parts[r], -r) for r in range(1, tx_size)])

        line = lax.broadcasted_iota(jnp.int32, (8, d_local), 0)
        small = jnp.zeros((8, d_local), jnp.bfloat16)
        for index, vector in enumerate((ln1_gain, ln1_bias, ln2_gain, ln2_bias, b_dense, b_down)):
            small = jnp.where(line == index, vector[None, :], small)
        small = [small] + [shift(small, r) for r in range(1, tx_size)]
        small = jnp.concatenate(small, axis=1).astype(jnp.float32)
        bias_out = small[4] + small[5]
        x_own = to_tokens(x_act)
        cot_own = to_tokens(cot_out)
        x_seqs = []
        for s in chunks:
            x_seqs.append(lax.all_gather(x_own[s], 'ty', axis=0, tiled=True))
        cot_group = lax.all_gather(cot_own, 'ty', axis=1, tiled=True)
        cot_group = cot_group.reshape(n_seq * seq_len, -1)
        w_in = jnp.concatenate([w_qkv.reshape(d_local, qkv_width), w_up], axis=1)
        w_in = sum(ring_gather(w_in, 0, shift, tx_size), [])
        w_back = jnp.concatenate([w_dense, w_down], axis=0)
        w_back = sum(ring_gather(w_back, 1, shift, tx_size), [])
        in_size, back_size = sum(w.size for w in w_in), sum(w.size for w in w_back)

        n_tok, d_model = cot_group.shape
        x_rows, cot_rows = x_own.reshape(-1, d_model), cot_own.reshape(-1, d_model)
        ff_width = w_up.shape[1]
        bias_rows = [b_qkv.reshape(1, -1).astype(jnp.float32), b_up.reshape(1, -1).astype(jnp.float32)]
        normed, front = (), ()
        for s in chunks:
            at = (s * seq_len, seq_len)
            normed = tile_call(
                norm_kernel, [x_seqs[s]], [small], [(d_model, jnp.bfloat16), (d_model, jnp.bfloat16)],
                at, 16 * x_seqs[s].size, total=n_tok, into=(*normed, *front[:1]))
            front = tile_call(
                front_kernel, [*normed, *tables], [*bias_rows, *w_in], [(qkv_width, jnp.bfloat16), (ff_width, jnp.bfloat16), (ff_width, jnp.bfloat16)],
                at, 2 * seq_len * in_size, total=n_tok, into=front)
        h_attn, h_mlp = normed
        qkv_act, pre_act, gelu_out = front
        qkv_seq = qkv_act.reshape(n_seq, seq_len, qkv_width)
        context = attn_fwd(qkv_seq).reshape(n_tok, head)
        blocks_per_seq = ty_size // 2
        y_form = ((ty_size, n_seq, own, d_model), (2, 1, own, d_model), lambda s: (lax.rem(s, blocks_per_seq), s // blocks_per_seq, 0, 0))
        (y_part,) = tile_call(y_kernel, [context, gelu_out], w_back, [(y_form, jnp.bfloat16)], (0, n_tok), 2 * n_tok * back_size, 2 * own)
        mixed = lax.psum_scatter(y_part.reshape(n_tok, d_model), 'ty', scatter_dimension=0, tiled=True)
        block = to_width(row_call(finish_y_kernel, tx_size, 0, n_seq * own, x_rows, mixed, bias_out.reshape(1, -1)))
        block = block.reshape(tx_size * n_seq, own, d_local)
        pieces, spans = [], []
        for distance, found in enumerate(ring_gather(block, 0, along, ty_size // 2)):
            for index, piece in enumerate(found):
                pieces += [piece, partner(piece)]
                spans += [(distance, other, index * (tx_size // 2)) for other in (0, 1)]
        y_out = place_call(
            functools.partial(place_pieces_kernel, spans=spans, n_seq=n_seq), place, pieces, None,
            (batch, seq_len, d_local), (batch * ty_size, own, d_local), len(spans))

        d_ctx, d_pre, d_b_up = tile_call(
            d_pre_kernel, [cot_group, pre_act], w_back,
            [(head, jnp.bfloat16), (ff_width, jnp.bfloat16), ((8, ff_width), jnp.float32)], (0, n_tok), 2 * n_tok * back_size)
        d_ctx, d_b_up = d_ctx.reshape(n_seq, seq_len, head), d_b_up.sum(0)
        d_qkv, d_b_qkv, d_ln, dx_act = [], [], [], None
        for s in chunks:
            d_qkv_seq, d_b_seq = attn_bwd(qkv_seq, d_ctx, s)
            d_qkv.append(d_qkv_seq.reshape(seq_len, qkv_width))
            d_b_qkv.append(d_b_seq.sum((0, 1)))
            a6_part, sums = tile_call(
                d_h_kernel, [d_qkv[s], d_pre, x_seqs[s]], [small, *w_in],
                [(d_model, jnp.bfloat16), ((4, 8, d_model), jnp.float32)], (s * seq_len, seq_len), 2 * seq_len * in_size)
            d_ln.append(sums)
            value_a6 = lax.psum_scatter(a6_part, 'ty', scatter_dimension=0, tiled=True)
            parts = row_call(finish_dx_kernel, tx_size, s, own, x_rows, value_a6, cot_rows)
            block = to_width(parts)
            full = lax.all_gather(block, 'ty', axis=1, tiled=True)
            dx_act = place_call(
                functools.partial(place_kernel, chunk=s, n_seq=n_seq), place, [full], dx_act,
                (batch, seq_len, d_local), full.shape, tx_size)
        d_qkv = jnp.concatenate(d_qkv, axis=0)

        d_ln = sum(d_ln).sum(1).reshape(4, tx_size, d_local)
        d_bias = jnp.concatenate([sum(d_b_qkv), d_b_up]).reshape(4, -1)
        sent = [jnp.concatenate([d_ln[:, r], d_bias], axis=1) for r in range(tx_size)]
        got = [sent[0]] + [shift(sent[r], -r) for r in range(1, tx_size)]
        got = sum(got[r] + got[r + antipode] for r in range(antipode))
        d_bias = got[:, d_local:].reshape(-1)
        d_ln = small_sum(got[:, :d_local], 'ty', ty_size)
        d_b_out = cot_out.astype(jnp.float32).sum((0, 1))

        cols = lambda act, r: act[:, r * d_local:(r + 1) * d_local]
        inner = jnp.concatenate([context, gelu_out], axis=1)
        add_back = ring_scatter(lambda r: dot(inner, cols(cot_group, r), TN), inner.shape[1])
        add_up = ring_scatter(lambda r: dot(cols(h_mlp, r), d_pre, TN), d_local)
        add_qkv = ring_scatter(lambda r: dot(cols(h_attn, r), d_qkv, TN), d_local)
        d_w_dense = add_back(dot(context, cols(cot_group, 0), TN), 0, head)
        d_w_down = add_back(dot(gelu_out, cols(cot_group, 0), TN), head, inner.shape[1])
        d_w_up = add_up(dot(cols(h_mlp, 0), d_pre, TN), 0, d_local)
        d_w_qkv = add_qkv(dot(cols(h_attn, 0), d_qkv, TN), 0, d_local)
        return (y_out, dx_act, d_ln[0], d_ln[1], d_ln[2], d_ln[3], d_w_qkv.reshape(w_qkv.shape), d_bias[:qkv_width].reshape(b_qkv.shape), d_w_dense, d_b_out, d_w_up, d_bias[qkv_width:], d_w_down, d_b_out)

    return jax.shard_map(body, mesh=mesh, in_specs=in_specs, out_specs=out_specs, check_vma=False)
```

```python
import functools
import jax
import jax.numpy as jnp
from jax import lax
from jax.experimental import pallas as pl
from jax.experimental.pallas import tpu as pltpu
from jax.sharding import PartitionSpec as P


LN_EPS = 1e-5
ROPE_BASE = 10000.0
ROTARY_DIVISOR = 4
LANES = 128
Q_ROWS = 256
LN_ROWS = 64
PAIRS = 2
MIB = 1024 * 1024
TILE = 256
SQRT_HALF = 0.5 ** 0.5
INV_SQRT_2PI = 0.3989422804014327

NT = (((1,), (1,)), ((), ()))
TN = (((0,), (0,)), ((), ()))
NN = (((1,), (0,)), ((), ()))


def dot(a, b, dims):
    return lax.dot_general(a, b, dims, preferred_element_type=jnp.float32)


def rotary_tables(seq_len, rot_dim):
    half = rot_dim // 2
    lane = jnp.arange(LANES)
    freq_index = jnp.where(lane < half, lane, lane - half)
    inv_freq = ROPE_BASE ** (-(2 * freq_index).astype(jnp.float32) / rot_dim)
    angles = jnp.arange(seq_len, dtype=jnp.float32)[:, None] * inv_freq[None, :]
    inside = (lane < rot_dim)[None, :]
    cos_tab = jnp.where(inside, jnp.cos(angles), 1.0)
    sin = jnp.where(inside, jnp.sin(angles), 0.0)
    first = (lane < half)[None, :]
    return cos_tab, jnp.where(first, -sin, 0.0), jnp.where(first, 0.0, sin)


def rotate(part, cos_tab, sin_lo, sin_hi, half, sign):
    head = part[:, :LANES]
    forward = pltpu.roll(head, half, 1)
    backward = pltpu.roll(head, LANES - half, 1)
    mixed = head * cos_tab + sign * (backward * sin_lo + forward * sin_hi)
    return jnp.concatenate([mixed, part[:, LANES:]], axis=1)


def causal_probs(q_rows, keys, row_start, scale):
    scores = dot(q_rows, keys, NT) * scale
    rows = row_start + lax.broadcasted_iota(jnp.int32, scores.shape, 0)
    cols = lax.broadcasted_iota(jnp.int32, scores.shape, 1)
    scores = jnp.where(rows >= cols, scores, -1e30)
    exps = jnp.exp(scores - jnp.max(scores, axis=1, keepdims=True))
    return exps * (1.0 / jnp.sum(exps, axis=1, keepdims=True))


def attn_fwd_kernel(qkv_ref, ctx_ref, *, scale, span):
    seq_len, width = ctx_ref.shape[1:]
    for end in range(span, seq_len + 1, span):
        @pl.loop(0, span // Q_ROWS)
        def _(step, end=end):
            start = pl.multiple_of(end - span + step * Q_ROWS, Q_ROWS)
            rows = pl.ds(start, Q_ROWS)
            probs = causal_probs(qkv_ref[0, rows, :width], qkv_ref[0, :end, width:2 * width], start, scale).astype(jnp.bfloat16)
            ctx_ref[0, rows, :] = dot(probs, qkv_ref[0, :end, 2 * width:], NN).astype(jnp.bfloat16)


def attn_bwd_kernel(qkv_ref, dctx_ref, cos_ref, lo_ref, hi_ref, dqkv_ref, db_ref, dk_ref, dv_ref, *, half, scale, span):
    seq_len, width = dctx_ref.shape[1:]
    dk_ref[...] = jnp.zeros(dk_ref.shape, jnp.float32)
    dv_ref[...] = jnp.zeros(dv_ref.shape, jnp.float32)
    db_ref[...] = jnp.zeros(db_ref.shape, jnp.float32)

    def store(rows, col, grad_rot, turn):
        grad = grad_rot.astype(jnp.bfloat16)
        if turn:
            wide = grad.astype(jnp.float32)
            grad = rotate(wide, cos_ref[rows, :], lo_ref[rows, :], hi_ref[rows, :], half, -1.0).astype(jnp.bfloat16)
        dqkv_ref[0, rows, col:col + width] = grad
        db_ref[0, :, col:col + width] += sublane_sum(grad.astype(jnp.float32))

    for end in range(span, seq_len + 1, span):
        @pl.loop(0, span // Q_ROWS)
        def _(step, end=end):
            start = pl.multiple_of(end - span + step * Q_ROWS, Q_ROWS)
            rows = pl.ds(start, Q_ROWS)
            q_rows, keys = qkv_ref[0, rows, :width], qkv_ref[0, :end, width:2 * width]
            dctx = dctx_ref[0, rows, :]
            probs = causal_probs(q_rows, keys, start, scale)
            dprobs = dot(dctx, qkv_ref[0, :end, 2 * width:], NT).astype(jnp.bfloat16).astype(jnp.float32)
            dv_ref[:end, :] += dot(probs.astype(jnp.bfloat16), dctx, TN)
            inner = jnp.sum(probs * dprobs, axis=1, keepdims=True)
            dscores = (probs * (dprobs - inner) * scale).astype(jnp.bfloat16)
            dk_ref[:end, :] += dot(dscores, q_rows, TN)
            store(rows, 0, dot(dscores, keys, NN), True)

    @pl.loop(0, seq_len // Q_ROWS)
    def _(step):
        rows = pl.ds(pl.multiple_of(step * Q_ROWS, Q_ROWS), Q_ROWS)
        store(rows, width, dk_ref[rows, :], True)
        store(rows, 2 * width, dv_ref[rows, :], False)


def attention_calls(n_seq, seq_len, width, tables):
    half = width // ROTARY_DIVISOR // 2
    scale = width ** -0.5
    span = 512 if seq_len % 512 == 0 else seq_len
    seq_spec = lambda cols, first=0: pl.BlockSpec((1, seq_len, cols), lambda s: (s + first, 0, 0))
    tab_spec = pl.BlockSpec((seq_len, LANES), lambda s: (0, 0))
    acc_scratch = pltpu.VMEM((seq_len, width), jnp.float32)
    pairs = seq_len * seq_len // 2
    params = pltpu.CompilerParams(dimension_semantics=("arbitrary",), vmem_limit_bytes=60 * MIB)

    def forward(qkv):
        return pl.pallas_call(
            functools.partial(attn_fwd_kernel, scale=scale, span=span),
            grid=(n_seq,),
            in_specs=[seq_spec(3 * width)],
            out_specs=seq_spec(width),
            out_shape=jax.ShapeDtypeStruct((n_seq, seq_len, width), jnp.bfloat16),
            compiler_params=params,
            name="af",
            cost_estimate=pl.CostEstimate(flops=8 * n_seq * pairs * width, bytes_accessed=8 * n_seq * seq_len * width, transcendentals=n_seq * pairs),
        )(qkv)

    def backward(qkv, dctx, index, into):
        kernel = functools.partial(attn_bwd_kernel, half=half, scale=scale, span=span)
        return pl.pallas_call(
            (lambda *refs: kernel(*refs[:5], *refs[5 + len(into):])),
            grid=(1,),
            in_specs=[seq_spec(3 * width, index), seq_spec(width, index), tab_spec, tab_spec, tab_spec] + [pl.BlockSpec(memory_space=pl.ANY)] * len(into),
            out_specs=[seq_spec(3 * width, index), pl.BlockSpec((1, 8, 3 * width), lambda s: (s, 0, 0))],
            input_output_aliases={5: 0} if into else {},
            out_shape=[jax.ShapeDtypeStruct((n_seq, seq_len, 3 * width), jnp.bfloat16), jax.ShapeDtypeStruct((1, 8, 3 * width), jnp.float32)],
            scratch_shapes=[acc_scratch, acc_scratch],
            compiler_params=params,
            name="ab",
            cost_estimate=pl.CostEstimate(flops=20 * pairs * width, bytes_accessed=14 * seq_len * width, transcendentals=pairs),
        )(qkv, dctx, *tables, *into)

    return forward, backward


def place_kernel(place_ref, same_ref, other_ref, *rest, per, chunk, n_seq):
    out_ref, held_ref, in_sems, out_sems = rest[-4:]
    groups = same_ref.shape[0] // per
    fetch, store = [], []
    for which, ref in enumerate((same_ref, other_ref)):
        core = place_ref[2] if which == 0 else 1 - place_ref[2]
        for r in range(groups):
            sem = which * groups + r
            part = pl.ds(r * per, per)
            to = lax.rem(place_ref[0] + groups - r, groups) * n_seq + chunk
            fetch.append(pltpu.make_async_copy(ref.at[part], held_ref.at[which, part], in_sems.at[sem]))
            store.append(pltpu.make_async_copy(held_ref.at[which, part], out_ref.at[pl.ds(to, per), :, core], out_sems.at[sem]))
    for copy in fetch:
        copy.start()
    for copy_in, copy_out in zip(fetch, store):
        copy_in.wait()
        copy_out.start()
    for copy in store:
        copy.wait()


def place_call(place, same, other, out, chunk, n_seq):
    total, columns, own, width = same.shape
    per = n_seq if out is None and chunk is None else 1
    groups = total // per
    operands = [place, same, other] + ([] if out is None else [out])
    any_spec = pl.BlockSpec(memory_space=pl.ANY)
    sems = pltpu.SemaphoreType.DMA((2 * groups,))
    return pl.pallas_call(
        functools.partial(place_kernel, per=per, chunk=chunk or 0, n_seq=n_seq),
        in_specs=[pl.BlockSpec(memory_space=pltpu.SMEM)] + [any_spec] * (len(operands) - 1),
        out_specs=any_spec,
        out_shape=jax.ShapeDtypeStruct((groups * n_seq, columns, 2, own, width), jnp.bfloat16),
        scratch_shapes=[pltpu.VMEM((2, *same.shape), jnp.bfloat16), sems, sems],
        input_output_aliases={} if out is None else {3: 0},
        cost_estimate=pl.CostEstimate(flops=2 * same.size, bytes_accessed=8 * same.size, transcendentals=0),
    )(*operands)


def grad_kernel(*refs, blocks, moving, splits):
    acc_ref = refs[-1]
    n_out = sum(len(parts) for parts in splits)
    ins, outs = refs[:-1 - n_out], list(refs[-1 - n_out:-1])
    step = pl.program_id(0)

    @pl.when(step == 0)
    def _():
        acc_ref[...] = jnp.zeros(acc_ref.shape, jnp.float32)

    for index, terms in enumerate(blocks):
        for lhs, rhs, row, column in terms:
            part = dot(ins[lhs][...], ins[rhs][...], TN)
            acc_ref[index, row:row + part.shape[0], column:column + part.shape[1]] += part

    @pl.when(step == pl.num_programs(0) - 1)
    def _():
        for index, adds in enumerate(moving):
            for ref, row in adds:
                at = slice(row, row + ins[ref].shape[0])
                acc_ref[index, at, :] += ins[ref][...].astype(jnp.float32)
        for index, parts in enumerate(splits):
            for rows, cols in parts:
                out = outs.pop(0)
                out[...] = acc_ref[index, rows, cols].astype(out.dtype)


def grad_call(blocks, shape, moving, splits, dtype, rows=512):
    ins, specs, keys = [], [], {}

    def operand(array, block, width):
        key = (id(array), block, width)
        if key not in keys:
            keys[key] = len(ins)
            ins.append(array)
            specs.append(pl.BlockSpec((rows, width), lambda s, b=block: (s, b)))
        return keys[key]

    count = blocks[0][0][0].shape[0]
    terms = [[(operand(lhs, lb, lw), operand(rhs, rb, rw), row, col) for lhs, lb, lw, rhs, rb, rw, row, col in block] for block in blocks]
    adds = []
    for block in moving:
        found = []
        for array, row in block:
            found.append((len(ins), row))
            ins.append(array)
            specs.append(pl.BlockSpec(array.shape, lambda s: (0, 0)))
        adds.append(found)
    span = lambda at, size: len(range(*at.indices(size)))
    shapes = [(span(r, shape[0]), span(c, shape[1])) for parts in splits for r, c in parts]
    return pl.pallas_call(
        functools.partial(grad_kernel, blocks=terms, moving=adds, splits=splits),
        grid=(count // rows,),
        in_specs=specs,
        out_specs=[pl.BlockSpec(one, lambda s: (0, 0)) for one in shapes],
        out_shape=[jax.ShapeDtypeStruct(one, dtype) for one in shapes],
        scratch_shapes=[pltpu.VMEM((len(blocks), *shape), jnp.float32)],
        compiler_params=pltpu.CompilerParams(dimension_semantics=("arbitrary",), vmem_limit_bytes=60 * MIB),
        cost_estimate=pl.CostEstimate(flops=2 * len(blocks) * count * shape[0] * shape[1], bytes_accessed=sum(2 * count * spec.block_shape[1] for spec in specs), transcendentals=0),
    )(*ins)


def split_width(value, out_refs):
    width = out_refs[0].shape[1]
    for index, out_ref in enumerate(out_refs):
        out_ref[...] = value[:, index * width:(index + 1) * width].astype(out_ref.dtype)


def finish_y_kernel(x_ref, mixed_ref, bias_ref, *out_refs):
    split_width(x_ref[...].astype(jnp.float32) + mixed_ref[...].astype(jnp.float32) + bias_ref[...], out_refs)


def normalize(act):
    act = act.astype(jnp.float32)
    mean = act.mean(-1, keepdims=True)
    inv_std = lax.rsqrt((act * act).mean(-1, keepdims=True) - mean * mean + LN_EPS)
    return (act - mean) * inv_std, inv_std


def finish_dx_kernel(x_ref, a6_ref, cot_ref, *out_refs):
    x_hat, inv_std = normalize(x_ref[...])
    value_a6 = a6_ref[...].astype(jnp.float32)
    mean_a6 = value_a6.mean(-1, keepdims=True)
    mean_a6x = (value_a6 * x_hat).mean(-1, keepdims=True)
    split_width(cot_ref[...].astype(jnp.float32) + inv_std * (value_a6 - mean_a6 - x_hat * mean_a6x), out_refs)


def row_call(kernel, parts, index, rows, *operands):
    width = operands[0].shape[1]
    specs = [pl.BlockSpec((min(rows, op.shape[0]), width), lambda s, i=(index if op.shape[0] > rows else 0): (i, 0)) for op in operands]
    return pl.pallas_call(
        kernel,
        grid=(1,),
        in_specs=specs,
        out_specs=[pl.BlockSpec((rows, width // parts), lambda s: (0, 0))] * parts,
        out_shape=[jax.ShapeDtypeStruct((rows, width // parts), jnp.bfloat16)] * parts,
        compiler_params=pltpu.CompilerParams(vmem_limit_bytes=16 * MIB),
        cost_estimate=pl.CostEstimate(flops=16 * rows * width, bytes_accessed=8 * rows * width, transcendentals=0),
    )(*operands)


def sublane_sum(value):
    return value.reshape(value.shape[0] // 8, 8, value.shape[1]).sum(0)


def norm_kernel(x_ref, small_ref, h_attn_ref, h_mlp_ref):
    @pl.loop(0, x_ref.shape[0] // LN_ROWS)
    def _(step):
        at = pl.ds(pl.multiple_of(step * LN_ROWS, LN_ROWS), LN_ROWS)
        x_hat, _ = normalize(x_ref[at, :])
        h_attn_ref[at, :] = (x_hat * small_ref[0:1, :] + small_ref[1:2, :]).astype(jnp.bfloat16)
        h_mlp_ref[at, :] = (x_hat * small_ref[2:3, :] + small_ref[3:4, :]).astype(jnp.bfloat16)


def offsets(refs, axis):
    starts = [0]
    for ref in refs:
        starts.append(starts[-1] + ref.shape[axis])
    return list(zip(refs, starts, starts[1:]))


def front_kernel(h_attn_ref, h_mlp_ref, cos_ref, lo_ref, hi_ref, b_qkv_ref, b_up_ref, *refs):
    w_refs, (qkv_ref, pre_ref, gelu_ref) = refs[:-3], refs[-3:]
    qkv_width = qkv_ref.shape[1]
    head = qkv_width // 3

    def project(h_ref, cols):
        return sum(dot(h_ref[:, start:stop], w_ref[:, cols], NN) for w_ref, start, stop in offsets(w_refs, 0))

    for low in range(0, qkv_width, head):
        at = slice(low, low + head)
        part = (project(h_attn_ref, at) + b_qkv_ref[:, at]).astype(jnp.bfloat16)
        if low < 2 * head:
            part = rotate(part.astype(jnp.float32), cos_ref[...], lo_ref[...], hi_ref[...], head // ROTARY_DIVISOR // 2, 1.0).astype(jnp.bfloat16)
        qkv_ref[:, at] = part
    for low in range(0, pre_ref.shape[1], TILE):
        at = slice(low, low + TILE)
        pre = (project(h_mlp_ref, slice(qkv_width + low, qkv_width + low + TILE)) + b_up_ref[:, at]).astype(jnp.bfloat16)
        pre_ref[:, at] = pre
        wide = pre.astype(jnp.float32)
        gelu_ref[:, at] = (0.5 * wide * (1.0 + lax.erf(wide * SQRT_HALF))).astype(jnp.bfloat16)


def split_places(rows_ref, place_ref, mine, other):
    core = place_ref[2]
    own = rows_ref.shape[0] // (2 * PAIRS)
    for pair in range(PAIRS):
        for store, which in ((mine, core), (other, 1 - core)):
            store(pair, rows_ref[pl.ds(pl.multiple_of((2 * pair + which) * own, own), own), :])


def y_kernel(ctx_ref, gelu_ref, place_ref, *refs):
    w_refs, (mine_ref, other_ref, rows_ref) = refs[:-3], refs[-3:]
    head = ctx_ref.shape[1]
    for w_ref, start, stop in offsets(w_refs, 1):
        acc = dot(ctx_ref[...], w_ref[:head, :], NN) + dot(gelu_ref[...], w_ref[head:, :], NN)
        rows_ref[:, start:stop] = acc.astype(jnp.bfloat16)

    def put(ref):
        def store(pair, value):
            ref[pair, 0] = value

        return store

    split_places(rows_ref, place_ref, put(mine_ref), put(other_ref))


def d_pre_kernel(cot_ref, pre_ref, *refs):
    w_refs, (d_ctx_ref, d_pre_ref, d_bias_ref) = refs[:-3], refs[-3:]

    def back(low, high):
        return sum(dot(cot_ref[:, start:stop], w_ref[low:high, :], NT) for w_ref, start, stop in offsets(w_refs, 1)).astype(jnp.bfloat16)

    head = d_ctx_ref.shape[1]

    @pl.when(pl.program_id(0) == 0)
    def _():
        d_bias_ref[...] = jnp.zeros(d_bias_ref.shape, jnp.float32)

    d_ctx_ref[...] = back(0, head)
    for low in range(0, d_pre_ref.shape[1], TILE):
        at = slice(low, low + TILE)
        d_gelu = back(head + low, head + low + TILE).astype(jnp.float32)
        pre = pre_ref[:, at].astype(jnp.float32)
        slope = 0.5 * (1.0 + lax.erf(pre * SQRT_HALF)) + pre * (jnp.exp(-0.5 * pre * pre) * INV_SQRT_2PI)
        d_pre = (d_gelu * slope).astype(jnp.bfloat16)
        d_pre_ref[:, at] = d_pre
        d_bias_ref[:, at] += sublane_sum(d_pre.astype(jnp.float32))


def d_h_kernel(d_qkv_ref, d_pre_ref, x_ref, small_ref, place_ref, *refs):
    w_refs, (mine_ref, other_ref, sums_ref, a6_ref) = refs[:-4], refs[-4:]
    qkv_width = d_qkv_ref.shape[1]

    @pl.when(pl.program_id(0) == 0)
    def _():
        sums_ref[...] = jnp.zeros(sums_ref.shape, jnp.float32)

    x_float = x_ref[...].astype(jnp.float32)
    mean = x_float.mean(-1, keepdims=True)
    inv_std = lax.rsqrt((x_float * x_float).mean(-1, keepdims=True) - mean * mean + LN_EPS)
    for w_ref, start, stop in offsets(w_refs, 0):
        for low in range(0, stop - start, TILE):
            part = slice(low, min(low + TILE, stop - start))
            at = slice(start + part.start, start + part.stop)
            d_attn = dot(d_qkv_ref[...], w_ref[part, :qkv_width], NT).astype(jnp.bfloat16).astype(jnp.float32)
            d_mlp = dot(d_pre_ref[...], w_ref[part, qkv_width:], NT).astype(jnp.bfloat16).astype(jnp.float32)
            a6_ref[:, at] = (d_attn * small_ref[0:1, at] + d_mlp * small_ref[2:3, at]).astype(jnp.bfloat16)
            x_hat = (x_ref[:, at].astype(jnp.float32) - mean) * inv_std
            sums_ref[0, :, at] += sublane_sum(d_attn * x_hat)
            sums_ref[1, :, at] += sublane_sum(d_attn)
            sums_ref[2, :, at] += sublane_sum(d_mlp * x_hat)
            sums_ref[3, :, at] += sublane_sum(d_mlp)

    def put(ref):
        def store(pair, value):
            ref[pair, 0] = value

        return store

    split_places(a6_ref, place_ref, put(mine_ref), put(other_ref))


def tile_call(kernel, tiled, whole, outs, row_range, flops, rows=512, scratch=()):
    start, count = row_range
    rows = next(r for r in (rows, 256, 128, 64, count) if count % r == 0 and all(op.shape[0] % r == 0 for op in tiled))
    first = start // rows

    def tile_spec(op):
        blocks = op.shape[0] // rows
        if blocks * rows < count:
            return pl.BlockSpec((rows, op.shape[1]), lambda s: (lax.rem(s, blocks), 0))
        return pl.BlockSpec((rows, op.shape[1]), lambda s, f=(first if op.shape[0] != count else 0): (s + f, 0))

    in_specs = [tile_spec(op) for op in tiled]
    for op in whole:
        if op.dtype == jnp.int32:
            in_specs.append(pl.BlockSpec(memory_space=pltpu.SMEM))
        else:
            in_specs.append(pl.BlockSpec(op.shape, lambda s, n=op.ndim: (0,) * n, pipeline_mode=pl.Buffered(1)))
    out_specs, out_shapes = [], []
    for form, dtype in outs:
        if isinstance(form, int):
            out_specs.append(pl.BlockSpec((rows, form), lambda s: (s, 0)))
            out_shapes.append(jax.ShapeDtypeStruct((count, form), dtype))
        elif isinstance(form[0], tuple):
            out_specs.append(pl.BlockSpec(form[1], form[2]))
            out_shapes.append(jax.ShapeDtypeStruct(form[0], dtype))
        else:
            out_specs.append(pl.BlockSpec(form, lambda s, n=len(form): (0,) * n))
            out_shapes.append(jax.ShapeDtypeStruct(form, dtype))
    moved = sum(2 * op.shape[1] * count for op in tiled) + sum(2 * op.size for op in whole) + sum(2 * shape.size for shape in out_shapes)
    return pl.pallas_call(
        kernel,
        grid=(count // rows,),
        in_specs=in_specs,
        out_specs=out_specs,
        out_shape=out_shapes,
        scratch_shapes=list(scratch),
        compiler_params=pltpu.CompilerParams(dimension_semantics=("arbitrary",), vmem_limit_bytes=60 * MIB),
        cost_estimate=pl.CostEstimate(flops=flops, bytes_accessed=moved, transcendentals=0),
    )(*tiled, *whole)


def solution(mesh):
    tx_size, ty_size = mesh.shape['tx'], mesh.shape['ty']
    act_spec = P('dp', None, 'tx')
    width_spec = P('tx')
    in_specs = (act_spec, act_spec, width_spec, width_spec, width_spec, width_spec, P('tx', 'ty', None), P('ty', None), P('ty', 'tx'), width_spec, P('tx', 'ty'), P('ty'), P('ty', 'tx'), width_spec)
    width_out = P(('dp', 'tx'))
    out_specs = (act_spec, act_spec, width_out, width_out, width_out, width_out, P(('dp', 'tx'), 'ty', None), P(('dp', 'ty'), None), P(('dp', 'ty'), 'tx'), width_out, P(('dp', 'tx'), 'ty'), P(('dp', 'ty')), P(('dp', 'ty'), 'tx'), width_out)
    antipode = tx_size // 2

    def shift(value, hops):
        return lax.ppermute(value, 'tx', [(s, (s - hops) % tx_size) for s in range(tx_size)])

    def small_sum(value, axis, size):
        step = 1
        while step < size:
            value = value + lax.ppermute(value, axis, [(s, s ^ step) for s in range(size)])
            step *= 2
        return value

    def partner(value):
        return lax.ppermute(value, 'ty', [(s, s ^ 1) for s in range(ty_size)])

    def ring_gather(block, axis):
        blocks = {0: [block]}
        for hops in range(1, antipode):
            blocks[hops] = [shift(blocks[hops - 1][0], 1)]
            blocks[tx_size - hops] = [shift(blocks[(tx_size - hops + 1) % tx_size][0], -1)]
        half = block.shape[axis] // 2
        low = lax.slice_in_dim(blocks[antipode - 1][0], 0, half, axis=axis)
        high = lax.slice_in_dim(blocks[antipode + 1][0], half, 2 * half, axis=axis)
        blocks[antipode] = [shift(low, 1), shift(high, -1)]
        return [piece for r in range(tx_size) for piece in blocks[r]]

    def ring_scatter(make_blocks, shape):
        whole, half = slice(None), shape[0] // 2
        assert tx_size == 4
        low, high = grad_call([make_blocks(2)], shape, [[]], [[(slice(0, half), whole), (slice(half, None), whole)]], jnp.bfloat16)
        low, high = shift(low, -1), shift(high, 1)
        up, down = grad_call([make_blocks(1), make_blocks(3)], shape, [[(low, 0)], [(high, half)]], [[(whole, whole)], [(whole, whole)]], jnp.bfloat16)
        return [(shift(up, -1), 0), (shift(down, 1), 0)]

    def body(x_act, cot_out, ln1_gain, ln1_bias, ln2_gain, ln2_bias, w_qkv, b_qkv, w_dense, b_dense, w_up, b_up, w_down, b_down):
        batch, seq_len, d_local = x_act.shape
        n_seq = batch // tx_size
        own = seq_len // ty_size
        row, col = lax.axis_index('tx'), lax.axis_index('ty')
        qkv_width = w_qkv.shape[1] * w_qkv.shape[2]
        head = qkv_width // 3
        chunks = range(n_seq)
        tables = rotary_tables(seq_len, head // ROTARY_DIVISOR)
        attn_fwd, attn_bwd = attention_calls(n_seq, seq_len, head, tables)

        def to_tokens(act):
            parts = act.reshape(tx_size, n_seq, ty_size, own, d_local)
            pick = lambda index: lax.dynamic_slice(parts, (index, 0, col, 0, 0), (1, n_seq, 1, own, d_local)).reshape(n_seq, own, d_local)
            blocks = [pick(row)] + [shift(pick((row - r) % tx_size), r) for r in range(1, tx_size)]
            return jnp.concatenate(blocks, axis=2)

        place = jnp.stack([row, col // 2, col % 2])

        def to_width(parts):
            return jnp.stack([parts[0]] + [shift(parts[r], -r) for r in range(1, tx_size)])

        line = lax.broadcasted_iota(jnp.int32, (8, d_local), 0)
        small = jnp.zeros((8, d_local), jnp.bfloat16)
        for index, vector in enumerate((ln1_gain, ln1_bias, ln2_gain, ln2_bias, b_dense, b_down)):
            small = jnp.where(line == index, vector[None, :], small)
        small = [small] + [shift(small, r) for r in range(1, tx_size)]
        small = jnp.concatenate(small, axis=1).astype(jnp.float32)
        bias_out = small[4] + small[5]
        x_own = to_tokens(x_act)
        cot_own = to_tokens(cot_out)
        x_group = lax.all_gather(x_own, 'ty', axis=1, tiled=True)
        cot_group = lax.all_gather(cot_own, 'ty', axis=1, tiled=True)
        x_group, cot_group = x_group.reshape(n_seq * seq_len, -1), cot_group.reshape(n_seq * seq_len, -1)
        w_in = jnp.concatenate([w_qkv.reshape(d_local, qkv_width), w_up], axis=1)
        w_in = ring_gather(w_in, 0)
        w_back = jnp.concatenate([w_dense, w_down], axis=0)
        w_back = ring_gather(w_back, 1)
        in_size, back_size = sum(w.size for w in w_in), sum(w.size for w in w_back)

        n_tok, d_model = x_group.shape
        x_rows, cot_rows = x_own.reshape(-1, d_model), cot_own.reshape(-1, d_model)
        ff_width = w_up.shape[1]
        h_attn, h_mlp = tile_call(norm_kernel, [x_group], [small], [(d_model, jnp.bfloat16), (d_model, jnp.bfloat16)], (0, n_tok), 16 * x_group.size)
        qkv_act, pre_act, gelu_out = tile_call(
            front_kernel, [h_attn, h_mlp, *tables], [b_qkv.reshape(1, -1).astype(jnp.float32), b_up.reshape(1, -1).astype(jnp.float32), *w_in],
            [(qkv_width, jnp.bfloat16), (ff_width, jnp.bfloat16), (ff_width, jnp.bfloat16)], (0, n_tok), 2 * n_tok * in_size)
        qkv_seq = qkv_act.reshape(n_seq, seq_len, qkv_width)
        context = attn_fwd(qkv_seq).reshape(n_tok, head)
        columns = ty_size // 2
        same_core = [[2 * x + c for x in range(columns)] for c in range(2)]
        tile = 2 * PAIRS * own
        tiles_per_seq = seq_len // tile
        form = ((columns, n_seq, own, d_model), (PAIRS, 1, own, d_model), lambda s: (lax.rem(s, tiles_per_seq), s // tiles_per_seq, 0, 0))
        mine, other = tile_call(
            y_kernel, [context, gelu_out], [place, *w_back], [(form, jnp.bfloat16)] * 2, (0, n_tok), 2 * n_tok * back_size, tile,
            [pltpu.VMEM((tile, d_model), jnp.bfloat16)])

        def scatter_columns(mine, other):
            other = partner(other)
            total = (mine.astype(jnp.float32) + other.astype(jnp.float32)).astype(jnp.bfloat16).reshape(-1, d_model)
            return lax.psum_scatter(total, 'ty', scatter_dimension=0, axis_index_groups=same_core, tiled=True)

        def gather_columns(block):
            same = lax.all_gather(block, 'ty', axis=1, axis_index_groups=same_core, tiled=True)
            other = partner(same)
            return [half.reshape(-1, columns, own, d_local) for half in (same, other)]

        mixed = scatter_columns(mine, other)
        block = to_width(row_call(finish_y_kernel, tx_size, 0, n_seq * own, x_rows, mixed, bias_out.reshape(1, -1)))
        y_out = place_call(place, *gather_columns(block.reshape(tx_size * n_seq, own, d_local)), None, None, n_seq)

        d_ctx, d_pre, d_b_up = tile_call(
            d_pre_kernel, [cot_group, pre_act], w_back,
            [(head, jnp.bfloat16), (ff_width, jnp.bfloat16), ((8, ff_width), jnp.float32)], (0, n_tok), 2 * n_tok * back_size)
        d_ctx, d_b_up = d_ctx.reshape(n_seq, seq_len, head), d_b_up.sum(0)
        d_b_qkv, d_ln, dx_act = [], [], None
        for s in chunks:
            d_qkv, d_b_seq = attn_bwd(qkv_seq, d_ctx, s, (d_qkv, sums) if s else ())
            d_b_qkv.append(d_b_seq.sum((0, 1)))
            form = ((columns, 1, own, d_model), (PAIRS, 1, own, d_model), lambda t: (t, 0, 0, 0))
            mine, other, sums = tile_call(
                d_h_kernel, [d_qkv.reshape(n_tok, qkv_width), d_pre, x_group], [small, place, *w_in],
                [(form, jnp.bfloat16), (form, jnp.bfloat16), ((4, 8, d_model), jnp.float32)], (s * seq_len, seq_len), 2 * seq_len * in_size, tile,
                [pltpu.VMEM((tile, d_model), jnp.bfloat16)])
            d_ln.append(sums)
            value_a6 = scatter_columns(mine, other)
            parts = row_call(finish_dx_kernel, tx_size, s, own, x_rows, value_a6, cot_rows)
            dx_act = place_call(place, *gather_columns(to_width(parts)), dx_act, s, n_seq)
        y_out, dx_act = y_out.reshape(x_act.shape), dx_act.reshape(x_act.shape)
        d_qkv = d_qkv.reshape(n_tok, qkv_width)

        d_ln = sum(d_ln).sum(1).reshape(4, tx_size, d_local)
        d_bias = jnp.concatenate([sum(d_b_qkv), d_b_up]).reshape(4, -1)
        sent = [jnp.concatenate([d_ln[:, r], d_bias], axis=1) for r in range(tx_size)]
        got = [sent[0]] + [shift(sent[r], -r) for r in range(1, tx_size)]
        got = sum(got[r] + got[r + antipode] for r in range(antipode))
        d_bias = got[:, d_local:].reshape(-1)
        d_ln = small_sum(got[:, :d_local], 'ty', ty_size)
        d_b_out = cot_out.astype(jnp.float32).sum((0, 1))

        in_shape, back_shape = (d_local, qkv_width + ff_width), (head + ff_width, d_local)
        in_blocks = lambda r: [(h_attn, r, d_local, d_qkv, 0, qkv_width, 0, 0), (h_mlp, r, d_local, d_pre, 0, ff_width, 0, qkv_width)]
        back_blocks = lambda r: [(context, 0, head, cot_group, r, d_local, 0, 0), (gelu_out, 0, ff_width, cot_group, r, d_local, head, 0)]
        add_back = ring_scatter(back_blocks, back_shape)
        add_in = ring_scatter(in_blocks, in_shape)
        whole = slice(None)
        d_w_dense, d_w_down = grad_call([back_blocks(0)], back_shape, [add_back], [[(slice(0, head), whole), (slice(head, None), whole)]], jnp.float32)
        d_w_qkv, d_w_up = grad_call([in_blocks(0)], in_shape, [add_in], [[(whole, slice(0, qkv_width)), (whole, slice(qkv_width, None))]], jnp.float32)
        return (y_out, dx_act, d_ln[0], d_ln[1], d_ln[2], d_ln[3], d_w_qkv.reshape(w_qkv.shape), d_bias[:qkv_width].reshape(b_qkv.shape), d_w_dense, d_b_out, d_w_up, d_bias[qkv_width:], d_w_down, d_b_out)

    return jax.shard_map(body, mesh=mesh, in_specs=in_specs, out_specs=out_specs, check_vma=False)
```

```python
import functools
import jax
import jax.numpy as jnp
from jax import lax
from jax.experimental import pallas as pl
from jax.experimental.pallas import tpu as pltpu
from jax.sharding import PartitionSpec as P


LN_EPS = 1e-5
ROPE_BASE = 10000.0
ROTARY_DIVISOR = 4
LANES = 128
Q_ROWS = 256
LN_ROWS = 64
MIB = 1024 * 1024
TILE = 256
SQRT_HALF = 0.5 ** 0.5
INV_SQRT_2PI = 0.3989422804014327

NT = (((1,), (1,)), ((), ()))
TN = (((0,), (0,)), ((), ()))
NN = (((1,), (0,)), ((), ()))


def dot(a, b, dims):
    return lax.dot_general(a, b, dims, preferred_element_type=jnp.float32)


def rotary_tables(seq_len, rot_dim):
    half = rot_dim // 2
    lane = jnp.arange(LANES)
    freq_index = jnp.where(lane < half, lane, lane - half)
    inv_freq = ROPE_BASE ** (-(2 * freq_index).astype(jnp.float32) / rot_dim)
    angles = jnp.arange(seq_len, dtype=jnp.float32)[:, None] * inv_freq[None, :]
    inside = (lane < rot_dim)[None, :]
    cos_tab = jnp.where(inside, jnp.cos(angles), 1.0)
    sin = jnp.where(inside, jnp.sin(angles), 0.0)
    first = (lane < half)[None, :]
    return cos_tab, jnp.where(first, -sin, 0.0), jnp.where(first, 0.0, sin)


def rotate(part, cos_tab, sin_lo, sin_hi, half, sign):
    head = part[:, :LANES]
    forward = pltpu.roll(head, half, 1)
    backward = pltpu.roll(head, LANES - half, 1)
    mixed = head * cos_tab + sign * (backward * sin_lo + forward * sin_hi)
    return jnp.concatenate([mixed, part[:, LANES:]], axis=1)


def causal_probs(q_rows, keys, row_start, scale):
    scores = dot(q_rows, keys, NT) * scale
    rows = row_start + lax.broadcasted_iota(jnp.int32, scores.shape, 0)
    cols = lax.broadcasted_iota(jnp.int32, scores.shape, 1)
    scores = jnp.where(rows >= cols, scores, -1e30)
    exps = jnp.exp(scores - jnp.max(scores, axis=1, keepdims=True))
    return exps * (1.0 / jnp.sum(exps, axis=1, keepdims=True))


def attn_fwd_kernel(qkv_ref, ctx_ref, *, scale, span):
    seq_len, width = ctx_ref.shape[1:]
    for end in range(span, seq_len + 1, span):
        for start in range(end - span, end, Q_ROWS):
            rows = slice(start, start + Q_ROWS)
            probs = causal_probs(qkv_ref[0, rows, :width], qkv_ref[0, :end, width:2 * width], start, scale).astype(jnp.bfloat16)
            ctx_ref[0, rows, :] = dot(probs, qkv_ref[0, :end, 2 * width:], NN).astype(jnp.bfloat16)


def attn_bwd_kernel(qkv_ref, dctx_ref, cos_ref, lo_ref, hi_ref, dqkv_ref, db_ref, dk_ref, dv_ref, *, half, scale, span):
    seq_len, width = dctx_ref.shape[1:]
    dk_ref[...] = jnp.zeros(dk_ref.shape, jnp.float32)
    dv_ref[...] = jnp.zeros(dv_ref.shape, jnp.float32)
    db_ref[...] = jnp.zeros(db_ref.shape, jnp.float32)

    def store(rows, col, grad_rot, turn):
        grad = grad_rot.astype(jnp.bfloat16)
        if turn:
            wide = grad.astype(jnp.float32)
            grad = rotate(wide, cos_ref[rows, :], lo_ref[rows, :], hi_ref[rows, :], half, -1.0).astype(jnp.bfloat16)
        dqkv_ref[0, rows, col:col + width] = grad
        db_ref[0, :, col:col + width] += sublane_sum(grad.astype(jnp.float32))

    for end in range(span, seq_len + 1, span):
        for start in range(end - span, end, Q_ROWS):
            rows = slice(start, start + Q_ROWS)
            q_rows, keys = qkv_ref[0, rows, :width], qkv_ref[0, :end, width:2 * width]
            dctx = dctx_ref[0, rows, :]
            probs = causal_probs(q_rows, keys, start, scale)
            dprobs = dot(dctx, qkv_ref[0, :end, 2 * width:], NT).astype(jnp.bfloat16).astype(jnp.float32)
            dv_ref[:end, :] += dot(probs.astype(jnp.bfloat16), dctx, TN)
            inner = jnp.sum(probs * dprobs, axis=1, keepdims=True)
            dscores = (probs * (dprobs - inner) * scale).astype(jnp.bfloat16)
            dk_ref[:end, :] += dot(dscores, q_rows, TN)
            store(rows, 0, dot(dscores, keys, NN), True)

    @pl.loop(0, seq_len // Q_ROWS)
    def _(step):
        rows = pl.ds(pl.multiple_of(step * Q_ROWS, Q_ROWS), Q_ROWS)
        store(rows, width, dk_ref[rows, :], True)
        store(rows, 2 * width, dv_ref[rows, :], False)


def attention_calls(n_seq, seq_len, width, tables):
    half = width // ROTARY_DIVISOR // 2
    scale = width ** -0.5
    span = 512 if seq_len % 512 == 0 else seq_len
    seq_spec = lambda cols, first=0: pl.BlockSpec((1, seq_len, cols), lambda s: (s + first, 0, 0))
    tab_spec = pl.BlockSpec((seq_len, LANES), lambda s: (0, 0))
    acc_scratch = pltpu.VMEM((seq_len, width), jnp.float32)
    pairs = seq_len * seq_len // 2
    params = pltpu.CompilerParams(dimension_semantics=("arbitrary",), vmem_limit_bytes=60 * MIB)

    def forward(qkv):
        return pl.pallas_call(
            functools.partial(attn_fwd_kernel, scale=scale, span=span),
            grid=(n_seq,),
            in_specs=[seq_spec(3 * width)],
            out_specs=seq_spec(width),
            out_shape=jax.ShapeDtypeStruct((n_seq, seq_len, width), jnp.bfloat16),
            compiler_params=params,
            name="af",
            cost_estimate=pl.CostEstimate(flops=8 * n_seq * pairs * width, bytes_accessed=8 * n_seq * seq_len * width, transcendentals=n_seq * pairs),
        )(qkv)

    def backward(qkv, dctx, index, into):
        kernel = functools.partial(attn_bwd_kernel, half=half, scale=scale, span=span)
        return pl.pallas_call(
            (lambda *refs: kernel(*refs[:5], *refs[5 + len(into):])),
            grid=(1,),
            in_specs=[seq_spec(3 * width, index), seq_spec(width, index), tab_spec, tab_spec, tab_spec] + [pl.BlockSpec(memory_space=pl.ANY)] * len(into),
            out_specs=[seq_spec(3 * width, index), pl.BlockSpec((1, 8, 3 * width), lambda s: (s, 0, 0))],
            input_output_aliases={5: 0} if into else {},
            out_shape=[jax.ShapeDtypeStruct((n_seq, seq_len, 3 * width), jnp.bfloat16), jax.ShapeDtypeStruct((1, 8, 3 * width), jnp.float32)],
            scratch_shapes=[acc_scratch, acc_scratch],
            compiler_params=params,
            name="ab",
            cost_estimate=pl.CostEstimate(flops=20 * pairs * width, bytes_accessed=14 * seq_len * width, transcendentals=pairs),
        )(qkv, dctx, *tables, *into)

    return forward, backward


def place_kernel(place_ref, full_ref, *rest, chunk, n_seq):
    out_ref, held_ref, in_sems, out_sems = rest[-4:]
    groups = full_ref.shape[0]
    fetch = [pltpu.make_async_copy(full_ref.at[lax.rem(place_ref[0] + groups - t, groups)], held_ref.at[t], in_sems.at[t]) for t in range(groups)]
    store = [pltpu.make_async_copy(held_ref.at[t], out_ref.at[t * n_seq + chunk], out_sems.at[t]) for t in range(groups)]
    for copy in fetch:
        copy.start()
    for t in range(groups):
        fetch[t].wait()
        store[t].start()
    for copy in store:
        copy.wait()


def place_pieces_kernel(place_ref, *refs, chunk, n_seq):
    out_ref, held_ref, in_sems, out_sems = refs[-4:]
    groups, own, _ = refs[0].shape
    columns = held_ref.shape[0] // 2
    row, column, core = place_ref[0], place_ref[1], place_ref[2]
    fetch, store = [], []
    for index in range(2 * columns):
        source = 2 * lax.rem(column + index % columns, columns) + (core if index < columns else 1 - core)
        at = pl.ds(pl.multiple_of(source * own, own), own)
        fetch.append(pltpu.make_async_copy(refs[index], held_ref.at[index], in_sems.at[index]))
        for t in range(groups):
            piece = held_ref.at[index, lax.rem(row + groups - t, groups)]
            store.append(pltpu.make_async_copy(piece, out_ref.at[t * n_seq + chunk, at], out_sems.at[index]))
    for copy in fetch:
        copy.start()
    for index in range(2 * columns):
        fetch[index].wait()
        for copy in store[index * groups:(index + 1) * groups]:
            copy.start()
    for copy in store:
        copy.wait()


def place_call(kernel, place, operands, out, chunk, n_seq, tokens):
    groups, _, width = operands[0].shape
    operands = [place, *operands] + ([] if out is None else [out])
    any_spec = pl.BlockSpec(memory_space=pl.ANY)
    pieces = len(operands) - 1 - (out is not None)
    held = operands[1].shape if pieces == 1 else (pieces,) + operands[1].shape
    sems = pltpu.SemaphoreType.DMA((groups if pieces == 1 else pieces,))
    return pl.pallas_call(
        functools.partial(kernel, chunk=chunk, n_seq=n_seq),
        in_specs=[pl.BlockSpec(memory_space=pltpu.SMEM)] + [any_spec] * (len(operands) - 1),
        out_specs=any_spec,
        out_shape=jax.ShapeDtypeStruct((groups * n_seq, tokens, width), jnp.bfloat16),
        scratch_shapes=[pltpu.VMEM(held, jnp.bfloat16), sems, sems],
        input_output_aliases={} if out is None else {len(operands) - 1: 0},
        cost_estimate=pl.CostEstimate(flops=groups * tokens * width, bytes_accessed=4 * groups * tokens * width, transcendentals=0),
    )(*operands)


def grad_kernel(*refs, blocks, moving, splits):
    acc_ref = refs[-1]
    n_out = sum(len(parts) for parts in splits)
    ins, outs = refs[:-1 - n_out], list(refs[-1 - n_out:-1])
    step = pl.program_id(0)

    @pl.when(step == 0)
    def _():
        acc_ref[...] = jnp.zeros(acc_ref.shape, jnp.float32)

    for index, terms in enumerate(blocks):
        for lhs, rhs, row, column in terms:
            part = dot(ins[lhs][...], ins[rhs][...], TN)
            acc_ref[index, row:row + part.shape[0], column:column + part.shape[1]] += part

    @pl.when(step == pl.num_programs(0) - 1)
    def _():
        for index, adds in enumerate(moving):
            for ref, row in adds:
                at = slice(row, row + ins[ref].shape[0])
                acc_ref[index, at, :] += ins[ref][...].astype(jnp.float32)
        for index, parts in enumerate(splits):
            for rows, cols in parts:
                out = outs.pop(0)
                out[...] = acc_ref[index, rows, cols].astype(out.dtype)


def grad_call(blocks, shape, moving, splits, dtype, rows=512):
    ins, specs, keys = [], [], {}

    def operand(array, block, width):
        key = (id(array), block, width)
        if key not in keys:
            keys[key] = len(ins)
            ins.append(array)
            specs.append(pl.BlockSpec((rows, width), lambda s, b=block: (s, b)))
        return keys[key]

    count = blocks[0][0][0].shape[0]
    terms = [[(operand(lhs, lb, lw), operand(rhs, rb, rw), row, col) for lhs, lb, lw, rhs, rb, rw, row, col in block] for block in blocks]
    adds = []
    for block in moving:
        found = []
        for array, row in block:
            found.append((len(ins), row))
            ins.append(array)
            specs.append(pl.BlockSpec(array.shape, lambda s: (0, 0)))
        adds.append(found)
    span = lambda at, size: len(range(*at.indices(size)))
    shapes = [(span(r, shape[0]), span(c, shape[1])) for parts in splits for r, c in parts]
    return pl.pallas_call(
        functools.partial(grad_kernel, blocks=terms, moving=adds, splits=splits),
        grid=(count // rows,),
        in_specs=specs,
        out_specs=[pl.BlockSpec(one, lambda s: (0, 0)) for one in shapes],
        out_shape=[jax.ShapeDtypeStruct(one, dtype) for one in shapes],
        scratch_shapes=[pltpu.VMEM((len(blocks), *shape), jnp.float32)],
        compiler_params=pltpu.CompilerParams(dimension_semantics=("arbitrary",), vmem_limit_bytes=60 * MIB),
        cost_estimate=pl.CostEstimate(flops=2 * len(blocks) * count * shape[0] * shape[1], bytes_accessed=sum(2 * count * spec.block_shape[1] for spec in specs), transcendentals=0),
    )(*ins)


def split_width(value, out_refs):
    width = out_refs[0].shape[1]
    for index, out_ref in enumerate(out_refs):
        out_ref[...] = value[:, index * width:(index + 1) * width].astype(out_ref.dtype)


def finish_y_kernel(x_ref, mixed_ref, bias_ref, *out_refs):
    split_width(x_ref[...].astype(jnp.float32) + mixed_ref[...].astype(jnp.float32) + bias_ref[...], out_refs)


def normalize(act):
    act = act.astype(jnp.float32)
    mean = act.mean(-1, keepdims=True)
    inv_std = lax.rsqrt((act * act).mean(-1, keepdims=True) - mean * mean + LN_EPS)
    return (act - mean) * inv_std, inv_std


def finish_dx_kernel(x_ref, a6_ref, cot_ref, *out_refs):
    x_hat, inv_std = normalize(x_ref[...])
    value_a6 = a6_ref[...].astype(jnp.float32)
    mean_a6 = value_a6.mean(-1, keepdims=True)
    mean_a6x = (value_a6 * x_hat).mean(-1, keepdims=True)
    split_width(cot_ref[...].astype(jnp.float32) + inv_std * (value_a6 - mean_a6 - x_hat * mean_a6x), out_refs)


def row_call(kernel, parts, index, rows, *operands):
    width = operands[0].shape[1]
    specs = [pl.BlockSpec((min(rows, op.shape[0]), width), lambda s, i=(index if op.shape[0] > rows else 0): (i, 0)) for op in operands]
    return pl.pallas_call(
        kernel,
        grid=(1,),
        in_specs=specs,
        out_specs=[pl.BlockSpec((rows, width // parts), lambda s: (0, 0))] * parts,
        out_shape=[jax.ShapeDtypeStruct((rows, width // parts), jnp.bfloat16)] * parts,
        compiler_params=pltpu.CompilerParams(vmem_limit_bytes=16 * MIB),
        cost_estimate=pl.CostEstimate(flops=16 * rows * width, bytes_accessed=8 * rows * width, transcendentals=0),
    )(*operands)


def sublane_sum(value):
    return value.reshape(value.shape[0] // 8, 8, value.shape[1]).sum(0)


def norm_kernel(x_ref, small_ref, h_attn_ref, h_mlp_ref):
    @pl.loop(0, x_ref.shape[0] // LN_ROWS)
    def _(step):
        at = pl.ds(pl.multiple_of(step * LN_ROWS, LN_ROWS), LN_ROWS)
        x_hat, _ = normalize(x_ref[at, :])
        h_attn_ref[at, :] = (x_hat * small_ref[0:1, :] + small_ref[1:2, :]).astype(jnp.bfloat16)
        h_mlp_ref[at, :] = (x_hat * small_ref[2:3, :] + small_ref[3:4, :]).astype(jnp.bfloat16)


def offsets(refs, axis):
    starts = [0]
    for ref in refs:
        starts.append(starts[-1] + ref.shape[axis])
    return list(zip(refs, starts, starts[1:]))


def front_kernel(h_attn_ref, h_mlp_ref, cos_ref, lo_ref, hi_ref, b_qkv_ref, b_up_ref, *refs):
    w_refs, (qkv_ref, pre_ref, gelu_ref) = refs[:-3], refs[-3:]
    qkv_width = qkv_ref.shape[1]
    head = qkv_width // 3

    def project(h_ref, cols):
        return sum(dot(h_ref[:, start:stop], w_ref[:, cols], NN) for w_ref, start, stop in offsets(w_refs, 0))

    for low in range(0, qkv_width, head):
        at = slice(low, low + head)
        part = (project(h_attn_ref, at) + b_qkv_ref[:, at]).astype(jnp.bfloat16)
        if low < 2 * head:
            part = rotate(part.astype(jnp.float32), cos_ref[...], lo_ref[...], hi_ref[...], head // ROTARY_DIVISOR // 2, 1.0).astype(jnp.bfloat16)
        qkv_ref[:, at] = part
    for low in range(0, pre_ref.shape[1], TILE):
        at = slice(low, low + TILE)
        pre = (project(h_mlp_ref, slice(qkv_width + low, qkv_width + low + TILE)) + b_up_ref[:, at]).astype(jnp.bfloat16)
        pre_ref[:, at] = pre
        wide = pre.astype(jnp.float32)
        gelu_ref[:, at] = (0.5 * wide * (1.0 + lax.erf(wide * SQRT_HALF))).astype(jnp.bfloat16)


def y_kernel(ctx_ref, gelu_ref, *refs):
    w_refs, y_ref = refs[:-1], refs[-1]
    head = ctx_ref.shape[1]
    places, _, own, _ = y_ref.shape
    for w_ref, start, stop in offsets(w_refs, 1):
        acc = dot(ctx_ref[...], w_ref[:head, :], NN) + dot(gelu_ref[...], w_ref[head:, :], NN)
        y_ref[:, 0, :, start:stop] = acc.astype(jnp.bfloat16).reshape(places, own, stop - start)


def d_pre_kernel(cot_ref, pre_ref, *refs):
    w_refs, (d_ctx_ref, d_pre_ref, d_bias_ref) = refs[:-3], refs[-3:]

    def back(low, high):
        return sum(dot(cot_ref[:, start:stop], w_ref[low:high, :], NT) for w_ref, start, stop in offsets(w_refs, 1)).astype(jnp.bfloat16)

    head = d_ctx_ref.shape[1]

    @pl.when(pl.program_id(0) == 0)
    def _():
        d_bias_ref[...] = jnp.zeros(d_bias_ref.shape, jnp.float32)

    d_ctx_ref[...] = back(0, head)
    for low in range(0, d_pre_ref.shape[1], TILE):
        at = slice(low, low + TILE)
        d_gelu = back(head + low, head + low + TILE).astype(jnp.float32)
        pre = pre_ref[:, at].astype(jnp.float32)
        slope = 0.5 * (1.0 + lax.erf(pre * SQRT_HALF)) + pre * (jnp.exp(-0.5 * pre * pre) * INV_SQRT_2PI)
        d_pre = (d_gelu * slope).astype(jnp.bfloat16)
        d_pre_ref[:, at] = d_pre
        d_bias_ref[:, at] += sublane_sum(d_pre.astype(jnp.float32))


def d_h_kernel(d_qkv_ref, d_pre_ref, x_ref, small_ref, *refs):
    w_refs, (a6_ref, sums_ref) = refs[:-2], refs[-2:]
    qkv_width = d_qkv_ref.shape[1]

    @pl.when(pl.program_id(0) == 0)
    def _():
        sums_ref[...] = jnp.zeros(sums_ref.shape, jnp.float32)

    x_float = x_ref[...].astype(jnp.float32)
    mean = x_float.mean(-1, keepdims=True)
    inv_std = lax.rsqrt((x_float * x_float).mean(-1, keepdims=True) - mean * mean + LN_EPS)
    for w_ref, start, stop in offsets(w_refs, 0):
        for low in range(0, stop - start, TILE):
            part = slice(low, min(low + TILE, stop - start))
            at = slice(start + part.start, start + part.stop)
            d_attn = dot(d_qkv_ref[...], w_ref[part, :qkv_width], NT).astype(jnp.bfloat16).astype(jnp.float32)
            d_mlp = dot(d_pre_ref[...], w_ref[part, qkv_width:], NT).astype(jnp.bfloat16).astype(jnp.float32)
            a6_ref[:, at] = (d_attn * small_ref[0:1, at] + d_mlp * small_ref[2:3, at]).astype(jnp.bfloat16)
            x_hat = (x_ref[:, at].astype(jnp.float32) - mean) * inv_std
            sums_ref[0, :, at] += sublane_sum(d_attn * x_hat)
            sums_ref[1, :, at] += sublane_sum(d_attn)
            sums_ref[2, :, at] += sublane_sum(d_mlp * x_hat)
            sums_ref[3, :, at] += sublane_sum(d_mlp)


def tile_call(kernel, tiled, whole, outs, row_range, flops, rows=512):
    start, count = row_range
    rows = next(r for r in (rows, 256, 128, 64, count) if count % r == 0 and all(op.shape[0] % r == 0 for op in tiled))
    first = start // rows

    def tile_spec(op):
        blocks = op.shape[0] // rows
        if blocks * rows < count:
            return pl.BlockSpec((rows, op.shape[1]), lambda s: (lax.rem(s, blocks), 0))
        return pl.BlockSpec((rows, op.shape[1]), lambda s, f=(first if op.shape[0] != count else 0): (s + f, 0))

    in_specs = [tile_spec(op) for op in tiled]
    in_specs += [pl.BlockSpec(op.shape, lambda s, n=op.ndim: (0,) * n, pipeline_mode=pl.Buffered(1)) for op in whole]
    out_specs, out_shapes = [], []
    for form, dtype in outs:
        if isinstance(form, int):
            out_specs.append(pl.BlockSpec((rows, form), lambda s: (s, 0)))
            out_shapes.append(jax.ShapeDtypeStruct((count, form), dtype))
        elif isinstance(form[0], tuple):
            out_specs.append(pl.BlockSpec(form[1], form[2]))
            out_shapes.append(jax.ShapeDtypeStruct(form[0], dtype))
        else:
            out_specs.append(pl.BlockSpec(form, lambda s, n=len(form): (0,) * n))
            out_shapes.append(jax.ShapeDtypeStruct(form, dtype))
    moved = sum(2 * op.shape[1] * count for op in tiled) + sum(2 * op.size for op in whole) + sum(2 * shape.size for shape in out_shapes)
    return pl.pallas_call(
        kernel,
        grid=(count // rows,),
        in_specs=in_specs,
        out_specs=out_specs,
        out_shape=out_shapes,
        compiler_params=pltpu.CompilerParams(dimension_semantics=("arbitrary",), vmem_limit_bytes=60 * MIB),
        cost_estimate=pl.CostEstimate(flops=flops, bytes_accessed=moved, transcendentals=0),
    )(*tiled, *whole)


def solution(mesh):
    tx_size, ty_size = mesh.shape['tx'], mesh.shape['ty']
    act_spec = P('dp', None, 'tx')
    width_spec = P('tx')
    in_specs = (act_spec, act_spec, width_spec, width_spec, width_spec, width_spec, P('tx', 'ty', None), P('ty', None), P('ty', 'tx'), width_spec, P('tx', 'ty'), P('ty'), P('ty', 'tx'), width_spec)
    width_out = P(('dp', 'tx'))
    out_specs = (act_spec, act_spec, width_out, width_out, width_out, width_out, P(('dp', 'tx'), 'ty', None), P(('dp', 'ty'), None), P(('dp', 'ty'), 'tx'), width_out, P(('dp', 'tx'), 'ty'), P(('dp', 'ty')), P(('dp', 'ty'), 'tx'), width_out)
    antipode = tx_size // 2

    def shift(value, hops):
        return lax.ppermute(value, 'tx', [(s, (s - hops) % tx_size) for s in range(tx_size)])

    def small_sum(value, axis, size):
        step = 1
        while step < size:
            value = value + lax.ppermute(value, axis, [(s, s ^ step) for s in range(size)])
            step *= 2
        return value

    def along(value, hops):
        return lax.ppermute(value, 'ty', [(s, (s - 2 * hops) % ty_size) for s in range(ty_size)])

    def partner(value):
        return lax.ppermute(value, 'ty', [(s, s ^ 1) for s in range(ty_size)])

    def ring_gather(block, axis):
        blocks = {0: [block]}
        for hops in range(1, antipode):
            blocks[hops] = [shift(blocks[hops - 1][0], 1)]
            blocks[tx_size - hops] = [shift(blocks[(tx_size - hops + 1) % tx_size][0], -1)]
        half = block.shape[axis] // 2
        low = lax.slice_in_dim(blocks[antipode - 1][0], 0, half, axis=axis)
        high = lax.slice_in_dim(blocks[antipode + 1][0], half, 2 * half, axis=axis)
        blocks[antipode] = [shift(low, 1), shift(high, -1)]
        return [piece for r in range(tx_size) for piece in blocks[r]]

    def ring_scatter(make_blocks, shape):
        whole, half = slice(None), shape[0] // 2
        assert tx_size == 4
        low, high = grad_call([make_blocks(2)], shape, [[]], [[(slice(0, half), whole), (slice(half, None), whole)]], jnp.bfloat16)
        low, high = shift(low, -1), shift(high, 1)
        up, down = grad_call([make_blocks(1), make_blocks(3)], shape, [[(low, 0)], [(high, half)]], [[(whole, whole)], [(whole, whole)]], jnp.bfloat16)
        return [(shift(up, -1), 0), (shift(down, 1), 0)]

    def body(x_act, cot_out, ln1_gain, ln1_bias, ln2_gain, ln2_bias, w_qkv, b_qkv, w_dense, b_dense, w_up, b_up, w_down, b_down):
        batch, seq_len, d_local = x_act.shape
        n_seq = batch // tx_size
        own = seq_len // ty_size
        row, col = lax.axis_index('tx'), lax.axis_index('ty')
        qkv_width = w_qkv.shape[1] * w_qkv.shape[2]
        head = qkv_width // 3
        chunks = range(n_seq)
        tables = rotary_tables(seq_len, head // ROTARY_DIVISOR)
        attn_fwd, attn_bwd = attention_calls(n_seq, seq_len, head, tables)

        def to_tokens(act):
            parts = act.reshape(tx_size, n_seq, ty_size, own, d_local)
            pick = lambda index: lax.dynamic_slice(parts, (index, 0, col, 0, 0), (1, n_seq, 1, own, d_local)).reshape(n_seq, own, d_local)
            blocks = [pick(row)] + [shift(pick((row - r) % tx_size), r) for r in range(1, tx_size)]
            return jnp.concatenate(blocks, axis=2)

        place = jnp.stack([row, col // 2, col % 2])

        def to_width(parts):
            return jnp.stack([parts[0]] + [shift(parts[r], -r) for r in range(1, tx_size)])

        line = lax.broadcasted_iota(jnp.int32, (8, d_local), 0)
        small = jnp.zeros((8, d_local), jnp.bfloat16)
        for index, vector in enumerate((ln1_gain, ln1_bias, ln2_gain, ln2_bias, b_dense, b_down)):
            small = jnp.where(line == index, vector[None, :], small)
        small = [small] + [shift(small, r) for r in range(1, tx_size)]
        small = jnp.concatenate(small, axis=1).astype(jnp.float32)
        bias_out = small[4] + small[5]
        x_own = to_tokens(x_act)
        cot_own = to_tokens(cot_out)
        x_group = lax.all_gather(x_own, 'ty', axis=1, tiled=True)
        cot_group = lax.all_gather(cot_own, 'ty', axis=1, tiled=True)
        x_group, cot_group = x_group.reshape(n_seq * seq_len, -1), cot_group.reshape(n_seq * seq_len, -1)
        w_in = jnp.concatenate([w_qkv.reshape(d_local, qkv_width), w_up], axis=1)
        w_in = ring_gather(w_in, 0)
        w_back = jnp.concatenate([w_dense, w_down], axis=0)
        w_back = ring_gather(w_back, 1)
        in_size, back_size = sum(w.size for w in w_in), sum(w.size for w in w_back)

        n_tok, d_model = x_group.shape
        x_rows, cot_rows = x_own.reshape(-1, d_model), cot_own.reshape(-1, d_model)
        ff_width = w_up.shape[1]
        h_attn, h_mlp = tile_call(norm_kernel, [x_group], [small], [(d_model, jnp.bfloat16), (d_model, jnp.bfloat16)], (0, n_tok), 16 * x_group.size)
        qkv_act, pre_act, gelu_out = tile_call(
            front_kernel, [h_attn, h_mlp, *tables], [b_qkv.reshape(1, -1).astype(jnp.float32), b_up.reshape(1, -1).astype(jnp.float32), *w_in],
            [(qkv_width, jnp.bfloat16), (ff_width, jnp.bfloat16), (ff_width, jnp.bfloat16)], (0, n_tok), 2 * n_tok * in_size)
        qkv_seq = qkv_act.reshape(n_seq, seq_len, qkv_width)
        context = attn_fwd(qkv_seq).reshape(n_tok, head)
        blocks_per_seq = ty_size // 2
        y_form = ((ty_size, n_seq, own, d_model), (2, 1, own, d_model), lambda s: (lax.rem(s, blocks_per_seq), s // blocks_per_seq, 0, 0))
        (y_part,) = tile_call(y_kernel, [context, gelu_out], w_back, [(y_form, jnp.bfloat16)], (0, n_tok), 2 * n_tok * back_size, 2 * own)
        mixed = lax.psum_scatter(y_part.reshape(n_tok, d_model), 'ty', scatter_dimension=0, tiled=True)
        blocks = to_width(row_call(finish_y_kernel, tx_size, 0, n_seq * own, x_rows, mixed, bias_out.reshape(1, -1)))
        full = lax.all_gather(blocks.reshape(tx_size * n_seq, own, d_local), 'ty', axis=1, tiled=True)
        y_out = place_call(place_kernel, place, [full.reshape(tx_size, n_seq * seq_len, d_local)], None, 0, 1, n_seq * seq_len)

        d_ctx, d_pre, d_b_up = tile_call(
            d_pre_kernel, [cot_group, pre_act], w_back,
            [(head, jnp.bfloat16), (ff_width, jnp.bfloat16), ((8, ff_width), jnp.float32)], (0, n_tok), 2 * n_tok * back_size)
        d_ctx, d_b_up = d_ctx.reshape(n_seq, seq_len, head), d_b_up.sum(0)
        d_b_qkv, d_ln, dx_act = [], [], None
        for s in chunks:
            d_qkv, d_b_seq = attn_bwd(qkv_seq, d_ctx, s, (d_qkv, sums) if s else ())
            d_b_qkv.append(d_b_seq.sum((0, 1)))
            a6_part, sums = tile_call(
                d_h_kernel, [d_qkv.reshape(n_tok, qkv_width), d_pre, x_group], [small, *w_in],
                [(d_model, jnp.bfloat16), ((4, 8, d_model), jnp.float32)], (s * seq_len, seq_len), 2 * seq_len * in_size)
            d_ln.append(sums)
            value_a6 = lax.psum_scatter(a6_part, 'ty', scatter_dimension=0, tiled=True)
            parts = row_call(finish_dx_kernel, tx_size, s, own, x_rows, value_a6, cot_rows)
            block = to_width(parts)
            blocks = [block] + [along(block, hops) for hops in range(1, ty_size // 2)]
            blocks = blocks + [partner(piece) for piece in blocks]
            dx_act = place_call(place_pieces_kernel, place, blocks, dx_act, s, n_seq, seq_len)
        d_qkv = d_qkv.reshape(n_tok, qkv_width)

        d_ln = sum(d_ln).sum(1).reshape(4, tx_size, d_local)
        d_bias = jnp.concatenate([sum(d_b_qkv), d_b_up]).reshape(4, -1)
        sent = [jnp.concatenate([d_ln[:, r], d_bias], axis=1) for r in range(tx_size)]
        got = [sent[0]] + [shift(sent[r], -r) for r in range(1, tx_size)]
        got = sum(got[r] + got[r + antipode] for r in range(antipode))
        d_bias = got[:, d_local:].reshape(-1)
        d_ln = small_sum(got[:, :d_local], 'ty', ty_size)
        d_b_out = cot_out.astype(jnp.float32).sum((0, 1))

        in_shape, back_shape = (d_local, qkv_width + ff_width), (head + ff_width, d_local)
        in_blocks = lambda r: [(h_attn, r, d_local, d_qkv, 0, qkv_width, 0, 0), (h_mlp, r, d_local, d_pre, 0, ff_width, 0, qkv_width)]
        back_blocks = lambda r: [(context, 0, head, cot_group, r, d_local, 0, 0), (gelu_out, 0, ff_width, cot_group, r, d_local, head, 0)]
        add_back = ring_scatter(back_blocks, back_shape)
        add_in = ring_scatter(in_blocks, in_shape)
        whole = slice(None)
        d_w_dense, d_w_down = grad_call([back_blocks(0)], back_shape, [add_back], [[(slice(0, head), whole), (slice(head, None), whole)]], jnp.float32)
        d_w_qkv, d_w_up = grad_call([in_blocks(0)], in_shape, [add_in], [[(whole, slice(0, qkv_width)), (whole, slice(qkv_width, None))]], jnp.float32)
        y_out = y_out.reshape(batch, seq_len, d_local)
        return (y_out, dx_act, d_ln[0], d_ln[1], d_ln[2], d_ln[3], d_w_qkv.reshape(w_qkv.shape), d_bias[:qkv_width].reshape(b_qkv.shape), d_w_dense, d_b_out, d_w_up, d_bias[qkv_width:], d_w_down, d_b_out)

    return jax.shard_map(body, mesh=mesh, in_specs=in_specs, out_specs=out_specs, check_vma=False)
```

```python
import functools
import jax
import jax.numpy as jnp
from jax import lax
from jax.experimental import pallas as pl
from jax.experimental.pallas import tpu as pltpu
from jax.sharding import PartitionSpec as P


LN_EPS = 1e-5
ROPE_BASE = 10000.0
ROTARY_DIVISOR = 4
LANES = 128
Q_ROWS = 256
LN_ROWS = 128
MIB = 1024 * 1024
TILE = 256
SQRT_HALF = 0.5 ** 0.5
INV_SQRT_2PI = 0.3989422804014327

NT = (((1,), (1,)), ((), ()))
TN = (((0,), (0,)), ((), ()))
NN = (((1,), (0,)), ((), ()))


def dot(a, b, dims):
    return lax.dot_general(a, b, dims, preferred_element_type=jnp.float32)


def rotary_tables(seq_len, rot_dim):
    half = rot_dim // 2
    lane = jnp.arange(LANES)
    freq_index = jnp.where(lane < half, lane, lane - half)
    inv_freq = ROPE_BASE ** (-(2 * freq_index).astype(jnp.float32) / rot_dim)
    angles = jnp.arange(seq_len, dtype=jnp.float32)[:, None] * inv_freq[None, :]
    inside = (lane < rot_dim)[None, :]
    cos_tab = jnp.where(inside, jnp.cos(angles), 1.0)
    sin = jnp.where(inside, jnp.sin(angles), 0.0)
    first = (lane < half)[None, :]
    return cos_tab, jnp.where(first, -sin, 0.0), jnp.where(first, 0.0, sin)


def rotate(part, cos_tab, sin_lo, sin_hi, half, sign):
    head = part[:, :LANES]
    forward = pltpu.roll(head, half, 1)
    backward = pltpu.roll(head, LANES - half, 1)
    mixed = head * cos_tab + sign * (backward * sin_lo + forward * sin_hi)
    return jnp.concatenate([mixed, part[:, LANES:]], axis=1)


def causal_probs(q_rows, keys, row_start, scale):
    scores = dot(q_rows, keys, NT) * scale
    rows = row_start + lax.broadcasted_iota(jnp.int32, scores.shape, 0)
    cols = lax.broadcasted_iota(jnp.int32, scores.shape, 1)
    scores = jnp.where(rows >= cols, scores, -1e30)
    exps = jnp.exp(scores - jnp.max(scores, axis=1, keepdims=True))
    return exps * (1.0 / jnp.sum(exps, axis=1, keepdims=True))


def attn_fwd_kernel(qkv_ref, ctx_ref, *, scale, span):
    seq_len, width = ctx_ref.shape[1:]
    for end in range(span, seq_len + 1, span):
        for start in range(end - span, end, Q_ROWS):
            rows = slice(start, start + Q_ROWS)
            probs = causal_probs(qkv_ref[0, rows, :width], qkv_ref[0, :end, width:2 * width], start, scale).astype(jnp.bfloat16)
            ctx_ref[0, rows, :] = dot(probs, qkv_ref[0, :end, 2 * width:], NN).astype(jnp.bfloat16)


def attn_bwd_kernel(qkv_ref, dctx_ref, cos_ref, lo_ref, hi_ref, dqkv_ref, db_ref, dk_ref, dv_ref, *, half, scale, span):
    seq_len, width = dctx_ref.shape[1:]
    dk_ref[...] = jnp.zeros(dk_ref.shape, jnp.float32)
    dv_ref[...] = jnp.zeros(dv_ref.shape, jnp.float32)
    db_ref[...] = jnp.zeros(db_ref.shape, jnp.float32)

    def store(rows, col, grad_rot, turn):
        grad = grad_rot.astype(jnp.bfloat16)
        if turn:
            wide = grad.astype(jnp.float32)
            grad = rotate(wide, cos_ref[rows, :], lo_ref[rows, :], hi_ref[rows, :], half, -1.0).astype(jnp.bfloat16)
        dqkv_ref[0, rows, col:col + width] = grad
        db_ref[0, :, col:col + width] += sublane_sum(grad.astype(jnp.float32))

    for end in range(span, seq_len + 1, span):
        for start in range(end - span, end, Q_ROWS):
            rows = slice(start, start + Q_ROWS)
            q_rows, keys = qkv_ref[0, rows, :width], qkv_ref[0, :end, width:2 * width]
            dctx = dctx_ref[0, rows, :]
            probs = causal_probs(q_rows, keys, start, scale)
            dprobs = dot(dctx, qkv_ref[0, :end, 2 * width:], NT).astype(jnp.bfloat16).astype(jnp.float32)
            dv_ref[:end, :] += dot(probs.astype(jnp.bfloat16), dctx, TN)
            inner = jnp.sum(probs * dprobs, axis=1, keepdims=True)
            dscores = (probs * (dprobs - inner) * scale).astype(jnp.bfloat16)
            dk_ref[:end, :] += dot(dscores, q_rows, TN)
            store(rows, 0, dot(dscores, keys, NN), True)

    @pl.loop(0, seq_len // Q_ROWS)
    def _(step):
        rows = pl.ds(pl.multiple_of(step * Q_ROWS, Q_ROWS), Q_ROWS)
        store(rows, width, dk_ref[rows, :], True)
        store(rows, 2 * width, dv_ref[rows, :], False)


def attention_calls(n_seq, seq_len, width, tables):
    half = width // ROTARY_DIVISOR // 2
    scale = width ** -0.5
    span = 512 if seq_len % 512 == 0 else seq_len
    seq_spec = lambda cols, first=0: pl.BlockSpec((1, seq_len, cols), lambda s: (s + first, 0, 0))
    tab_spec = pl.BlockSpec((seq_len, LANES), lambda s: (0, 0))
    acc_scratch = pltpu.VMEM((seq_len, width), jnp.float32)
    pairs = seq_len * seq_len // 2
    params = pltpu.CompilerParams(dimension_semantics=("arbitrary",), vmem_limit_bytes=60 * MIB)

    def forward(qkv):
        return pl.pallas_call(
            functools.partial(attn_fwd_kernel, scale=scale, span=span),
            grid=(n_seq,),
            in_specs=[seq_spec(3 * width)],
            out_specs=seq_spec(width),
            out_shape=jax.ShapeDtypeStruct((n_seq, seq_len, width), jnp.bfloat16),
            compiler_params=params,
            name="af",
            cost_estimate=pl.CostEstimate(flops=8 * n_seq * pairs * width, bytes_accessed=8 * n_seq * seq_len * width, transcendentals=n_seq * pairs),
        )(qkv)

    def backward(qkv, dctx, index, into):
        kernel = functools.partial(attn_bwd_kernel, half=half, scale=scale, span=span)
        return pl.pallas_call(
            (lambda *refs: kernel(*refs[:5], *refs[5 + len(into):])),
            grid=(1,),
            in_specs=[seq_spec(3 * width, index), seq_spec(width, index), tab_spec, tab_spec, tab_spec] + [pl.BlockSpec(memory_space=pl.ANY)] * len(into),
            out_specs=[seq_spec(3 * width, index), pl.BlockSpec((1, 8, 3 * width), lambda s: (s, 0, 0))],
            input_output_aliases={5: 0} if into else {},
            out_shape=[jax.ShapeDtypeStruct((n_seq, seq_len, 3 * width), jnp.bfloat16), jax.ShapeDtypeStruct((1, 8, 3 * width), jnp.float32)],
            scratch_shapes=[acc_scratch, acc_scratch],
            compiler_params=params,
            name="ab",
            cost_estimate=pl.CostEstimate(flops=20 * pairs * width, bytes_accessed=14 * seq_len * width, transcendentals=pairs),
        )(qkv, dctx, *tables, *into)

    return forward, backward


def place_kernel(place_ref, full_ref, *rest, chunk, n_seq):
    out_ref, held_ref, in_sems, out_sems = rest[-4:]
    groups = full_ref.shape[0]
    fetch = [pltpu.make_async_copy(full_ref.at[lax.rem(place_ref[0] + groups - t, groups)], held_ref.at[t], in_sems.at[t]) for t in range(groups)]
    store = [pltpu.make_async_copy(held_ref.at[t], out_ref.at[t * n_seq + chunk], out_sems.at[t]) for t in range(groups)]
    for copy in fetch:
        copy.start()
    for t in range(groups):
        fetch[t].wait()
        store[t].start()
    for copy in store:
        copy.wait()


def place_pieces_kernel(place_ref, *refs, chunk, n_seq):
    out_ref, held_ref, in_sems, out_sems = refs[-4:]
    groups, own, _ = refs[0].shape
    columns = held_ref.shape[0] // 2
    row, column, core = place_ref[0], place_ref[1], place_ref[2]
    fetch, store = [], []
    for index in range(2 * columns):
        source = 2 * lax.rem(column + index % columns, columns) + (core if index < columns else 1 - core)
        at = pl.ds(pl.multiple_of(source * own, own), own)
        fetch.append(pltpu.make_async_copy(refs[index], held_ref.at[index], in_sems.at[index]))
        for t in range(groups):
            piece = held_ref.at[index, lax.rem(row + groups - t, groups)]
            store.append(pltpu.make_async_copy(piece, out_ref.at[t * n_seq + chunk, at], out_sems.at[index]))
    for copy in fetch:
        copy.start()
    for index in range(2 * columns):
        fetch[index].wait()
        for copy in store[index * groups:(index + 1) * groups]:
            copy.start()
    for copy in store:
        copy.wait()


def place_call(kernel, place, operands, out, chunk, n_seq, tokens):
    groups, _, width = operands[0].shape
    operands = [place, *operands] + ([] if out is None else [out])
    any_spec = pl.BlockSpec(memory_space=pl.ANY)
    pieces = len(operands) - 1 - (out is not None)
    held = operands[1].shape if pieces == 1 else (pieces,) + operands[1].shape
    sems = pltpu.SemaphoreType.DMA((groups if pieces == 1 else pieces,))
    return pl.pallas_call(
        functools.partial(kernel, chunk=chunk, n_seq=n_seq),
        in_specs=[pl.BlockSpec(memory_space=pltpu.SMEM)] + [any_spec] * (len(operands) - 1),
        out_specs=any_spec,
        out_shape=jax.ShapeDtypeStruct((groups * n_seq, tokens, width), jnp.bfloat16),
        scratch_shapes=[pltpu.VMEM(held, jnp.bfloat16), sems, sems],
        input_output_aliases={} if out is None else {len(operands) - 1: 0},
        cost_estimate=pl.CostEstimate(flops=groups * tokens * width, bytes_accessed=4 * groups * tokens * width, transcendentals=0),
    )(*operands)


def grad_kernel(*refs, blocks, moving, splits):
    acc_ref = refs[-1]
    n_out = sum(len(parts) for parts in splits)
    ins, outs = refs[:-1 - n_out], list(refs[-1 - n_out:-1])
    step = pl.program_id(0)

    @pl.when(step == 0)
    def _():
        acc_ref[...] = jnp.zeros(acc_ref.shape, jnp.float32)

    for index, terms in enumerate(blocks):
        for lhs, rhs, row, column in terms:
            part = dot(ins[lhs][...], ins[rhs][...], TN)
            acc_ref[index, row:row + part.shape[0], column:column + part.shape[1]] += part

    @pl.when(step == pl.num_programs(0) - 1)
    def _():
        for index, adds in enumerate(moving):
            for ref, row in adds:
                at = slice(row, row + ins[ref].shape[0])
                acc_ref[index, at, :] += ins[ref][...].astype(jnp.float32)
        for index, parts in enumerate(splits):
            for rows, cols in parts:
                out = outs.pop(0)
                out[...] = acc_ref[index, rows, cols].astype(out.dtype)


def grad_call(blocks, shape, moving, splits, dtype, rows=512):
    ins, specs, keys = [], [], {}

    def operand(array, block, width):
        key = (id(array), block, width)
        if key not in keys:
            keys[key] = len(ins)
            ins.append(array)
            specs.append(pl.BlockSpec((rows, width), lambda s, b=block: (s, b)))
        return keys[key]

    count = blocks[0][0][0].shape[0]
    terms = [[(operand(lhs, lb, lw), operand(rhs, rb, rw), row, col) for lhs, lb, lw, rhs, rb, rw, row, col in block] for block in blocks]
    adds = []
    for block in moving:
        found = []
        for array, row in block:
            found.append((len(ins), row))
            ins.append(array)
            specs.append(pl.BlockSpec(array.shape, lambda s: (0, 0)))
        adds.append(found)
    span = lambda at, size: len(range(*at.indices(size)))
    shapes = [(span(r, shape[0]), span(c, shape[1])) for parts in splits for r, c in parts]
    return pl.pallas_call(
        functools.partial(grad_kernel, blocks=terms, moving=adds, splits=splits),
        grid=(count // rows,),
        in_specs=specs,
        out_specs=[pl.BlockSpec(one, lambda s: (0, 0)) for one in shapes],
        out_shape=[jax.ShapeDtypeStruct(one, dtype) for one in shapes],
        scratch_shapes=[pltpu.VMEM((len(blocks), *shape), jnp.float32)],
        compiler_params=pltpu.CompilerParams(dimension_semantics=("arbitrary",), vmem_limit_bytes=60 * MIB),
        cost_estimate=pl.CostEstimate(flops=2 * len(blocks) * count * shape[0] * shape[1], bytes_accessed=sum(2 * count * spec.block_shape[1] for spec in specs), transcendentals=0),
    )(*ins)


def split_width(value, out_refs):
    width = out_refs[0].shape[1]
    for index, out_ref in enumerate(out_refs):
        out_ref[...] = value[:, index * width:(index + 1) * width].astype(out_ref.dtype)


def finish_y_kernel(x_ref, mixed_ref, bias_ref, *out_refs):
    split_width(x_ref[...].astype(jnp.float32) + mixed_ref[...].astype(jnp.float32) + bias_ref[...], out_refs)


def normalize(act):
    act = act.astype(jnp.float32)
    mean = act.mean(-1, keepdims=True)
    inv_std = lax.rsqrt((act * act).mean(-1, keepdims=True) - mean * mean + LN_EPS)
    return (act - mean) * inv_std, inv_std


def finish_dx_kernel(x_ref, a6_ref, cot_ref, *out_refs):
    x_hat, inv_std = normalize(x_ref[...])
    value_a6 = a6_ref[...].astype(jnp.float32)
    mean_a6 = value_a6.mean(-1, keepdims=True)
    mean_a6x = (value_a6 * x_hat).mean(-1, keepdims=True)
    split_width(cot_ref[...].astype(jnp.float32) + inv_std * (value_a6 - mean_a6 - x_hat * mean_a6x), out_refs)


def row_call(kernel, parts, index, rows, *operands):
    width = operands[0].shape[1]
    specs = [pl.BlockSpec((min(rows, op.shape[0]), width), lambda s, i=(index if op.shape[0] > rows else 0): (i, 0)) for op in operands]
    return pl.pallas_call(
        kernel,
        grid=(1,),
        in_specs=specs,
        out_specs=[pl.BlockSpec((rows, width // parts), lambda s: (0, 0))] * parts,
        out_shape=[jax.ShapeDtypeStruct((rows, width // parts), jnp.bfloat16)] * parts,
        compiler_params=pltpu.CompilerParams(vmem_limit_bytes=16 * MIB),
        cost_estimate=pl.CostEstimate(flops=16 * rows * width, bytes_accessed=8 * rows * width, transcendentals=0),
    )(*operands)


def sublane_sum(value):
    return value.reshape(value.shape[0] // 8, 8, value.shape[1]).sum(0)


def norm_kernel(x_ref, small_ref, h_attn_ref, h_mlp_ref):
    @pl.loop(0, x_ref.shape[0] // LN_ROWS)
    def _(step):
        at = pl.ds(pl.multiple_of(step * LN_ROWS, LN_ROWS), LN_ROWS)
        x_hat, _ = normalize(x_ref[at, :])
        h_attn_ref[at, :] = (x_hat * small_ref[0:1, :] + small_ref[1:2, :]).astype(jnp.bfloat16)
        h_mlp_ref[at, :] = (x_hat * small_ref[2:3, :] + small_ref[3:4, :]).astype(jnp.bfloat16)


def offsets(refs, axis):
    starts = [0]
    for ref in refs:
        starts.append(starts[-1] + ref.shape[axis])
    return list(zip(refs, starts, starts[1:]))


def front_kernel(h_attn_ref, h_mlp_ref, cos_ref, lo_ref, hi_ref, b_qkv_ref, b_up_ref, *refs):
    w_refs, (qkv_ref, pre_ref, gelu_ref) = refs[:-3], refs[-3:]
    qkv_width = qkv_ref.shape[1]
    head = qkv_width // 3

    def project(h_ref, cols):
        return sum(dot(h_ref[:, start:stop], w_ref[:, cols], NN) for w_ref, start, stop in offsets(w_refs, 0))

    for low in range(0, qkv_width, head):
        at = slice(low, low + head)
        part = (project(h_attn_ref, at) + b_qkv_ref[:, at]).astype(jnp.bfloat16)
        if low < 2 * head:
            part = rotate(part.astype(jnp.float32), cos_ref[...], lo_ref[...], hi_ref[...], head // ROTARY_DIVISOR // 2, 1.0).astype(jnp.bfloat16)
        qkv_ref[:, at] = part
    for low in range(0, pre_ref.shape[1], TILE):
        at = slice(low, low + TILE)
        pre = (project(h_mlp_ref, slice(qkv_width + low, qkv_width + low + TILE)) + b_up_ref[:, at]).astype(jnp.bfloat16)
        pre_ref[:, at] = pre
        wide = pre.astype(jnp.float32)
        gelu_ref[:, at] = (0.5 * wide * (1.0 + lax.erf(wide * SQRT_HALF))).astype(jnp.bfloat16)


def y_kernel(ctx_ref, gelu_ref, *refs):
    w_refs, y_ref = refs[:-1], refs[-1]
    head = ctx_ref.shape[1]
    places, _, own, _ = y_ref.shape
    for w_ref, start, stop in offsets(w_refs, 1):
        acc = dot(ctx_ref[...], w_ref[:head, :], NN) + dot(gelu_ref[...], w_ref[head:, :], NN)
        y_ref[:, 0, :, start:stop] = acc.astype(jnp.bfloat16).reshape(places, own, stop - start)


def d_pre_kernel(cot_ref, pre_ref, *refs):
    w_refs, (d_ctx_ref, d_pre_ref, d_bias_ref) = refs[:-3], refs[-3:]

    def back(low, high):
        return sum(dot(cot_ref[:, start:stop], w_ref[low:high, :], NT) for w_ref, start, stop in offsets(w_refs, 1)).astype(jnp.bfloat16)

    head = d_ctx_ref.shape[1]

    @pl.when(pl.program_id(0) == 0)
    def _():
        d_bias_ref[...] = jnp.zeros(d_bias_ref.shape, jnp.float32)

    d_ctx_ref[...] = back(0, head)
    for low in range(0, d_pre_ref.shape[1], TILE):
        at = slice(low, low + TILE)
        d_gelu = back(head + low, head + low + TILE).astype(jnp.float32)
        pre = pre_ref[:, at].astype(jnp.float32)
        slope = 0.5 * (1.0 + lax.erf(pre * SQRT_HALF)) + pre * (jnp.exp(-0.5 * pre * pre) * INV_SQRT_2PI)
        d_pre = (d_gelu * slope).astype(jnp.bfloat16)
        d_pre_ref[:, at] = d_pre
        d_bias_ref[:, at] += sublane_sum(d_pre.astype(jnp.float32))


def d_h_kernel(d_qkv_ref, d_pre_ref, x_ref, small_ref, *refs):
    w_refs, (a6_ref, sums_ref) = refs[:-2], refs[-2:]
    qkv_width = d_qkv_ref.shape[1]

    @pl.when(pl.program_id(0) == 0)
    def _():
        sums_ref[...] = jnp.zeros(sums_ref.shape, jnp.float32)

    x_float = x_ref[...].astype(jnp.float32)
    mean = x_float.mean(-1, keepdims=True)
    inv_std = lax.rsqrt((x_float * x_float).mean(-1, keepdims=True) - mean * mean + LN_EPS)
    for w_ref, start, stop in offsets(w_refs, 0):
        for low in range(0, stop - start, TILE):
            part = slice(low, min(low + TILE, stop - start))
            at = slice(start + part.start, start + part.stop)
            d_attn = dot(d_qkv_ref[...], w_ref[part, :qkv_width], NT).astype(jnp.bfloat16).astype(jnp.float32)
            d_mlp = dot(d_pre_ref[...], w_ref[part, qkv_width:], NT).astype(jnp.bfloat16).astype(jnp.float32)
            a6_ref[:, at] = (d_attn * small_ref[0:1, at] + d_mlp * small_ref[2:3, at]).astype(jnp.bfloat16)
            x_hat = (x_ref[:, at].astype(jnp.float32) - mean) * inv_std
            sums_ref[0, :, at] += sublane_sum(d_attn * x_hat)
            sums_ref[1, :, at] += sublane_sum(d_attn)
            sums_ref[2, :, at] += sublane_sum(d_mlp * x_hat)
            sums_ref[3, :, at] += sublane_sum(d_mlp)


def tile_call(kernel, tiled, whole, outs, row_range, flops, rows=512):
    start, count = row_range
    rows = next(r for r in (rows, 256, 128, 64, count) if count % r == 0 and all(op.shape[0] % r == 0 for op in tiled))
    first = start // rows

    def tile_spec(op):
        blocks = op.shape[0] // rows
        if blocks * rows < count:
            return pl.BlockSpec((rows, op.shape[1]), lambda s: (lax.rem(s, blocks), 0))
        return pl.BlockSpec((rows, op.shape[1]), lambda s, f=(first if op.shape[0] != count else 0): (s + f, 0))

    in_specs = [tile_spec(op) for op in tiled]
    in_specs += [pl.BlockSpec(op.shape, lambda s, n=op.ndim: (0,) * n, pipeline_mode=pl.Buffered(1)) for op in whole]
    out_specs, out_shapes = [], []
    for form, dtype in outs:
        if isinstance(form, int):
            out_specs.append(pl.BlockSpec((rows, form), lambda s: (s, 0)))
            out_shapes.append(jax.ShapeDtypeStruct((count, form), dtype))
        elif isinstance(form[0], tuple):
            out_specs.append(pl.BlockSpec(form[1], form[2]))
            out_shapes.append(jax.ShapeDtypeStruct(form[0], dtype))
        else:
            out_specs.append(pl.BlockSpec(form, lambda s, n=len(form): (0,) * n))
            out_shapes.append(jax.ShapeDtypeStruct(form, dtype))
    moved = sum(2 * op.shape[1] * count for op in tiled) + sum(2 * op.size for op in whole) + sum(2 * shape.size for shape in out_shapes)
    return pl.pallas_call(
        kernel,
        grid=(count // rows,),
        in_specs=in_specs,
        out_specs=out_specs,
        out_shape=out_shapes,
        compiler_params=pltpu.CompilerParams(dimension_semantics=("arbitrary",), vmem_limit_bytes=60 * MIB),
        cost_estimate=pl.CostEstimate(flops=flops, bytes_accessed=moved, transcendentals=0),
    )(*tiled, *whole)


def solution(mesh):
    tx_size, ty_size = mesh.shape['tx'], mesh.shape['ty']
    act_spec = P('dp', None, 'tx')
    width_spec = P('tx')
    in_specs = (act_spec, act_spec, width_spec, width_spec, width_spec, width_spec, P('tx', 'ty', None), P('ty', None), P('ty', 'tx'), width_spec, P('tx', 'ty'), P('ty'), P('ty', 'tx'), width_spec)
    width_out = P(('dp', 'tx'))
    out_specs = (act_spec, act_spec, width_out, width_out, width_out, width_out, P(('dp', 'tx'), 'ty', None), P(('dp', 'ty'), None), P(('dp', 'ty'), 'tx'), width_out, P(('dp', 'tx'), 'ty'), P(('dp', 'ty')), P(('dp', 'ty'), 'tx'), width_out)
    antipode = tx_size // 2

    def shift(value, hops):
        return lax.ppermute(value, 'tx', [(s, (s - hops) % tx_size) for s in range(tx_size)])

    def small_sum(value, axis, size):
        step = 1
        while step < size:
            value = value + lax.ppermute(value, axis, [(s, s ^ step) for s in range(size)])
            step *= 2
        return value

    def along(value, hops):
        return lax.ppermute(value, 'ty', [(s, (s - 2 * hops) % ty_size) for s in range(ty_size)])

    def partner(value):
        return lax.ppermute(value, 'ty', [(s, s ^ 1) for s in range(ty_size)])

    def ring_gather(block, axis):
        blocks = {0: [block]}
        for hops in range(1, antipode):
            blocks[hops] = [shift(blocks[hops - 1][0], 1)]
            blocks[tx_size - hops] = [shift(blocks[(tx_size - hops + 1) % tx_size][0], -1)]
        half = block.shape[axis] // 2
        low = lax.slice_in_dim(blocks[antipode - 1][0], 0, half, axis=axis)
        high = lax.slice_in_dim(blocks[antipode + 1][0], half, 2 * half, axis=axis)
        blocks[antipode] = [shift(low, 1), shift(high, -1)]
        return [piece for r in range(tx_size) for piece in blocks[r]]

    def ring_scatter(make_blocks, shape):
        whole, half = slice(None), shape[0] // 2
        assert tx_size == 4
        low, high = grad_call([make_blocks(2)], shape, [[]], [[(slice(0, half), whole), (slice(half, None), whole)]], jnp.bfloat16)
        low, high = shift(low, -1), shift(high, 1)
        up, down = grad_call([make_blocks(1), make_blocks(3)], shape, [[(low, 0)], [(high, half)]], [[(whole, whole)], [(whole, whole)]], jnp.bfloat16)
        return [(shift(up, -1), 0), (shift(down, 1), 0)]

    def body(x_act, cot_out, ln1_gain, ln1_bias, ln2_gain, ln2_bias, w_qkv, b_qkv, w_dense, b_dense, w_up, b_up, w_down, b_down):
        batch, seq_len, d_local = x_act.shape
        n_seq = batch // tx_size
        own = seq_len // ty_size
        row, col = lax.axis_index('tx'), lax.axis_index('ty')
        qkv_width = w_qkv.shape[1] * w_qkv.shape[2]
        head = qkv_width // 3
        chunks = range(n_seq)
        tables = rotary_tables(seq_len, head // ROTARY_DIVISOR)
        attn_fwd, attn_bwd = attention_calls(n_seq, seq_len, head, tables)

        def to_tokens(act):
            parts = act.reshape(tx_size, n_seq, ty_size, own, d_local)
            pick = lambda index: lax.dynamic_slice(parts, (index, 0, col, 0, 0), (1, n_seq, 1, own, d_local)).reshape(n_seq, own, d_local)
            blocks = [pick(row)] + [shift(pick((row - r) % tx_size), r) for r in range(1, tx_size)]
            return jnp.concatenate(blocks, axis=2)

        place = jnp.stack([row, col // 2, col % 2])

        def to_width(parts):
            return jnp.stack([parts[0]] + [shift(parts[r], -r) for r in range(1, tx_size)])

        line = lax.broadcasted_iota(jnp.int32, (8, d_local), 0)
        small = jnp.zeros((8, d_local), jnp.bfloat16)
        for index, vector in enumerate((ln1_gain, ln1_bias, ln2_gain, ln2_bias, b_dense, b_down)):
            small = jnp.where(line == index, vector[None, :], small)
        small = [small] + [shift(small, r) for r in range(1, tx_size)]
        small = jnp.concatenate(small, axis=1).astype(jnp.float32)
        bias_out = small[4] + small[5]
        x_own = to_tokens(x_act)
        cot_own = to_tokens(cot_out)
        x_group = lax.all_gather(x_own, 'ty', axis=1, tiled=True)
        cot_group = lax.all_gather(cot_own, 'ty', axis=1, tiled=True)
        x_group, cot_group = x_group.reshape(n_seq * seq_len, -1), cot_group.reshape(n_seq * seq_len, -1)
        w_in = jnp.concatenate([w_qkv.reshape(d_local, qkv_width), w_up], axis=1)
        w_in = ring_gather(w_in, 0)
        w_back = jnp.concatenate([w_dense, w_down], axis=0)
        w_back = ring_gather(w_back, 1)
        in_size, back_size = sum(w.size for w in w_in), sum(w.size for w in w_back)

        n_tok, d_model = x_group.shape
        x_rows, cot_rows = x_own.reshape(-1, d_model), cot_own.reshape(-1, d_model)
        ff_width = w_up.shape[1]
        h_attn, h_mlp = tile_call(norm_kernel, [x_group], [small], [(d_model, jnp.bfloat16), (d_model, jnp.bfloat16)], (0, n_tok), 16 * x_group.size)
        qkv_act, pre_act, gelu_out = tile_call(
            front_kernel, [h_attn, h_mlp, *tables], [b_qkv.reshape(1, -1).astype(jnp.float32), b_up.reshape(1, -1).astype(jnp.float32), *w_in],
            [(qkv_width, jnp.bfloat16), (ff_width, jnp.bfloat16), (ff_width, jnp.bfloat16)], (0, n_tok), 2 * n_tok * in_size)
        qkv_seq = qkv_act.reshape(n_seq, seq_len, qkv_width)
        context = attn_fwd(qkv_seq).reshape(n_tok, head)
        blocks_per_seq = ty_size // 2
        y_form = ((ty_size, n_seq, own, d_model), (2, 1, own, d_model), lambda s: (lax.rem(s, blocks_per_seq), s // blocks_per_seq, 0, 0))
        (y_part,) = tile_call(y_kernel, [context, gelu_out], w_back, [(y_form, jnp.bfloat16)], (0, n_tok), 2 * n_tok * back_size, 2 * own)
        mixed = lax.psum_scatter(y_part.reshape(n_tok, d_model), 'ty', scatter_dimension=0, tiled=True)
        blocks = to_width(row_call(finish_y_kernel, tx_size, 0, n_seq * own, x_rows, mixed, bias_out.reshape(1, -1)))
        full = lax.all_gather(blocks.reshape(tx_size * n_seq, own, d_local), 'ty', axis=1, tiled=True)
        y_out = place_call(place_kernel, place, [full.reshape(tx_size, n_seq * seq_len, d_local)], None, 0, 1, n_seq * seq_len)

        d_ctx, d_pre, d_b_up = tile_call(
            d_pre_kernel, [cot_group, pre_act], w_back,
            [(head, jnp.bfloat16), (ff_width, jnp.bfloat16), ((8, ff_width), jnp.float32)], (0, n_tok), 2 * n_tok * back_size)
        d_ctx, d_b_up = d_ctx.reshape(n_seq, seq_len, head), d_b_up.sum(0)
        d_b_qkv, d_ln, dx_act = [], [], None
        for s in chunks:
            d_qkv, d_b_seq = attn_bwd(qkv_seq, d_ctx, s, (d_qkv, sums) if s else ())
            d_b_qkv.append(d_b_seq.sum((0, 1)))
            a6_part, sums = tile_call(
                d_h_kernel, [d_qkv.reshape(n_tok, qkv_width), d_pre, x_group], [small, *w_in],
                [(d_model, jnp.bfloat16), ((4, 8, d_model), jnp.float32)], (s * seq_len, seq_len), 2 * seq_len * in_size)
            d_ln.append(sums)
            value_a6 = lax.psum_scatter(a6_part, 'ty', scatter_dimension=0, tiled=True)
            parts = row_call(finish_dx_kernel, tx_size, s, own, x_rows, value_a6, cot_rows)
            block = to_width(parts)
            if s < n_seq - 1:
                blocks = [block] + [along(block, hops) for hops in range(1, ty_size // 2)]
                blocks = blocks + [partner(piece) for piece in blocks]
                dx_act = place_call(place_pieces_kernel, place, blocks, dx_act, s, n_seq, seq_len)
            else:
                full = lax.all_gather(block, 'ty', axis=1, tiled=True)
                dx_act = place_call(place_kernel, place, [full], dx_act, s, n_seq, seq_len)
        d_qkv = d_qkv.reshape(n_tok, qkv_width)

        d_ln = sum(d_ln).sum(1).reshape(4, tx_size, d_local)
        d_bias = jnp.concatenate([sum(d_b_qkv), d_b_up]).reshape(4, -1)
        sent = [jnp.concatenate([d_ln[:, r], d_bias], axis=1) for r in range(tx_size)]
        got = [sent[0]] + [shift(sent[r], -r) for r in range(1, tx_size)]
        got = sum(got[r] + got[r + antipode] for r in range(antipode))
        d_bias = got[:, d_local:].reshape(-1)
        d_ln = small_sum(got[:, :d_local], 'ty', ty_size)
        d_b_out = cot_out.astype(jnp.float32).sum((0, 1))

        in_shape, back_shape = (d_local, qkv_width + ff_width), (head + ff_width, d_local)
        in_blocks = lambda r: [(h_attn, r, d_local, d_qkv, 0, qkv_width, 0, 0), (h_mlp, r, d_local, d_pre, 0, ff_width, 0, qkv_width)]
        back_blocks = lambda r: [(context, 0, head, cot_group, r, d_local, 0, 0), (gelu_out, 0, ff_width, cot_group, r, d_local, head, 0)]
        add_back = ring_scatter(back_blocks, back_shape)
        add_in = ring_scatter(in_blocks, in_shape)
        whole = slice(None)
        d_w_dense, d_w_down = grad_call([back_blocks(0)], back_shape, [add_back], [[(slice(0, head), whole), (slice(head, None), whole)]], jnp.float32)
        d_w_qkv, d_w_up = grad_call([in_blocks(0)], in_shape, [add_in], [[(whole, slice(0, qkv_width)), (whole, slice(qkv_width, None))]], jnp.float32)
        y_out = y_out.reshape(batch, seq_len, d_local)
        return (y_out, dx_act, d_ln[0], d_ln[1], d_ln[2], d_ln[3], d_w_qkv.reshape(w_qkv.shape), d_bias[:qkv_width].reshape(b_qkv.shape), d_w_dense, d_b_out, d_w_up, d_bias[qkv_width:], d_w_down, d_b_out)

    return jax.shard_map(body, mesh=mesh, in_specs=in_specs, out_specs=out_specs, check_vma=False)
```

```python
import functools
import jax
import jax.numpy as jnp
from jax import lax
from jax.experimental import pallas as pl
from jax.experimental.pallas import tpu as pltpu
from jax.sharding import PartitionSpec as P


LN_EPS = 1e-5
ROPE_BASE = 10000.0
ROTARY_DIVISOR = 4
LANES = 128
Q_ROWS = 256
LN_ROWS = 128
MIB = 1024 * 1024
TILE = 256
SQRT_HALF = 0.5 ** 0.5
INV_SQRT_2PI = 0.3989422804014327

NT = (((1,), (1,)), ((), ()))
TN = (((0,), (0,)), ((), ()))
NN = (((1,), (0,)), ((), ()))


def dot(a, b, dims):
    return lax.dot_general(a, b, dims, preferred_element_type=jnp.float32)


def rotary_tables(seq_len, rot_dim):
    half = rot_dim // 2
    lane = jnp.arange(LANES)
    freq_index = jnp.where(lane < half, lane, lane - half)
    inv_freq = ROPE_BASE ** (-(2 * freq_index).astype(jnp.float32) / rot_dim)
    angles = jnp.arange(seq_len, dtype=jnp.float32)[:, None] * inv_freq[None, :]
    inside = (lane < rot_dim)[None, :]
    cos_tab = jnp.where(inside, jnp.cos(angles), 1.0)
    sin = jnp.where(inside, jnp.sin(angles), 0.0)
    first = (lane < half)[None, :]
    return cos_tab, jnp.where(first, -sin, 0.0), jnp.where(first, 0.0, sin)


def rotate(part, cos_tab, sin_lo, sin_hi, half, sign):
    head = part[:, :LANES]
    forward = pltpu.roll(head, half, 1)
    backward = pltpu.roll(head, LANES - half, 1)
    mixed = head * cos_tab + sign * (backward * sin_lo + forward * sin_hi)
    return jnp.concatenate([mixed, part[:, LANES:]], axis=1)


def causal_probs(q_rows, keys, row_start, scale):
    scores = dot(q_rows, keys, NT) * scale
    rows = row_start + lax.broadcasted_iota(jnp.int32, scores.shape, 0)
    cols = lax.broadcasted_iota(jnp.int32, scores.shape, 1)
    scores = jnp.where(rows >= cols, scores, -1e30)
    exps = jnp.exp(scores - jnp.max(scores, axis=1, keepdims=True))
    return exps * (1.0 / jnp.sum(exps, axis=1, keepdims=True))


def attn_fwd_kernel(qkv_ref, ctx_ref, *, scale, span):
    seq_len, width = ctx_ref.shape[1:]
    for end in range(span, seq_len + 1, span):
        for start in range(end - span, end, Q_ROWS):
            rows = slice(start, start + Q_ROWS)
            probs = causal_probs(qkv_ref[0, rows, :width], qkv_ref[0, :end, width:2 * width], start, scale).astype(jnp.bfloat16)
            ctx_ref[0, rows, :] = dot(probs, qkv_ref[0, :end, 2 * width:], NN).astype(jnp.bfloat16)


def attn_bwd_kernel(qkv_ref, dctx_ref, cos_ref, lo_ref, hi_ref, dqkv_ref, db_ref, dk_ref, dv_ref, *, half, scale, span):
    seq_len, width = dctx_ref.shape[1:]
    dk_ref[...] = jnp.zeros(dk_ref.shape, jnp.float32)
    dv_ref[...] = jnp.zeros(dv_ref.shape, jnp.float32)
    db_ref[...] = jnp.zeros(db_ref.shape, jnp.float32)

    def store(rows, col, grad_rot, turn):
        grad = grad_rot.astype(jnp.bfloat16)
        if turn:
            wide = grad.astype(jnp.float32)
            grad = rotate(wide, cos_ref[rows, :], lo_ref[rows, :], hi_ref[rows, :], half, -1.0).astype(jnp.bfloat16)
        dqkv_ref[0, rows, col:col + width] = grad
        db_ref[0, :, col:col + width] += sublane_sum(grad.astype(jnp.float32))

    for end in range(span, seq_len + 1, span):
        for start in range(end - span, end, Q_ROWS):
            rows = slice(start, start + Q_ROWS)
            q_rows, keys = qkv_ref[0, rows, :width], qkv_ref[0, :end, width:2 * width]
            dctx = dctx_ref[0, rows, :]
            probs = causal_probs(q_rows, keys, start, scale)
            dprobs = dot(dctx, qkv_ref[0, :end, 2 * width:], NT).astype(jnp.bfloat16).astype(jnp.float32)
            dv_ref[:end, :] += dot(probs.astype(jnp.bfloat16), dctx, TN)
            inner = jnp.sum(probs * dprobs, axis=1, keepdims=True)
            dscores = (probs * (dprobs - inner) * scale).astype(jnp.bfloat16)
            dk_ref[:end, :] += dot(dscores, q_rows, TN)
            store(rows, 0, dot(dscores, keys, NN), True)

    @pl.loop(0, seq_len // Q_ROWS)
    def _(step):
        rows = pl.ds(pl.multiple_of(step * Q_ROWS, Q_ROWS), Q_ROWS)
        store(rows, width, dk_ref[rows, :], True)
        store(rows, 2 * width, dv_ref[rows, :], False)


def attention_calls(n_seq, seq_len, width, tables):
    half = width // ROTARY_DIVISOR // 2
    scale = width ** -0.5
    span = 512 if seq_len % 512 == 0 else seq_len
    seq_spec = lambda cols, first=0: pl.BlockSpec((1, seq_len, cols), lambda s: (s + first, 0, 0))
    tab_spec = pl.BlockSpec((seq_len, LANES), lambda s: (0, 0))
    acc_scratch = pltpu.VMEM((seq_len, width), jnp.float32)
    pairs = seq_len * seq_len // 2
    params = pltpu.CompilerParams(dimension_semantics=("arbitrary",), vmem_limit_bytes=60 * MIB)

    def forward(qkv):
        return pl.pallas_call(
            functools.partial(attn_fwd_kernel, scale=scale, span=span),
            grid=(n_seq,),
            in_specs=[seq_spec(3 * width)],
            out_specs=seq_spec(width),
            out_shape=jax.ShapeDtypeStruct((n_seq, seq_len, width), jnp.bfloat16),
            compiler_params=params,
            name="af",
            cost_estimate=pl.CostEstimate(flops=8 * n_seq * pairs * width, bytes_accessed=8 * n_seq * seq_len * width, transcendentals=n_seq * pairs),
        )(qkv)

    def backward(qkv, dctx, index, into):
        kernel = functools.partial(attn_bwd_kernel, half=half, scale=scale, span=span)
        return pl.pallas_call(
            (lambda *refs: kernel(*refs[:5], *refs[5 + len(into):])),
            grid=(1,),
            in_specs=[seq_spec(3 * width, index), seq_spec(width, index), tab_spec, tab_spec, tab_spec] + [pl.BlockSpec(memory_space=pl.ANY)] * len(into),
            out_specs=[seq_spec(3 * width, index), pl.BlockSpec((1, 8, 3 * width), lambda s: (s, 0, 0))],
            input_output_aliases={5: 0} if into else {},
            out_shape=[jax.ShapeDtypeStruct((n_seq, seq_len, 3 * width), jnp.bfloat16), jax.ShapeDtypeStruct((1, 8, 3 * width), jnp.float32)],
            scratch_shapes=[acc_scratch, acc_scratch],
            compiler_params=params,
            name="ab",
            cost_estimate=pl.CostEstimate(flops=20 * pairs * width, bytes_accessed=14 * seq_len * width, transcendentals=pairs),
        )(qkv, dctx, *tables, *into)

    return forward, backward


def place_kernel(place_ref, full_ref, *rest, chunk, n_seq):
    out_ref, held_ref, in_sems, out_sems = rest[-4:]
    groups = full_ref.shape[0]
    fetch = [pltpu.make_async_copy(full_ref.at[lax.rem(place_ref[0] + groups - t, groups)], held_ref.at[t], in_sems.at[t]) for t in range(groups)]
    store = [pltpu.make_async_copy(held_ref.at[t], out_ref.at[t * n_seq + chunk], out_sems.at[t]) for t in range(groups)]
    for copy in fetch:
        copy.start()
    for t in range(groups):
        fetch[t].wait()
        store[t].start()
    for copy in store:
        copy.wait()


def place_pieces_kernel(place_ref, *refs, chunk, n_seq):
    out_ref, held_ref, in_sems, out_sems = refs[-4:]
    groups, own, _ = refs[0].shape
    columns = held_ref.shape[0] // 2
    row, column, core = place_ref[0], place_ref[1], place_ref[2]
    fetch, store = [], []
    for index in range(2 * columns):
        source = 2 * lax.rem(column + index % columns, columns) + (core if index < columns else 1 - core)
        at = pl.ds(pl.multiple_of(source * own, own), own)
        fetch.append(pltpu.make_async_copy(refs[index], held_ref.at[index], in_sems.at[index]))
        for t in range(groups):
            piece = held_ref.at[index, lax.rem(row + groups - t, groups)]
            store.append(pltpu.make_async_copy(piece, out_ref.at[t * n_seq + chunk, at], out_sems.at[index]))
    for copy in fetch:
        copy.start()
    for index in range(2 * columns):
        fetch[index].wait()
        for copy in store[index * groups:(index + 1) * groups]:
            copy.start()
    for copy in store:
        copy.wait()


def place_call(kernel, place, operands, out, chunk, n_seq, tokens):
    groups, _, width = operands[0].shape
    operands = [place, *operands] + ([] if out is None else [out])
    any_spec = pl.BlockSpec(memory_space=pl.ANY)
    pieces = len(operands) - 1 - (out is not None)
    held = operands[1].shape if pieces == 1 else (pieces,) + operands[1].shape
    sems = pltpu.SemaphoreType.DMA((groups if pieces == 1 else pieces,))
    return pl.pallas_call(
        functools.partial(kernel, chunk=chunk, n_seq=n_seq),
        in_specs=[pl.BlockSpec(memory_space=pltpu.SMEM)] + [any_spec] * (len(operands) - 1),
        out_specs=any_spec,
        out_shape=jax.ShapeDtypeStruct((groups * n_seq, tokens, width), jnp.bfloat16),
        scratch_shapes=[pltpu.VMEM(held, jnp.bfloat16), sems, sems],
        input_output_aliases={} if out is None else {len(operands) - 1: 0},
        cost_estimate=pl.CostEstimate(flops=groups * tokens * width, bytes_accessed=4 * groups * tokens * width, transcendentals=0),
    )(*operands)


def grad_kernel(*refs, blocks, moving, splits):
    acc_ref = refs[-1]
    n_out = sum(len(parts) for parts in splits)
    ins, outs = refs[:-1 - n_out], list(refs[-1 - n_out:-1])
    step = pl.program_id(0)

    @pl.when(step == 0)
    def _():
        acc_ref[...] = jnp.zeros(acc_ref.shape, jnp.float32)

    for index, terms in enumerate(blocks):
        for lhs, rhs, row, column in terms:
            part = dot(ins[lhs][...], ins[rhs][...], TN)
            acc_ref[index, row:row + part.shape[0], column:column + part.shape[1]] += part

    @pl.when(step == pl.num_programs(0) - 1)
    def _():
        for index, adds in enumerate(moving):
            for ref, row in adds:
                at = slice(row, row + ins[ref].shape[0])
                acc_ref[index, at, :] += ins[ref][...].astype(jnp.float32)
        for index, parts in enumerate(splits):
            for rows, cols in parts:
                out = outs.pop(0)
                out[...] = acc_ref[index, rows, cols].astype(out.dtype)


def grad_call(blocks, shape, moving, splits, dtype, rows=512):
    ins, specs, keys = [], [], {}

    def operand(array, block, width):
        key = (id(array), block, width)
        if key not in keys:
            keys[key] = len(ins)
            ins.append(array)
            specs.append(pl.BlockSpec((rows, width), lambda s, b=block: (s, b)))
        return keys[key]

    count = blocks[0][0][0].shape[0]
    terms = [[(operand(lhs, lb, lw), operand(rhs, rb, rw), row, col) for lhs, lb, lw, rhs, rb, rw, row, col in block] for block in blocks]
    adds = []
    for block in moving:
        found = []
        for array, row in block:
            found.append((len(ins), row))
            ins.append(array)
            specs.append(pl.BlockSpec(array.shape, lambda s: (0, 0)))
        adds.append(found)
    span = lambda at, size: len(range(*at.indices(size)))
    shapes = [(span(r, shape[0]), span(c, shape[1])) for parts in splits for r, c in parts]
    return pl.pallas_call(
        functools.partial(grad_kernel, blocks=terms, moving=adds, splits=splits),
        grid=(count // rows,),
        in_specs=specs,
        out_specs=[pl.BlockSpec(one, lambda s: (0, 0)) for one in shapes],
        out_shape=[jax.ShapeDtypeStruct(one, dtype) for one in shapes],
        scratch_shapes=[pltpu.VMEM((len(blocks), *shape), jnp.float32)],
        compiler_params=pltpu.CompilerParams(dimension_semantics=("arbitrary",), vmem_limit_bytes=60 * MIB),
        cost_estimate=pl.CostEstimate(flops=2 * len(blocks) * count * shape[0] * shape[1], bytes_accessed=sum(2 * count * spec.block_shape[1] for spec in specs), transcendentals=0),
    )(*ins)


def split_width(value, out_refs):
    width = out_refs[0].shape[1]
    for index, out_ref in enumerate(out_refs):
        out_ref[...] = value[:, index * width:(index + 1) * width].astype(out_ref.dtype)


def finish_y_kernel(x_ref, mixed_ref, bias_ref, *out_refs):
    split_width(x_ref[...].astype(jnp.float32) + mixed_ref[...].astype(jnp.float32) + bias_ref[...], out_refs)


def normalize(act):
    act = act.astype(jnp.float32)
    mean = act.mean(-1, keepdims=True)
    inv_std = lax.rsqrt((act * act).mean(-1, keepdims=True) - mean * mean + LN_EPS)
    return (act - mean) * inv_std, inv_std


def finish_dx_kernel(x_ref, a6_ref, cot_ref, *out_refs):
    x_hat, inv_std = normalize(x_ref[...])
    value_a6 = a6_ref[...].astype(jnp.float32)
    mean_a6 = value_a6.mean(-1, keepdims=True)
    mean_a6x = (value_a6 * x_hat).mean(-1, keepdims=True)
    split_width(cot_ref[...].astype(jnp.float32) + inv_std * (value_a6 - mean_a6 - x_hat * mean_a6x), out_refs)


def row_call(kernel, parts, index, rows, *operands):
    width = operands[0].shape[1]
    specs = [pl.BlockSpec((min(rows, op.shape[0]), width), lambda s, i=(index if op.shape[0] > rows else 0): (i, 0)) for op in operands]
    return pl.pallas_call(
        kernel,
        grid=(1,),
        in_specs=specs,
        out_specs=[pl.BlockSpec((rows, width // parts), lambda s: (0, 0))] * parts,
        out_shape=[jax.ShapeDtypeStruct((rows, width // parts), jnp.bfloat16)] * parts,
        compiler_params=pltpu.CompilerParams(vmem_limit_bytes=16 * MIB),
        cost_estimate=pl.CostEstimate(flops=16 * rows * width, bytes_accessed=8 * rows * width, transcendentals=0),
    )(*operands)


def sublane_sum(value):
    return value.reshape(value.shape[0] // 8, 8, value.shape[1]).sum(0)


def norm_kernel(x_ref, small_ref, h_attn_ref, h_mlp_ref):
    @pl.loop(0, x_ref.shape[0] // LN_ROWS)
    def _(step):
        at = pl.ds(pl.multiple_of(step * LN_ROWS, LN_ROWS), LN_ROWS)
        x_hat, _ = normalize(x_ref[at, :])
        h_attn_ref[at, :] = (x_hat * small_ref[0:1, :] + small_ref[1:2, :]).astype(jnp.bfloat16)
        h_mlp_ref[at, :] = (x_hat * small_ref[2:3, :] + small_ref[3:4, :]).astype(jnp.bfloat16)


def offsets(refs, axis):
    starts = [0]
    for ref in refs:
        starts.append(starts[-1] + ref.shape[axis])
    return list(zip(refs, starts, starts[1:]))


def front_kernel(h_attn_ref, h_mlp_ref, cos_ref, lo_ref, hi_ref, b_qkv_ref, b_up_ref, *refs):
    w_refs, (qkv_ref, pre_ref, gelu_ref) = refs[:-3], refs[-3:]
    qkv_width = qkv_ref.shape[1]
    head = qkv_width // 3

    def project(h_ref, cols):
        return sum(dot(h_ref[:, start:stop], w_ref[:, cols], NN) for w_ref, start, stop in offsets(w_refs, 0))

    for low in range(0, qkv_width, head):
        at = slice(low, low + head)
        part = (project(h_attn_ref, at) + b_qkv_ref[:, at]).astype(jnp.bfloat16)
        if low < 2 * head:
            part = rotate(part.astype(jnp.float32), cos_ref[...], lo_ref[...], hi_ref[...], head // ROTARY_DIVISOR // 2, 1.0).astype(jnp.bfloat16)
        qkv_ref[:, at] = part
    for low in range(0, pre_ref.shape[1], TILE):
        at = slice(low, low + TILE)
        pre = (project(h_mlp_ref, slice(qkv_width + low, qkv_width + low + TILE)) + b_up_ref[:, at]).astype(jnp.bfloat16)
        pre_ref[:, at] = pre
        wide = pre.astype(jnp.float32)
        gelu_ref[:, at] = (0.5 * wide * (1.0 + lax.erf(wide * SQRT_HALF))).astype(jnp.bfloat16)


def y_kernel(ctx_ref, gelu_ref, *refs):
    w_refs, y_ref = refs[:-1], refs[-1]
    head = ctx_ref.shape[1]
    places, _, own, _ = y_ref.shape
    for w_ref, start, stop in offsets(w_refs, 1):
        acc = dot(ctx_ref[...], w_ref[:head, :], NN) + dot(gelu_ref[...], w_ref[head:, :], NN)
        y_ref[:, 0, :, start:stop] = acc.astype(jnp.bfloat16).reshape(places, own, stop - start)


def d_pre_kernel(cot_ref, pre_ref, *refs):
    w_refs, (d_ctx_ref, d_pre_ref, d_bias_ref) = refs[:-3], refs[-3:]

    def back(low, high):
        return sum(dot(cot_ref[:, start:stop], w_ref[low:high, :], NT) for w_ref, start, stop in offsets(w_refs, 1)).astype(jnp.bfloat16)

    head = d_ctx_ref.shape[1]

    @pl.when(pl.program_id(0) == 0)
    def _():
        d_bias_ref[...] = jnp.zeros(d_bias_ref.shape, jnp.float32)

    d_ctx_ref[...] = back(0, head)
    for low in range(0, d_pre_ref.shape[1], TILE):
        at = slice(low, low + TILE)
        d_gelu = back(head + low, head + low + TILE).astype(jnp.float32)
        pre = pre_ref[:, at].astype(jnp.float32)
        slope = 0.5 * (1.0 + lax.erf(pre * SQRT_HALF)) + pre * (jnp.exp(-0.5 * pre * pre) * INV_SQRT_2PI)
        d_pre = (d_gelu * slope).astype(jnp.bfloat16)
        d_pre_ref[:, at] = d_pre
        d_bias_ref[:, at] += sublane_sum(d_pre.astype(jnp.float32))


def d_h_kernel(d_qkv_ref, d_pre_ref, x_ref, small_ref, *refs):
    w_refs, (a6_ref, sums_ref) = refs[:-2], refs[-2:]
    qkv_width = d_qkv_ref.shape[1]

    @pl.when(pl.program_id(0) == 0)
    def _():
        sums_ref[...] = jnp.zeros(sums_ref.shape, jnp.float32)

    x_float = x_ref[...].astype(jnp.float32)
    mean = x_float.mean(-1, keepdims=True)
    inv_std = lax.rsqrt((x_float * x_float).mean(-1, keepdims=True) - mean * mean + LN_EPS)
    for w_ref, start, stop in offsets(w_refs, 0):
        for low in range(0, stop - start, TILE):
            part = slice(low, min(low + TILE, stop - start))
            at = slice(start + part.start, start + part.stop)
            d_attn = dot(d_qkv_ref[...], w_ref[part, :qkv_width], NT).astype(jnp.bfloat16).astype(jnp.float32)
            d_mlp = dot(d_pre_ref[...], w_ref[part, qkv_width:], NT).astype(jnp.bfloat16).astype(jnp.float32)
            a6_ref[:, at] = (d_attn * small_ref[0:1, at] + d_mlp * small_ref[2:3, at]).astype(jnp.bfloat16)
            x_hat = (x_ref[:, at].astype(jnp.float32) - mean) * inv_std
            sums_ref[0, :, at] += sublane_sum(d_attn * x_hat)
            sums_ref[1, :, at] += sublane_sum(d_attn)
            sums_ref[2, :, at] += sublane_sum(d_mlp * x_hat)
            sums_ref[3, :, at] += sublane_sum(d_mlp)


def tile_call(kernel, tiled, whole, outs, row_range, flops, rows=512):
    start, count = row_range
    rows = next(r for r in (rows, 256, 128, 64, count) if count % r == 0 and all(op.shape[0] % r == 0 for op in tiled))
    first = start // rows

    def tile_spec(op):
        blocks = op.shape[0] // rows
        if blocks * rows < count:
            return pl.BlockSpec((rows, op.shape[1]), lambda s: (lax.rem(s, blocks), 0))
        return pl.BlockSpec((rows, op.shape[1]), lambda s, f=(first if op.shape[0] != count else 0): (s + f, 0))

    in_specs = [tile_spec(op) for op in tiled]
    in_specs += [pl.BlockSpec(op.shape, lambda s, n=op.ndim: (0,) * n, pipeline_mode=pl.Buffered(1)) for op in whole]
    out_specs, out_shapes = [], []
    for form, dtype in outs:
        if isinstance(form, int):
            out_specs.append(pl.BlockSpec((rows, form), lambda s: (s, 0)))
            out_shapes.append(jax.ShapeDtypeStruct((count, form), dtype))
        elif isinstance(form[0], tuple):
            out_specs.append(pl.BlockSpec(form[1], form[2]))
            out_shapes.append(jax.ShapeDtypeStruct(form[0], dtype))
        else:
            out_specs.append(pl.BlockSpec(form, lambda s, n=len(form): (0,) * n))
            out_shapes.append(jax.ShapeDtypeStruct(form, dtype))
    moved = sum(2 * op.shape[1] * count for op in tiled) + sum(2 * op.size for op in whole) + sum(2 * shape.size for shape in out_shapes)
    return pl.pallas_call(
        kernel,
        grid=(count // rows,),
        in_specs=in_specs,
        out_specs=out_specs,
        out_shape=out_shapes,
        compiler_params=pltpu.CompilerParams(dimension_semantics=("arbitrary",), vmem_limit_bytes=60 * MIB),
        cost_estimate=pl.CostEstimate(flops=flops, bytes_accessed=moved, transcendentals=0),
    )(*tiled, *whole)


def solution(mesh):
    tx_size, ty_size = mesh.shape['tx'], mesh.shape['ty']
    act_spec = P('dp', None, 'tx')
    width_spec = P('tx')
    in_specs = (act_spec, act_spec, width_spec, width_spec, width_spec, width_spec, P('tx', 'ty', None), P('ty', None), P('ty', 'tx'), width_spec, P('tx', 'ty'), P('ty'), P('ty', 'tx'), width_spec)
    width_out = P(('dp', 'tx'))
    out_specs = (act_spec, act_spec, width_out, width_out, width_out, width_out, P(('dp', 'tx'), 'ty', None), P(('dp', 'ty'), None), P(('dp', 'ty'), 'tx'), width_out, P(('dp', 'tx'), 'ty'), P(('dp', 'ty')), P(('dp', 'ty'), 'tx'), width_out)
    antipode = tx_size // 2

    def shift(value, hops):
        return lax.ppermute(value, 'tx', [(s, (s - hops) % tx_size) for s in range(tx_size)])

    def small_sum(value, axis, size):
        step = 1
        while step < size:
            value = value + lax.ppermute(value, axis, [(s, s ^ step) for s in range(size)])
            step *= 2
        return value

    def along(value, hops):
        return lax.ppermute(value, 'ty', [(s, (s - 2 * hops) % ty_size) for s in range(ty_size)])

    def partner(value):
        return lax.ppermute(value, 'ty', [(s, s ^ 1) for s in range(ty_size)])

    def ring_gather(block, axis):
        blocks = {0: [block]}
        for hops in range(1, antipode):
            blocks[hops] = [shift(blocks[hops - 1][0], 1)]
            blocks[tx_size - hops] = [shift(blocks[(tx_size - hops + 1) % tx_size][0], -1)]
        half = block.shape[axis] // 2
        low = lax.slice_in_dim(blocks[antipode - 1][0], 0, half, axis=axis)
        high = lax.slice_in_dim(blocks[antipode + 1][0], half, 2 * half, axis=axis)
        blocks[antipode] = [shift(low, 1), shift(high, -1)]
        return [piece for r in range(tx_size) for piece in blocks[r]]

    def ring_scatter(make_blocks, shape):
        whole, half = slice(None), shape[0] // 2
        assert tx_size == 4
        low, high = grad_call([make_blocks(2)], shape, [[]], [[(slice(0, half), whole), (slice(half, None), whole)]], jnp.bfloat16)
        low, high = shift(low, -1), shift(high, 1)
        up, down = grad_call([make_blocks(1), make_blocks(3)], shape, [[(low, 0)], [(high, half)]], [[(whole, whole)], [(whole, whole)]], jnp.bfloat16)
        return [(shift(up, -1), 0), (shift(down, 1), 0)]

    def body(x_act, cot_out, ln1_gain, ln1_bias, ln2_gain, ln2_bias, w_qkv, b_qkv, w_dense, b_dense, w_up, b_up, w_down, b_down):
        batch, seq_len, d_local = x_act.shape
        n_seq = batch // tx_size
        own = seq_len // ty_size
        row, col = lax.axis_index('tx'), lax.axis_index('ty')
        qkv_width = w_qkv.shape[1] * w_qkv.shape[2]
        head = qkv_width // 3
        chunks = range(n_seq)
        tables = rotary_tables(seq_len, head // ROTARY_DIVISOR)
        attn_fwd, attn_bwd = attention_calls(n_seq, seq_len, head, tables)

        def to_tokens(act):
            parts = act.reshape(tx_size, n_seq, ty_size, own, d_local)
            pick = lambda index: lax.dynamic_slice(parts, (index, 0, col, 0, 0), (1, n_seq, 1, own, d_local)).reshape(n_seq, own, d_local)
            blocks = [pick(row)] + [shift(pick((row - r) % tx_size), r) for r in range(1, tx_size)]
            return jnp.concatenate(blocks, axis=2)

        place = jnp.stack([row, col // 2, col % 2])

        def to_width(parts):
            return jnp.stack([parts[0]] + [shift(parts[r], -r) for r in range(1, tx_size)])

        line = lax.broadcasted_iota(jnp.int32, (8, d_local), 0)
        small = jnp.zeros((8, d_local), jnp.bfloat16)
        for index, vector in enumerate((ln1_gain, ln1_bias, ln2_gain, ln2_bias, b_dense, b_down)):
            small = jnp.where(line == index, vector[None, :], small)
        small = [small] + [shift(small, r) for r in range(1, tx_size)]
        small = jnp.concatenate(small, axis=1).astype(jnp.float32)
        bias_out = small[4] + small[5]
        x_own = to_tokens(x_act)
        cot_own = to_tokens(cot_out)
        x_group = lax.all_gather(x_own, 'ty', axis=1, tiled=True)
        cot_group = lax.all_gather(cot_own, 'ty', axis=1, tiled=True)
        x_group, cot_group = x_group.reshape(n_seq * seq_len, -1), cot_group.reshape(n_seq * seq_len, -1)
        w_in = jnp.concatenate([w_qkv.reshape(d_local, qkv_width), w_up], axis=1)
        w_in = ring_gather(w_in, 0)
        w_back = jnp.concatenate([w_dense, w_down], axis=0)
        w_back = ring_gather(w_back, 1)
        in_size, back_size = sum(w.size for w in w_in), sum(w.size for w in w_back)

        n_tok, d_model = x_group.shape
        x_rows, cot_rows = x_own.reshape(-1, d_model), cot_own.reshape(-1, d_model)
        ff_width = w_up.shape[1]
        h_attn, h_mlp = tile_call(norm_kernel, [x_group], [small], [(d_model, jnp.bfloat16), (d_model, jnp.bfloat16)], (0, n_tok), 16 * x_group.size)
        qkv_act, pre_act, gelu_out = tile_call(
            front_kernel, [h_attn, h_mlp, *tables], [b_qkv.reshape(1, -1).astype(jnp.float32), b_up.reshape(1, -1).astype(jnp.float32), *w_in],
            [(qkv_width, jnp.bfloat16), (ff_width, jnp.bfloat16), (ff_width, jnp.bfloat16)], (0, n_tok), 2 * n_tok * in_size)
        qkv_seq = qkv_act.reshape(n_seq, seq_len, qkv_width)
        context = attn_fwd(qkv_seq).reshape(n_tok, head)
        blocks_per_seq = ty_size // 4
        y_form = ((ty_size, n_seq, own, d_model), (4, 1, own, d_model), lambda s: (lax.rem(s, blocks_per_seq), s // blocks_per_seq, 0, 0))
        (y_part,) = tile_call(y_kernel, [context, gelu_out], w_back, [(y_form, jnp.bfloat16)], (0, n_tok), 2 * n_tok * back_size, 4 * own)
        mixed = lax.psum_scatter(y_part.reshape(n_tok, d_model), 'ty', scatter_dimension=0, tiled=True)
        blocks = to_width(row_call(finish_y_kernel, tx_size, 0, n_seq * own, x_rows, mixed, bias_out.reshape(1, -1)))
        full = lax.all_gather(blocks.reshape(tx_size * n_seq, own, d_local), 'ty', axis=1, tiled=True)
        y_out = place_call(place_kernel, place, [full.reshape(tx_size, n_seq * seq_len, d_local)], None, 0, 1, n_seq * seq_len)

        d_ctx, d_pre, d_b_up = tile_call(
            d_pre_kernel, [cot_group, pre_act], w_back,
            [(head, jnp.bfloat16), (ff_width, jnp.bfloat16), ((8, ff_width), jnp.float32)], (0, n_tok), 2 * n_tok * back_size)
        d_ctx, d_b_up = d_ctx.reshape(n_seq, seq_len, head), d_b_up.sum(0)
        d_b_qkv, d_ln, dx_act = [], [], None
        for s in chunks:
            d_qkv, d_b_seq = attn_bwd(qkv_seq, d_ctx, s, (d_qkv, sums) if s else ())
            d_b_qkv.append(d_b_seq.sum((0, 1)))
            a6_part, sums = tile_call(
                d_h_kernel, [d_qkv.reshape(n_tok, qkv_width), d_pre, x_group], [small, *w_in],
                [(d_model, jnp.bfloat16), ((4, 8, d_model), jnp.float32)], (s * seq_len, seq_len), 2 * seq_len * in_size)
            d_ln.append(sums)
            value_a6 = lax.psum_scatter(a6_part, 'ty', scatter_dimension=0, tiled=True)
            parts = row_call(finish_dx_kernel, tx_size, s, own, x_rows, value_a6, cot_rows)
            block = to_width(parts)
            if s < n_seq - 1:
                assert ty_size == 8
                half = block.shape[0] // 2
                ahead, behind = along(block, 1), along(block, -1)
                far = jnp.concatenate([along(ahead[:half], 1), along(behind[half:], -1)], axis=0)
                blocks = [block, ahead, far, behind]
                blocks = blocks + [partner(piece) for piece in blocks]
                dx_act = place_call(place_pieces_kernel, place, blocks, dx_act, s, n_seq, seq_len)
            else:
                full = lax.all_gather(block, 'ty', axis=1, tiled=True)
                dx_act = place_call(place_kernel, place, [full], dx_act, s, n_seq, seq_len)
        d_qkv = d_qkv.reshape(n_tok, qkv_width)

        d_ln = sum(d_ln).sum(1).reshape(4, tx_size, d_local)
        d_bias = jnp.concatenate([sum(d_b_qkv), d_b_up]).reshape(4, -1)
        sent = [jnp.concatenate([d_ln[:, r], d_bias], axis=1) for r in range(tx_size)]
        got = [sent[0]] + [shift(sent[r], -r) for r in range(1, tx_size)]
        got = sum(got[r] + got[r + antipode] for r in range(antipode))
        d_bias = got[:, d_local:].reshape(-1)
        d_ln = small_sum(got[:, :d_local], 'ty', ty_size)
        d_b_out = cot_out.astype(jnp.float32).sum((0, 1))

        in_shape, back_shape = (d_local, qkv_width + ff_width), (head + ff_width, d_local)
        in_blocks = lambda r: [(h_attn, r, d_local, d_qkv, 0, qkv_width, 0, 0), (h_mlp, r, d_local, d_pre, 0, ff_width, 0, qkv_width)]
        back_blocks = lambda r: [(context, 0, head, cot_group, r, d_local, 0, 0), (gelu_out, 0, ff_width, cot_group, r, d_local, head, 0)]
        add_back = ring_scatter(back_blocks, back_shape)
        add_in = ring_scatter(in_blocks, in_shape)
        whole = slice(None)
        d_w_dense, d_w_down = grad_call([back_blocks(0)], back_shape, [add_back], [[(slice(0, head), whole), (slice(head, None), whole)]], jnp.float32)
        d_w_qkv, d_w_up = grad_call([in_blocks(0)], in_shape, [add_in], [[(whole, slice(0, qkv_width)), (whole, slice(qkv_width, None))]], jnp.float32)
        y_out = y_out.reshape(batch, seq_len, d_local)
        return (y_out, dx_act, d_ln[0], d_ln[1], d_ln[2], d_ln[3], d_w_qkv.reshape(w_qkv.shape), d_bias[:qkv_width].reshape(b_qkv.shape), d_w_dense, d_b_out, d_w_up, d_bias[qkv_width:], d_w_down, d_b_out)

    return jax.shard_map(body, mesh=mesh, in_specs=in_specs, out_specs=out_specs, check_vma=False)
```

```python
import functools
import jax
import jax.numpy as jnp
from jax import lax
from jax.experimental import pallas as pl
from jax.experimental.pallas import tpu as pltpu
from jax.sharding import PartitionSpec as P


LN_EPS = 1e-5
ROPE_BASE = 10000.0
ROTARY_DIVISOR = 4
LANES = 128
Q_ROWS = 256
LN_ROWS = 128
MIB = 1024 * 1024
TILE = 256
SQRT_HALF = 0.5 ** 0.5
INV_SQRT_2PI = 0.3989422804014327

NT = (((1,), (1,)), ((), ()))
TN = (((0,), (0,)), ((), ()))
NN = (((1,), (0,)), ((), ()))


def dot(a, b, dims):
    return lax.dot_general(a, b, dims, preferred_element_type=jnp.float32)


def rotary_tables(seq_len, rot_dim):
    half = rot_dim // 2
    lane = jnp.arange(LANES)
    freq_index = jnp.where(lane < half, lane, lane - half)
    inv_freq = ROPE_BASE ** (-(2 * freq_index).astype(jnp.float32) / rot_dim)
    angles = jnp.arange(seq_len, dtype=jnp.float32)[:, None] * inv_freq[None, :]
    inside = (lane < rot_dim)[None, :]
    cos_tab = jnp.where(inside, jnp.cos(angles), 1.0)
    sin = jnp.where(inside, jnp.sin(angles), 0.0)
    first = (lane < half)[None, :]
    return cos_tab, jnp.where(first, -sin, 0.0), jnp.where(first, 0.0, sin)


def rotate(part, cos_tab, sin_lo, sin_hi, half, sign):
    head = part[:, :LANES]
    forward = pltpu.roll(head, half, 1)
    backward = pltpu.roll(head, LANES - half, 1)
    mixed = head * cos_tab + sign * (backward * sin_lo + forward * sin_hi)
    return jnp.concatenate([mixed, part[:, LANES:]], axis=1)


def causal_probs(q_rows, keys, row_start, scale):
    scores = dot(q_rows, keys, NT) * scale
    rows = row_start + lax.broadcasted_iota(jnp.int32, scores.shape, 0)
    cols = lax.broadcasted_iota(jnp.int32, scores.shape, 1)
    scores = jnp.where(rows >= cols, scores, -1e30)
    exps = jnp.exp(scores - jnp.max(scores, axis=1, keepdims=True))
    return exps * (1.0 / jnp.sum(exps, axis=1, keepdims=True))


def attn_fwd_kernel(qkv_ref, ctx_ref, *, scale, span):
    seq_len, width = ctx_ref.shape[1:]
    for end in range(span, seq_len + 1, span):
        for start in range(end - span, end, Q_ROWS):
            rows = slice(start, start + Q_ROWS)
            probs = causal_probs(qkv_ref[0, rows, :width], qkv_ref[0, :end, width:2 * width], start, scale).astype(jnp.bfloat16)
            ctx_ref[0, rows, :] = dot(probs, qkv_ref[0, :end, 2 * width:], NN).astype(jnp.bfloat16)


def attn_bwd_kernel(qkv_ref, dctx_ref, cos_ref, lo_ref, hi_ref, dqkv_ref, db_ref, dk_ref, dv_ref, *, half, scale, span):
    seq_len, width = dctx_ref.shape[1:]
    dk_ref[...] = jnp.zeros(dk_ref.shape, jnp.float32)
    dv_ref[...] = jnp.zeros(dv_ref.shape, jnp.float32)
    db_ref[...] = jnp.zeros(db_ref.shape, jnp.float32)

    def store(rows, col, grad_rot, turn):
        grad = grad_rot.astype(jnp.bfloat16)
        if turn:
            wide = grad.astype(jnp.float32)
            grad = rotate(wide, cos_ref[rows, :], lo_ref[rows, :], hi_ref[rows, :], half, -1.0).astype(jnp.bfloat16)
        dqkv_ref[0, rows, col:col + width] = grad
        db_ref[0, :, col:col + width] += sublane_sum(grad.astype(jnp.float32))

    for end in range(span, seq_len + 1, span):
        for start in range(end - span, end, Q_ROWS):
            rows = slice(start, start + Q_ROWS)
            q_rows, keys = qkv_ref[0, rows, :width], qkv_ref[0, :end, width:2 * width]
            dctx = dctx_ref[0, rows, :]
            probs = causal_probs(q_rows, keys, start, scale)
            dprobs = dot(dctx, qkv_ref[0, :end, 2 * width:], NT).astype(jnp.bfloat16).astype(jnp.float32)
            dv_ref[:end, :] += dot(probs.astype(jnp.bfloat16), dctx, TN)
            inner = jnp.sum(probs * dprobs, axis=1, keepdims=True)
            dscores = (probs * (dprobs - inner) * scale).astype(jnp.bfloat16)
            dk_ref[:end, :] += dot(dscores, q_rows, TN)
            store(rows, 0, dot(dscores, keys, NN), True)

    @pl.loop(0, seq_len // Q_ROWS)
    def _(step):
        rows = pl.ds(pl.multiple_of(step * Q_ROWS, Q_ROWS), Q_ROWS)
        store(rows, width, dk_ref[rows, :], True)
        store(rows, 2 * width, dv_ref[rows, :], False)


def attention_calls(n_seq, seq_len, width, tables):
    half = width // ROTARY_DIVISOR // 2
    scale = width ** -0.5
    span = 512 if seq_len % 512 == 0 else seq_len
    seq_spec = lambda cols, first=0: pl.BlockSpec((1, seq_len, cols), lambda s: (s + first, 0, 0))
    tab_spec = pl.BlockSpec((seq_len, LANES), lambda s: (0, 0))
    acc_scratch = pltpu.VMEM((seq_len, width), jnp.float32)
    pairs = seq_len * seq_len // 2
    params = pltpu.CompilerParams(dimension_semantics=("arbitrary",), vmem_limit_bytes=60 * MIB)

    def forward(qkv):
        return pl.pallas_call(
            functools.partial(attn_fwd_kernel, scale=scale, span=span),
            grid=(n_seq,),
            in_specs=[seq_spec(3 * width)],
            out_specs=seq_spec(width),
            out_shape=jax.ShapeDtypeStruct((n_seq, seq_len, width), jnp.bfloat16),
            compiler_params=params,
            name="af",
            cost_estimate=pl.CostEstimate(flops=8 * n_seq * pairs * width, bytes_accessed=8 * n_seq * seq_len * width, transcendentals=n_seq * pairs),
        )(qkv)

    def backward(qkv, dctx, index, into):
        kernel = functools.partial(attn_bwd_kernel, half=half, scale=scale, span=span)
        return pl.pallas_call(
            (lambda *refs: kernel(*refs[:5], *refs[5 + len(into):])),
            grid=(1,),
            in_specs=[seq_spec(3 * width, index), seq_spec(width, index), tab_spec, tab_spec, tab_spec] + [pl.BlockSpec(memory_space=pl.ANY)] * len(into),
            out_specs=[seq_spec(3 * width, index), pl.BlockSpec((1, 8, 3 * width), lambda s: (s, 0, 0))],
            input_output_aliases={5: 0} if into else {},
            out_shape=[jax.ShapeDtypeStruct((n_seq, seq_len, 3 * width), jnp.bfloat16), jax.ShapeDtypeStruct((1, 8, 3 * width), jnp.float32)],
            scratch_shapes=[acc_scratch, acc_scratch],
            compiler_params=params,
            name="ab",
            cost_estimate=pl.CostEstimate(flops=20 * pairs * width, bytes_accessed=14 * seq_len * width, transcendentals=pairs),
        )(qkv, dctx, *tables, *into)

    return forward, backward


def place_kernel(place_ref, full_ref, *rest, chunk, n_seq):
    out_ref, held_ref, in_sems, out_sems = rest[-4:]
    groups = full_ref.shape[0]
    fetch = [pltpu.make_async_copy(full_ref.at[lax.rem(place_ref[0] + groups - t, groups)], held_ref.at[t], in_sems.at[t]) for t in range(groups)]
    store = [pltpu.make_async_copy(held_ref.at[t], out_ref.at[t * n_seq + chunk], out_sems.at[t]) for t in range(groups)]
    for copy in fetch:
        copy.start()
    for t in range(groups):
        fetch[t].wait()
        store[t].start()
    for copy in store:
        copy.wait()


def place_pieces_kernel(place_ref, *refs, chunk, n_seq):
    out_ref, held_ref, in_sems, out_sems = refs[-4:]
    groups, own, _ = refs[0].shape
    columns = held_ref.shape[0] // 2
    row, column, core = place_ref[0], place_ref[1], place_ref[2]
    fetch, store = [], []
    for index in range(2 * columns):
        source = 2 * lax.rem(column + index % columns, columns) + (core if index < columns else 1 - core)
        at = pl.ds(pl.multiple_of(source * own, own), own)
        fetch.append(pltpu.make_async_copy(refs[index], held_ref.at[index], in_sems.at[index]))
        for t in range(groups):
            piece = held_ref.at[index, lax.rem(row + groups - t, groups)]
            store.append(pltpu.make_async_copy(piece, out_ref.at[t * n_seq + chunk, at], out_sems.at[index]))
    for copy in fetch:
        copy.start()
    for index in range(2 * columns):
        fetch[index].wait()
        for copy in store[index * groups:(index + 1) * groups]:
            copy.start()
    for copy in store:
        copy.wait()


def place_call(kernel, place, operands, out, chunk, n_seq, tokens):
    groups, _, width = operands[0].shape
    operands = [place, *operands] + ([] if out is None else [out])
    any_spec = pl.BlockSpec(memory_space=pl.ANY)
    pieces = len(operands) - 1 - (out is not None)
    held = operands[1].shape if pieces == 1 else (pieces,) + operands[1].shape
    sems = pltpu.SemaphoreType.DMA((groups if pieces == 1 else pieces,))
    return pl.pallas_call(
        functools.partial(kernel, chunk=chunk, n_seq=n_seq),
        in_specs=[pl.BlockSpec(memory_space=pltpu.SMEM)] + [any_spec] * (len(operands) - 1),
        out_specs=any_spec,
        out_shape=jax.ShapeDtypeStruct((groups * n_seq, tokens, width), jnp.bfloat16),
        scratch_shapes=[pltpu.VMEM(held, jnp.bfloat16), sems, sems],
        input_output_aliases={} if out is None else {len(operands) - 1: 0},
        cost_estimate=pl.CostEstimate(flops=groups * tokens * width, bytes_accessed=4 * groups * tokens * width, transcendentals=0),
    )(*operands)


def grad_kernel(*refs, blocks, moving, splits):
    acc_ref = refs[-1]
    n_out = sum(len(parts) for parts in splits)
    ins, outs = refs[:-1 - n_out], list(refs[-1 - n_out:-1])
    step = pl.program_id(0)

    @pl.when(step == 0)
    def _():
        acc_ref[...] = jnp.zeros(acc_ref.shape, jnp.float32)

    for index, terms in enumerate(blocks):
        for lhs, rhs, row, column in terms:
            part = dot(ins[lhs][...], ins[rhs][...], TN)
            acc_ref[index, row:row + part.shape[0], column:column + part.shape[1]] += part

    @pl.when(step == pl.num_programs(0) - 1)
    def _():
        for index, adds in enumerate(moving):
            for ref, row in adds:
                at = slice(row, row + ins[ref].shape[0])
                acc_ref[index, at, :] += ins[ref][...].astype(jnp.float32)
        for index, parts in enumerate(splits):
            for rows, cols in parts:
                out = outs.pop(0)
                out[...] = acc_ref[index, rows, cols].astype(out.dtype)


def grad_call(blocks, shape, moving, splits, dtype, rows=512):
    ins, specs, keys = [], [], {}

    def operand(array, block, width):
        key = (id(array), block, width)
        if key not in keys:
            keys[key] = len(ins)
            ins.append(array)
            specs.append(pl.BlockSpec((rows, width), lambda s, b=block: (s, b)))
        return keys[key]

    count = blocks[0][0][0].shape[0]
    terms = [[(operand(lhs, lb, lw), operand(rhs, rb, rw), row, col) for lhs, lb, lw, rhs, rb, rw, row, col in block] for block in blocks]
    adds = []
    for block in moving:
        found = []
        for array, row in block:
            found.append((len(ins), row))
            ins.append(array)
            specs.append(pl.BlockSpec(array.shape, lambda s: (0, 0)))
        adds.append(found)
    span = lambda at, size: len(range(*at.indices(size)))
    shapes = [(span(r, shape[0]), span(c, shape[1])) for parts in splits for r, c in parts]
    return pl.pallas_call(
        functools.partial(grad_kernel, blocks=terms, moving=adds, splits=splits),
        grid=(count // rows,),
        in_specs=specs,
        out_specs=[pl.BlockSpec(one, lambda s: (0, 0)) for one in shapes],
        out_shape=[jax.ShapeDtypeStruct(one, dtype) for one in shapes],
        scratch_shapes=[pltpu.VMEM((len(blocks), *shape), jnp.float32)],
        compiler_params=pltpu.CompilerParams(dimension_semantics=("arbitrary",), vmem_limit_bytes=60 * MIB),
        cost_estimate=pl.CostEstimate(flops=2 * len(blocks) * count * shape[0] * shape[1], bytes_accessed=sum(2 * count * spec.block_shape[1] for spec in specs), transcendentals=0),
    )(*ins)


def join_kernel(low_ref, high_ref, out_ref):
    half = low_ref.shape[0]
    out_ref[:half] = low_ref[...]
    out_ref[half:] = high_ref[...]


def split_width(value, out_refs):
    width = out_refs[0].shape[1]
    for index, out_ref in enumerate(out_refs):
        out_ref[...] = value[:, index * width:(index + 1) * width].astype(out_ref.dtype)


def finish_y_kernel(x_ref, mixed_ref, bias_ref, *out_refs):
    split_width(x_ref[...].astype(jnp.float32) + mixed_ref[...].astype(jnp.float32) + bias_ref[...], out_refs)


def normalize(act):
    act = act.astype(jnp.float32)
    mean = act.mean(-1, keepdims=True)
    inv_std = lax.rsqrt((act * act).mean(-1, keepdims=True) - mean * mean + LN_EPS)
    return (act - mean) * inv_std, inv_std


def finish_dx_kernel(x_ref, a6_ref, cot_ref, *out_refs):
    x_hat, inv_std = normalize(x_ref[...])
    value_a6 = a6_ref[...].astype(jnp.float32)
    mean_a6 = value_a6.mean(-1, keepdims=True)
    mean_a6x = (value_a6 * x_hat).mean(-1, keepdims=True)
    split_width(cot_ref[...].astype(jnp.float32) + inv_std * (value_a6 - mean_a6 - x_hat * mean_a6x), out_refs)


def row_call(kernel, parts, index, rows, *operands):
    width = operands[0].shape[1]
    specs = [pl.BlockSpec((min(rows, op.shape[0]), width), lambda s, i=(index if op.shape[0] > rows else 0): (i, 0)) for op in operands]
    return pl.pallas_call(
        kernel,
        grid=(1,),
        in_specs=specs,
        out_specs=[pl.BlockSpec((rows, width // parts), lambda s: (0, 0))] * parts,
        out_shape=[jax.ShapeDtypeStruct((rows, width // parts), jnp.bfloat16)] * parts,
        compiler_params=pltpu.CompilerParams(vmem_limit_bytes=16 * MIB),
        cost_estimate=pl.CostEstimate(flops=16 * rows * width, bytes_accessed=8 * rows * width, transcendentals=0),
    )(*operands)


def sublane_sum(value):
    return value.reshape(value.shape[0] // 8, 8, value.shape[1]).sum(0)


def norm_kernel(x_ref, small_ref, h_attn_ref, h_mlp_ref):
    @pl.loop(0, x_ref.shape[0] // LN_ROWS)
    def _(step):
        at = pl.ds(pl.multiple_of(step * LN_ROWS, LN_ROWS), LN_ROWS)
        x_hat, _ = normalize(x_ref[at, :])
        h_attn_ref[at, :] = (x_hat * small_ref[0:1, :] + small_ref[1:2, :]).astype(jnp.bfloat16)
        h_mlp_ref[at, :] = (x_hat * small_ref[2:3, :] + small_ref[3:4, :]).astype(jnp.bfloat16)


def offsets(refs, axis):
    starts = [0]
    for ref in refs:
        starts.append(starts[-1] + ref.shape[axis])
    return list(zip(refs, starts, starts[1:]))


def front_kernel(h_attn_ref, h_mlp_ref, cos_ref, lo_ref, hi_ref, b_qkv_ref, b_up_ref, *refs):
    w_refs, (qkv_ref, pre_ref, gelu_ref) = refs[:-3], refs[-3:]
    qkv_width = qkv_ref.shape[1]
    head = qkv_width // 3

    def project(h_ref, cols):
        return sum(dot(h_ref[:, start:stop], w_ref[:, cols], NN) for w_ref, start, stop in offsets(w_refs, 0))

    for low in range(0, qkv_width, head):
        at = slice(low, low + head)
        part = (project(h_attn_ref, at) + b_qkv_ref[:, at]).astype(jnp.bfloat16)
        if low < 2 * head:
            part = rotate(part.astype(jnp.float32), cos_ref[...], lo_ref[...], hi_ref[...], head // ROTARY_DIVISOR // 2, 1.0).astype(jnp.bfloat16)
        qkv_ref[:, at] = part
    for low in range(0, pre_ref.shape[1], TILE):
        at = slice(low, low + TILE)
        pre = (project(h_mlp_ref, slice(qkv_width + low, qkv_width + low + TILE)) + b_up_ref[:, at]).astype(jnp.bfloat16)
        pre_ref[:, at] = pre
        wide = pre.astype(jnp.float32)
        gelu_ref[:, at] = (0.5 * wide * (1.0 + lax.erf(wide * SQRT_HALF))).astype(jnp.bfloat16)


def y_kernel(ctx_ref, gelu_ref, *refs):
    w_refs, y_ref = refs[:-1], refs[-1]
    head = ctx_ref.shape[1]
    places, _, own, _ = y_ref.shape
    for w_ref, start, stop in offsets(w_refs, 1):
        acc = dot(ctx_ref[...], w_ref[:head, :], NN) + dot(gelu_ref[...], w_ref[head:, :], NN)
        y_ref[:, 0, :, start:stop] = acc.astype(jnp.bfloat16).reshape(places, own, stop - start)


def d_pre_kernel(cot_ref, pre_ref, *refs):
    w_refs, (d_ctx_ref, d_pre_ref, d_bias_ref) = refs[:-3], refs[-3:]

    def back(low, high):
        return sum(dot(cot_ref[:, start:stop], w_ref[low:high, :], NT) for w_ref, start, stop in offsets(w_refs, 1)).astype(jnp.bfloat16)

    head = d_ctx_ref.shape[1]

    @pl.when(pl.program_id(0) == 0)
    def _():
        d_bias_ref[...] = jnp.zeros(d_bias_ref.shape, jnp.float32)

    d_ctx_ref[...] = back(0, head)
    for low in range(0, d_pre_ref.shape[1], TILE):
        at = slice(low, low + TILE)
        d_gelu = back(head + low, head + low + TILE).astype(jnp.float32)
        pre = pre_ref[:, at].astype(jnp.float32)
        slope = 0.5 * (1.0 + lax.erf(pre * SQRT_HALF)) + pre * (jnp.exp(-0.5 * pre * pre) * INV_SQRT_2PI)
        d_pre = (d_gelu * slope).astype(jnp.bfloat16)
        d_pre_ref[:, at] = d_pre
        d_bias_ref[:, at] += sublane_sum(d_pre.astype(jnp.float32))


def d_h_kernel(d_qkv_ref, d_pre_ref, x_ref, small_ref, *refs):
    w_refs, (a6_ref, sums_ref) = refs[:-2], refs[-2:]
    qkv_width = d_qkv_ref.shape[1]

    @pl.when(pl.program_id(0) == 0)
    def _():
        sums_ref[...] = jnp.zeros(sums_ref.shape, jnp.float32)

    x_float = x_ref[...].astype(jnp.float32)
    mean = x_float.mean(-1, keepdims=True)
    inv_std = lax.rsqrt((x_float * x_float).mean(-1, keepdims=True) - mean * mean + LN_EPS)
    for w_ref, start, stop in offsets(w_refs, 0):
        for low in range(0, stop - start, TILE):
            part = slice(low, min(low + TILE, stop - start))
            at = slice(start + part.start, start + part.stop)
            d_attn = dot(d_qkv_ref[...], w_ref[part, :qkv_width], NT).astype(jnp.bfloat16).astype(jnp.float32)
            d_mlp = dot(d_pre_ref[...], w_ref[part, qkv_width:], NT).astype(jnp.bfloat16).astype(jnp.float32)
            a6_ref[:, at] = (d_attn * small_ref[0:1, at] + d_mlp * small_ref[2:3, at]).astype(jnp.bfloat16)
            x_hat = (x_ref[:, at].astype(jnp.float32) - mean) * inv_std
            sums_ref[0, :, at] += sublane_sum(d_attn * x_hat)
            sums_ref[1, :, at] += sublane_sum(d_attn)
            sums_ref[2, :, at] += sublane_sum(d_mlp * x_hat)
            sums_ref[3, :, at] += sublane_sum(d_mlp)


def tile_call(kernel, tiled, whole, outs, row_range, flops, rows=512):
    start, count = row_range
    rows = next(r for r in (rows, 256, 128, 64, count) if count % r == 0 and all(op.shape[0] % r == 0 for op in tiled))
    first = start // rows

    def tile_spec(op):
        blocks = op.shape[0] // rows
        if blocks * rows < count:
            return pl.BlockSpec((rows, op.shape[1]), lambda s: (lax.rem(s, blocks), 0))
        return pl.BlockSpec((rows, op.shape[1]), lambda s, f=(first if op.shape[0] != count else 0): (s + f, 0))

    in_specs = [tile_spec(op) for op in tiled]
    in_specs += [pl.BlockSpec(op.shape, lambda s, n=op.ndim: (0,) * n, pipeline_mode=pl.Buffered(1)) for op in whole]
    out_specs, out_shapes = [], []
    for form, dtype in outs:
        if isinstance(form, int):
            out_specs.append(pl.BlockSpec((rows, form), lambda s: (s, 0)))
            out_shapes.append(jax.ShapeDtypeStruct((count, form), dtype))
        elif isinstance(form[0], tuple):
            out_specs.append(pl.BlockSpec(form[1], form[2]))
            out_shapes.append(jax.ShapeDtypeStruct(form[0], dtype))
        else:
            out_specs.append(pl.BlockSpec(form, lambda s, n=len(form): (0,) * n))
            out_shapes.append(jax.ShapeDtypeStruct(form, dtype))
    moved = sum(2 * op.shape[1] * count for op in tiled) + sum(2 * op.size for op in whole) + sum(2 * shape.size for shape in out_shapes)
    return pl.pallas_call(
        kernel,
        grid=(count // rows,),
        in_specs=in_specs,
        out_specs=out_specs,
        out_shape=out_shapes,
        compiler_params=pltpu.CompilerParams(dimension_semantics=("arbitrary",), vmem_limit_bytes=60 * MIB),
        cost_estimate=pl.CostEstimate(flops=flops, bytes_accessed=moved, transcendentals=0),
    )(*tiled, *whole)


def solution(mesh):
    tx_size, ty_size = mesh.shape['tx'], mesh.shape['ty']
    act_spec = P('dp', None, 'tx')
    width_spec = P('tx')
    in_specs = (act_spec, act_spec, width_spec, width_spec, width_spec, width_spec, P('tx', 'ty', None), P('ty', None), P('ty', 'tx'), width_spec, P('tx', 'ty'), P('ty'), P('ty', 'tx'), width_spec)
    width_out = P(('dp', 'tx'))
    out_specs = (act_spec, act_spec, width_out, width_out, width_out, width_out, P(('dp', 'tx'), 'ty', None), P(('dp', 'ty'), None), P(('dp', 'ty'), 'tx'), width_out, P(('dp', 'tx'), 'ty'), P(('dp', 'ty')), P(('dp', 'ty'), 'tx'), width_out)
    antipode = tx_size // 2

    def shift(value, hops):
        return lax.ppermute(value, 'tx', [(s, (s - hops) % tx_size) for s in range(tx_size)])

    def small_sum(value, axis, size):
        step = 1
        while step < size:
            value = value + lax.ppermute(value, axis, [(s, s ^ step) for s in range(size)])
            step *= 2
        return value

    def along(value, hops):
        return lax.ppermute(value, 'ty', [(s, (s - 2 * hops) % ty_size) for s in range(ty_size)])

    def partner(value):
        return lax.ppermute(value, 'ty', [(s, s ^ 1) for s in range(ty_size)])

    def ring_gather(block, axis):
        blocks = {0: [block]}
        for hops in range(1, antipode):
            blocks[hops] = [shift(blocks[hops - 1][0], 1)]
            blocks[tx_size - hops] = [shift(blocks[(tx_size - hops + 1) % tx_size][0], -1)]
        half = block.shape[axis] // 2
        low = lax.slice_in_dim(blocks[antipode - 1][0], 0, half, axis=axis)
        high = lax.slice_in_dim(blocks[antipode + 1][0], half, 2 * half, axis=axis)
        blocks[antipode] = [shift(low, 1), shift(high, -1)]
        return [piece for r in range(tx_size) for piece in blocks[r]]

    def ring_scatter(make_blocks, shape):
        whole, half = slice(None), shape[0] // 2
        assert tx_size == 4
        low, high = grad_call([make_blocks(2)], shape, [[]], [[(slice(0, half), whole), (slice(half, None), whole)]], jnp.bfloat16)
        low, high = shift(low, -1), shift(high, 1)
        up, down = grad_call([make_blocks(1), make_blocks(3)], shape, [[(low, 0)], [(high, half)]], [[(whole, whole)], [(whole, whole)]], jnp.bfloat16)
        return [(shift(up, -1), 0), (shift(down, 1), 0)]

    def body(x_act, cot_out, ln1_gain, ln1_bias, ln2_gain, ln2_bias, w_qkv, b_qkv, w_dense, b_dense, w_up, b_up, w_down, b_down):
        batch, seq_len, d_local = x_act.shape
        n_seq = batch // tx_size
        own = seq_len // ty_size
        row, col = lax.axis_index('tx'), lax.axis_index('ty')
        qkv_width = w_qkv.shape[1] * w_qkv.shape[2]
        head = qkv_width // 3
        chunks = range(n_seq)
        tables = rotary_tables(seq_len, head // ROTARY_DIVISOR)
        attn_fwd, attn_bwd = attention_calls(n_seq, seq_len, head, tables)

        def to_tokens(act):
            parts = act.reshape(tx_size, n_seq, ty_size, own, d_local)
            pick = lambda index: lax.dynamic_slice(parts, (index, 0, col, 0, 0), (1, n_seq, 1, own, d_local)).reshape(n_seq, own, d_local)
            blocks = [pick(row)] + [shift(pick((row - r) % tx_size), r) for r in range(1, tx_size)]
            return jnp.concatenate(blocks, axis=2)

        place = jnp.stack([row, col // 2, col % 2])

        def to_width(parts):
            return jnp.stack([parts[0]] + [shift(parts[r], -r) for r in range(1, tx_size)])

        line = lax.broadcasted_iota(jnp.int32, (8, d_local), 0)
        small = jnp.zeros((8, d_local), jnp.bfloat16)
        for index, vector in enumerate((ln1_gain, ln1_bias, ln2_gain, ln2_bias, b_dense, b_down)):
            small = jnp.where(line == index, vector[None, :], small)
        small = [small] + [shift(small, r) for r in range(1, tx_size)]
        small = jnp.concatenate(small, axis=1).astype(jnp.float32)
        bias_out = small[4] + small[5]
        x_own = to_tokens(x_act)
        cot_own = to_tokens(cot_out)
        x_group = lax.all_gather(x_own, 'ty', axis=1, tiled=True)
        cot_group = lax.all_gather(cot_own, 'ty', axis=1, tiled=True)
        x_group, cot_group = x_group.reshape(n_seq * seq_len, -1), cot_group.reshape(n_seq * seq_len, -1)
        w_in = jnp.concatenate([w_qkv.reshape(d_local, qkv_width), w_up], axis=1)
        w_in = ring_gather(w_in, 0)
        w_back = jnp.concatenate([w_dense, w_down], axis=0)
        w_back = ring_gather(w_back, 1)
        in_size, back_size = sum(w.size for w in w_in), sum(w.size for w in w_back)

        n_tok, d_model = x_group.shape
        x_rows, cot_rows = x_own.reshape(-1, d_model), cot_own.reshape(-1, d_model)
        ff_width = w_up.shape[1]
        h_attn, h_mlp = tile_call(norm_kernel, [x_group], [small], [(d_model, jnp.bfloat16), (d_model, jnp.bfloat16)], (0, n_tok), 16 * x_group.size)
        qkv_act, pre_act, gelu_out = tile_call(
            front_kernel, [h_attn, h_mlp, *tables], [b_qkv.reshape(1, -1).astype(jnp.float32), b_up.reshape(1, -1).astype(jnp.float32), *w_in],
            [(qkv_width, jnp.bfloat16), (ff_width, jnp.bfloat16), (ff_width, jnp.bfloat16)], (0, n_tok), 2 * n_tok * in_size)
        qkv_seq = qkv_act.reshape(n_seq, seq_len, qkv_width)
        context = attn_fwd(qkv_seq).reshape(n_tok, head)
        blocks_per_seq = ty_size // 4
        y_form = ((ty_size, n_seq, own, d_model), (4, 1, own, d_model), lambda s: (lax.rem(s, blocks_per_seq), s // blocks_per_seq, 0, 0))
        (y_part,) = tile_call(y_kernel, [context, gelu_out], w_back, [(y_form, jnp.bfloat16)], (0, n_tok), 2 * n_tok * back_size, 4 * own)
        mixed = lax.psum_scatter(y_part.reshape(n_tok, d_model), 'ty', scatter_dimension=0, tiled=True)
        blocks = to_width(row_call(finish_y_kernel, tx_size, 0, n_seq * own, x_rows, mixed, bias_out.reshape(1, -1)))
        full = lax.all_gather(blocks.reshape(tx_size * n_seq, own, d_local), 'ty', axis=1, tiled=True)
        y_out = place_call(place_kernel, place, [full.reshape(tx_size, n_seq * seq_len, d_local)], None, 0, 1, n_seq * seq_len)

        d_ctx, d_pre, d_b_up = tile_call(
            d_pre_kernel, [cot_group, pre_act], w_back,
            [(head, jnp.bfloat16), (ff_width, jnp.bfloat16), ((8, ff_width), jnp.float32)], (0, n_tok), 2 * n_tok * back_size)
        d_ctx, d_b_up = d_ctx.reshape(n_seq, seq_len, head), d_b_up.sum(0)
        d_b_qkv, d_ln, dx_act = [], [], None
        for s in chunks:
            d_qkv, d_b_seq = attn_bwd(qkv_seq, d_ctx, s, (d_qkv, sums) if s else ())
            d_b_qkv.append(d_b_seq.sum((0, 1)))
            a6_part, sums = tile_call(
                d_h_kernel, [d_qkv.reshape(n_tok, qkv_width), d_pre, x_group], [small, *w_in],
                [(d_model, jnp.bfloat16), ((4, 8, d_model), jnp.float32)], (s * seq_len, seq_len), 2 * seq_len * in_size)
            d_ln.append(sums)
            value_a6 = lax.psum_scatter(a6_part, 'ty', scatter_dimension=0, tiled=True)
            parts = row_call(finish_dx_kernel, tx_size, s, own, x_rows, value_a6, cot_rows)
            block = to_width(parts)
            if s < n_seq - 1:
                assert ty_size == 8
                half = block.shape[0] // 2
                ahead, behind = along(block, 1), along(block, -1)
                halves = [along(ahead[:half], 1), along(behind[half:], -1)]
                far = pl.pallas_call(
                    join_kernel,
                    out_shape=jax.ShapeDtypeStruct(block.shape, block.dtype),
                    compiler_params=pltpu.CompilerParams(vmem_limit_bytes=16 * MIB),
                    name="cat",
                    cost_estimate=pl.CostEstimate(flops=block.size, bytes_accessed=4 * block.size, transcendentals=0),
                )(*halves)
                blocks = [block, ahead, far, behind]
                blocks = blocks + [partner(piece) for piece in blocks]
                dx_act = place_call(place_pieces_kernel, place, blocks, dx_act, s, n_seq, seq_len)
            else:
                full = lax.all_gather(block, 'ty', axis=1, tiled=True)
                dx_act = place_call(place_kernel, place, [full], dx_act, s, n_seq, seq_len)
        d_qkv = d_qkv.reshape(n_tok, qkv_width)

        d_ln = sum(d_ln).sum(1).reshape(4, tx_size, d_local)
        d_bias = jnp.concatenate([sum(d_b_qkv), d_b_up]).reshape(4, -1)
        sent = [jnp.concatenate([d_ln[:, r], d_bias], axis=1) for r in range(tx_size)]
        got = [sent[0]] + [shift(sent[r], -r) for r in range(1, tx_size)]
        got = sum(got[r] + got[r + antipode] for r in range(antipode))
        d_bias = got[:, d_local:].reshape(-1)
        d_ln = small_sum(got[:, :d_local], 'ty', ty_size)
        d_b_out = cot_out.astype(jnp.float32).sum((0, 1))

        in_shape, back_shape = (d_local, qkv_width + ff_width), (head + ff_width, d_local)
        in_blocks = lambda r: [(h_attn, r, d_local, d_qkv, 0, qkv_width, 0, 0), (h_mlp, r, d_local, d_pre, 0, ff_width, 0, qkv_width)]
        back_blocks = lambda r: [(context, 0, head, cot_group, r, d_local, 0, 0), (gelu_out, 0, ff_width, cot_group, r, d_local, head, 0)]
        add_back = ring_scatter(back_blocks, back_shape)
        add_in = ring_scatter(in_blocks, in_shape)
        whole = slice(None)
        d_w_dense, d_w_down = grad_call([back_blocks(0)], back_shape, [add_back], [[(slice(0, head), whole), (slice(head, None), whole)]], jnp.float32)
        d_w_qkv, d_w_up = grad_call([in_blocks(0)], in_shape, [add_in], [[(whole, slice(0, qkv_width)), (whole, slice(qkv_width, None))]], jnp.float32)
        y_out = y_out.reshape(batch, seq_len, d_local)
        return (y_out, dx_act, d_ln[0], d_ln[1], d_ln[2], d_ln[3], d_w_qkv.reshape(w_qkv.shape), d_bias[:qkv_width].reshape(b_qkv.shape), d_w_dense, d_b_out, d_w_up, d_bias[qkv_width:], d_w_down, d_b_out)

    return jax.shard_map(body, mesh=mesh, in_specs=in_specs, out_specs=out_specs, check_vma=False)
```
